256 devices in a mesh: dp: 4 (over x_hi, core), vocab: 64 (over y, z, x_lo).
Axes of the slice: x: 4 (x_hi: 2, x_lo: 2; x = x_hi * 2 + x_lo), y: 4, z: 8, core: 2. Of those that a mesh axis runs over, the one named last changes fastest.
Arguments:
- hidden: bfloat16 [1024, 2048], P('dp', 'vocab'), may hold values from -30 to 30
- table: bfloat16 [128000, 2048], P('vocab'), may hold values from -20 to 20
- targets: int32 [1024], P('dp'), may hold values from 0 to 127999
- input_ids: int32 [16384], P(('dp', 'vocab')), may hold values from 0 to 127999, as said below
- cotangent: bfloat16 [16384, 2048], P(('dp', 'vocab')), may hold values from -0.4375 to 0.4375
Outputs:
- token_loss: float32 [1024], P('dp')
- hidden_grad: bfloat16 [1024, 2048], P('dp', 'vocab')
- table_grad: bfloat16 [128000, 2048], P('vocab', 'dp')
The draws below stay inside these ranges and needn't reach their ends.
Inputs may be any that keep to these rules, and one draw needn't show every extreme that they name: `input_ids`: within the 64 rows of one device, at most 2 ids fall in any one block of 2000 consecutive ids (the rows of one index of vocab); in every draw some block receives exactly 2 ids from every device.
All inputs are finite; a program needn't handle non-finite values.
Results may differ from the reference program's by a relative error of at most 0.0034.
Values may be sent and summed in bfloat16 or wider, within the bound.
No kernel may reach another device: no remote copies, remote signals or barrier semaphores. Data moves between devices by JAX's collectives and lax.ppermute only.
A program may use at most 128 MiB of HBM per device.

```python
import math
import jax
import jax.numpy as jnp
import numpy as np
from jax import lax

D = 2048
V_DEV = 2000
IN_DEV = 64
VOCAB = 128000
TOKENS = 1024
IN_TOK = 16384
CAP = 2
N_DP = 4
N_VOCAB = 64


def table_line(base_key, row_index):
    return jax.random.normal(jax.random.fold_in(base_key, row_index), (D,), jnp.float32)


def common_axis(key):
    raw = jax.random.normal(jax.random.fold_in(key, 601), (D,), jnp.float32)
    return raw / jnp.sqrt(jnp.sum(raw * raw))


def draw_table(key, part):
    base_key = jax.random.fold_in(key, 501)
    values = jax.vmap(lambda row_index: table_line(base_key, row_index))(jnp.arange(VOCAB))
    values = jnp.clip(values, -6.0, 6.0)
    favored_count = min(16, V_DEV // 2)
    picks = jax.random.randint(jax.random.fold_in(key, 602), (VOCAB, 1), 0, V_DEV) < favored_count
    levels = jax.random.uniform(jax.random.fold_in(key, 603), (VOCAB, 1), jnp.float32, 4.0, 7.0)
    direction = common_axis(key)
    values = jnp.where(picks, 0.5 * values + levels * direction[None, :], values)
    return values.astype(jnp.bfloat16)


def draw_hidden(key, part):
    spread = 0.9 * D ** (-0.5)
    direction = common_axis(key)
    noise = jnp.clip(jax.random.normal(jax.random.fold_in(key, 11), (TOKENS, D), jnp.float32), -6.0, 6.0)
    amounts = jnp.exp(jax.random.uniform(jax.random.fold_in(key, 14), (TOKENS, 1), jnp.float32, math.log(0.7), math.log(1.4)))
    values = noise * spread + amounts * direction[None, :]
    return values.astype(jnp.bfloat16)


def draw_input_ids(key, part):
    common = jax.random.fold_in(key, 777)
    forced = jax.random.randint(jax.random.fold_in(common, 1), (), 0, N_VOCAB)
    popular = jax.random.randint(jax.random.fold_in(common, 2), (N_VOCAB,), 0, 4) * 4096
    slot_total = N_VOCAB * CAP
    slot_owner = jnp.arange(slot_total) // CAP

    def one_block(block_index):
        block_key = jax.random.fold_in(common, block_index + 10)
        noise = jax.random.randint(jax.random.fold_in(block_key, 1), (slot_total,), 0, 4096)
        score = noise + popular[slot_owner] + jnp.where(slot_owner == forced, 65536, 0)
        distinct = score * slot_total + jnp.arange(slot_total)
        order = jnp.argsort(-distinct, stable=True)
        chosen = slot_owner[order[:IN_DEV]]
        chosen = jax.random.permutation(jax.random.fold_in(block_key, 2), chosen)
        first_draw = jax.random.randint(jax.random.fold_in(block_key, 3), (IN_DEV,), 0, V_DEV)
        second_draw = jax.random.randint(jax.random.fold_in(block_key, 4), (IN_DEV,), 0, V_DEV)
        offset = first_draw * second_draw // V_DEV
        return chosen * V_DEV + offset
    blocks = jax.vmap(one_block)(jnp.arange(N_DP * N_VOCAB))
    return blocks.reshape(-1).astype(jnp.int32)


def place_ends(values, stream_key, low, largest):
    longest = values.shape.index(max(values.shape))
    spots = []
    for shift in (0, 1):
        where = [jax.random.randint(jax.random.fold_in(stream_key, axis), (), 0, length) for axis, length in enumerate(values.shape)]
        where[longest] = (where[longest] + shift) % values.shape[longest]
        spots.append(tuple(where))
    return values.at[spots[0]].set(low).at[spots[1]].set(largest)


def steps_of(rng, shape, shards, low, top_value):
    level = 1.0
    for axis_at, parts in shards:
        steps = jax.random.uniform(jax.random.fold_in(jax.random.fold_in(rng, 6), axis_at), (parts,), jnp.float32, low / len(shards), top_value / len(shards))
        level = level * jnp.repeat(jnp.exp(steps), shape[axis_at] // parts).reshape((-1,) + (1,) * (len(shape) - 1 - axis_at))
    return level


def skewed_wide(key, extent, count, skew):
    weights = [min(1 << octave, count + 1 - (1 << octave)) * (1 << 20) // math.isqrt((1 << octave) ** skew) + 1 for octave in range((count + 1).bit_length()) if 1 << octave <= count]
    deviation = 1 + sum(weights) // (1 << 30)
    listing = np.cumsum(np.array([max(1, weight // deviation) for weight in weights]))
    lot = jax.random.randint(jax.random.fold_in(key, 1), extent, 0, int(listing[len(weights) - 1]))
    start = jnp.left_shift(1, jnp.searchsorted(jnp.asarray(listing, jnp.int32), lot, side="right").astype(jnp.int32))
    rank = start - 1 + jax.random.randint(jax.random.fold_in(key, 4), extent, 0, 1 << 30) % jnp.minimum(start, count + 1 - start)
    return jax.random.permutation(jax.random.fold_in(key, 2), count)[rank].astype(jnp.int32)


def normal_values(rng, shape, width, limit, cuts=(), kind=jnp.bfloat16):
    level = steps_of(rng, shape, cuts, -0.22, 0.18) if cuts else 1.0
    values = jax.random.normal(rng, shape, jnp.float32) * width * level
    return jnp.minimum(jnp.maximum(values, -limit), limit).astype(kind)


def setup_inputs(seed: int = 0) -> dict:
    arg_keys = jax.random.split(jax.random.key(seed), 6)
    hidden = draw_hidden(jax.random.fold_in(arg_keys[5], 71), 0)
    table = draw_table(jax.random.fold_in(arg_keys[5], 71), 0)
    targets = place_ends(skewed_wide(arg_keys[2], (TOKENS,), VOCAB, 1), jax.random.fold_in(arg_keys[2], 3), 0, VOCAB - 1).astype(jnp.int32)
    input_ids = draw_input_ids(jax.random.fold_in(arg_keys[5], 71), 0)
    cotangent = normal_values(arg_keys[4], (IN_TOK, D), 0.03, 0.4375, ((0, 256),))
    return {"hidden": hidden, "table": table, "targets": targets, "input_ids": input_ids, "cotangent": cotangent}


def reference(hidden, table, targets, input_ids, cotangent):
    blocks = table.reshape(N_VOCAB, V_DEV, D)
    starts = jnp.arange(N_VOCAB, dtype=jnp.int32) * V_DEV
    cot_wide = cotangent.astype(jnp.float32)

    def block_logits(rows):
        return lax.dot_general(hidden, rows, (((1,), (1,)), ((), ())), preferred_element_type=jnp.float32)

    def stats_step(carry, item):
        running_max, running_sum, target_logit = carry
        rows, first_row = item
        logits = block_logits(rows)
        columns = lax.broadcasted_iota(jnp.int32, logits.shape, 1) + first_row
        target_logit = target_logit + jnp.sum(jnp.where(columns == targets[:, None], logits, 0.0), axis=1)
        new_max = jnp.maximum(running_max, jnp.max(logits, axis=1))
        running_sum = running_sum * jnp.exp(running_max - new_max) + jnp.sum(jnp.exp(logits - new_max[:, None]), axis=1)
        return (new_max, running_sum, target_logit), None

    start_carry = (jnp.full((TOKENS,), -jnp.inf, jnp.float32), jnp.zeros((TOKENS,), jnp.float32), jnp.zeros((TOKENS,), jnp.float32))
    (row_max, row_sum, target_logit), unused = lax.scan(stats_step, start_carry, (blocks, starts))
    token_loss = row_max + jnp.log(row_sum) - target_logit

    def grad_step(hidden_acc, item):
        rows, first_row = item
        logits = block_logits(rows)
        columns = lax.broadcasted_iota(jnp.int32, logits.shape, 1) + first_row
        residual = (jnp.exp(logits - row_max[:, None]) / row_sum[:, None] - jnp.where(columns == targets[:, None], 1.0, 0.0)).astype(jnp.bfloat16)
        hidden_acc = hidden_acc + jnp.dot(residual, rows, preferred_element_type=jnp.float32)
        local_ids = input_ids - first_row
        local_ids = jnp.where((local_ids >= 0) & (local_ids < V_DEV), local_ids, V_DEV).astype(jnp.int32)
        scattered = jax.ops.segment_sum(cot_wide, local_ids, num_segments=V_DEV + 1)[:V_DEV]
        table_part = lax.dot_general(residual, hidden, (((0,), (0,)), ((), ())), preferred_element_type=jnp.float32) + scattered
        return hidden_acc, table_part.astype(jnp.bfloat16)

    hidden_acc, table_parts = lax.scan(grad_step, jnp.zeros((TOKENS, D), jnp.float32), (blocks, starts))
    return token_loss, hidden_acc.astype(jnp.bfloat16), table_parts.reshape(VOCAB, D)
```

```python
import jax
import jax.numpy as jnp
from jax import lax
from jax.sharding import Mesh, PartitionSpec as P

BF16 = jnp.bfloat16
F32 = jnp.float32
ALL = ("xh", "c", "y", "z", "xl")
DP = ("xh", "c")
VOCAB = ("y", "z", "xl")
PLANE = ("y", "xl")


def exchange(pieces, axes):
    return lax.all_to_all(pieces, axes, 0, 0, tiled=True)


def to_each(value, count):
    return jnp.broadcast_to(value, (count, *value.shape))


def swap(value, axis):
    return lax.ppermute(value, axis, [(0, 1), (1, 0)])


def by_plane(rows, ny, nz, nx):
    tail = rows.shape[1:]
    rows = rows.reshape(ny, nz, nx, -1, *tail)
    return rows.transpose(0, 2, 1, 3, *range(4, 4 + len(tail)))


def body(hidden, table, targets, input_ids, cotangent):
    vocab_rows, width = table.shape
    ny, nz, nx = (lax.axis_size(a) for a in VOCAB)
    plane = ny * nx
    vocab_count = plane * nz
    data_count = lax.axis_size(DP)
    block = width // data_count
    first_row = lax.axis_index(VOCAB) * vocab_rows
    xh, c = lax.axis_index("xh"), lax.axis_index("c")

    owners = input_ids // vocab_rows
    offsets = input_ids - owners * vocab_rows
    count = input_ids.shape[0]
    later = lax.broadcasted_iota(jnp.int32, (count, count), 0)
    early = lax.broadcasted_iota(jnp.int32, (count, count), 1)
    before = (owners[:, None] == owners[None, :]) & (early < later)
    slot = owners * 2 + jnp.sum(before.astype(jnp.int32), axis=1)
    chosen = lax.broadcasted_iota(jnp.int32, (2 * vocab_count, count), 0) == slot[None, :]
    sent = jnp.dot(chosen.astype(BF16), cotangent, preferred_element_type=F32).astype(BF16)
    spots = jnp.sum(jnp.where(chosen, offsets[None, :] + 1, 0), axis=1)
    lane = lax.broadcasted_iota(jnp.int32, (2 * vocab_count, 128), 1)
    code = jnp.where(lane == 0, (spots // 64)[:, None], jnp.where(lane == 1, (spots % 64)[:, None], 0))
    code = code.astype(BF16)
    sent = jnp.stack(
        [jnp.concatenate([sent[:, d * block : (d + 1) * block], code], axis=1) for d in range(data_count)]
    )
    sent = sent.reshape(data_count * vocab_count, 2, block + 128)

    mine = hidden.T
    stage = exchange(to_each(mine, nz), "z").reshape(-1, mine.shape[1])
    stage = exchange(to_each(stage, plane), PLANE)
    tokens = mine.shape[1]
    hid = stage.reshape(ny, nx, nz, -1, tokens).transpose(0, 2, 1, 3, 4).reshape(width, tokens)
    logits = jnp.dot(table, hid, preferred_element_type=F32)
    rows = lax.broadcasted_iota(jnp.int32, logits.shape, 0)
    hit = rows == (targets - first_row)[None, :]
    picked = jnp.sum(jnp.where(hit, logits, 0.0), axis=0)
    top = jnp.max(logits, axis=0)
    total = jnp.sum(jnp.exp(logits - top[None]), axis=0)
    stats = exchange(to_each(jnp.stack([top, total, picked]), vocab_count), VOCAB)
    row_max = jnp.max(stats[:, 0], axis=0)
    row_sum = jnp.sum(stats[:, 1] * jnp.exp(stats[:, 0] - row_max[None]), axis=0)
    token_loss = row_max + jnp.log(row_sum) - jnp.sum(stats[:, 2], axis=0)
    residual = (jnp.exp(logits - row_max[None]) / row_sum[None] - jnp.where(hit, 1.0, 0.0)).astype(BF16)

    part = lax.dot_general(table, residual, (((0,), (0,)), ((), ())), preferred_element_type=F32)
    part = by_plane(part.astype(BF16), ny, nz, nx).reshape(plane, -1, tokens)
    part = exchange(part, PLANE)
    part = jnp.sum(part.astype(F32), axis=0).reshape(nz, -1, tokens)
    part = jnp.sum(exchange(part, "z"), axis=0)
    hidden_grad = part.astype(BF16).T

    res_far = swap(residual, "xh")
    res_sib = swap(residual, "c")
    res_far_sib = swap(res_far, "c")

    def cut(value, start, size):
        return lax.dynamic_slice_in_dim(value, start, size, 0)

    hb_own = cut(hid, (2 * xh + c) * block, block)
    hb_sib = swap(cut(hid, (2 * xh + 1 - c) * block, block), "c")
    far = swap(cut(hid, 2 * (1 - xh) * block, 2 * block), "xh")
    hb_far = cut(far, c * block, block)
    hb_far_sib = swap(cut(far, (1 - c) * block, block), "c")
    res_all = jnp.concatenate([residual, res_sib, res_far, res_far_sib], axis=1)
    hid_all = jnp.concatenate([hb_own, hb_sib, hb_far, hb_far_sib], axis=1)

    got = exchange(sent, ALL).reshape(-1, block + 128)
    code = got[:, block:].astype(F32)
    place = (code[:, 0] * 64 + code[:, 1]).astype(jnp.int32) - 1
    match = lax.broadcasted_iota(jnp.int32, (vocab_rows, place.shape[0]), 0) == place[None, :]
    start = jnp.dot(match.astype(BF16), got[:, :block], preferred_element_type=F32)
    table_grad = start + lax.dot_general(
        res_all, hid_all, (((1,), (1,)), ((), ())), preferred_element_type=F32
    )
    return token_loss, hidden_grad, table_grad.astype(BF16)


def solution(mesh):
    fine = Mesh(mesh.devices.reshape(2, 2, 4, 8, 2), ALL)
    placed = (P(DP, VOCAB), P(VOCAB, None), P(DP), P(ALL), P(ALL, None))
    return jax.shard_map(
        body,
        mesh=fine,
        in_specs=placed,
        out_specs=(P(DP), P(DP, VOCAB), P(VOCAB, DP)),
        check_vma=False,
    )
```

```python
import functools

import jax
import jax.numpy as jnp
from jax import lax
from jax.experimental import pallas as pl
from jax.experimental.pallas import tpu as pltpu
from jax.sharding import Mesh, PartitionSpec as P

BF16 = jnp.bfloat16
F32 = jnp.float32
I32 = jnp.int32
ALL = ("xh", "c", "y", "z", "xl")
DP = ("xh", "c")
VOCAB = ("y", "z", "xl")
PLANE = ("y", "xl")
CHUNK = 400
PARAMS = pltpu.CompilerParams(vmem_limit_bytes=48 * 1024 * 1024)


def exchange(pieces, axes):
    return lax.all_to_all(pieces, axes, 0, 0, tiled=True)


def to_each(value, count):
    return jnp.broadcast_to(value, (count, *value.shape))


def swap(value, axis):
    return lax.ppermute(value, axis, [(0, 1), (1, 0)])


def cost(flops, moved, special=0):
    return pl.CostEstimate(flops=flops, bytes_accessed=moved, transcendentals=special)


def logits_kernel(where_ref, tgt_ref, got_ref, table_ref, near_ref, far_ref, stats_ref, hid, log, acc):
    step = pl.program_id(0)
    rows, tokens = table_ref.shape[0], hid.shape[1]
    width = hid.shape[0]
    half = width // 2

    @pl.when(step == 0)
    def _():
        plane, depth, _ = got_ref.shape
        nz = depth // 32
        nx = 2
        for p in range(plane):
            y, x = p // nx, p % nx
            for z in range(nz):
                at = ((y * nz + z) * nx + x) * 32
                hid[at : at + 32, :] = got_ref[p, z * 32 : z * 32 + 32, :]
        acc[0:1, :] = jnp.full((1, tokens), -jnp.inf, F32)
        acc[1:2, :] = jnp.zeros((1, tokens), F32)

    values = jnp.dot(table_ref[...], hid[...], preferred_element_type=F32)
    log[pl.ds(pl.multiple_of(step * rows, rows), rows), :] = values
    index = lax.broadcasted_iota(I32, values.shape, 0) + (where_ref[0] + step * rows)
    acc[1:2, :] += jnp.sum(jnp.where(index == tgt_ref[...], values, 0.0), axis=0, keepdims=True)
    acc[0:1, :] = jnp.maximum(acc[0:1, :], jnp.max(values, axis=0, keepdims=True))

    @pl.when(step == pl.num_programs(0) - 1)
    def _():
        top = acc[0:1, :]
        piece = 80

        def one(i, total):
            at = pl.ds(pl.multiple_of(i * piece, piece), piece)
            e = jnp.exp(log[at, :] - top)
            near_ref[at, :] = e.astype(BF16)
            far_ref[at, :] = e.astype(BF16)
            return total + jnp.sum(e, axis=0, keepdims=True)

        count = log.shape[0]
        total = lax.fori_loop(0, count // piece, one, jnp.zeros((1, tokens), F32))
        base = near_ref.shape[0] - half
        near_ref[count:base, :] = jnp.zeros((base - count, tokens), BF16)
        far_ref[count:base, :] = jnp.zeros((base - count, tokens), BF16)
        near_ref[base:, :] = hid[pl.ds(pl.multiple_of(where_ref[1] * half, half), half), :]
        far_ref[base:, :] = hid[pl.ds(pl.multiple_of((1 - where_ref[1]) * half, half), half), :]
        line = jnp.concatenate([top, total, acc[1:2, :], jnp.zeros((1, tokens), F32)], axis=0)
        stats_ref[...] = jnp.broadcast_to(line[None], stats_ref.shape)


def logits_call(where, targets, got, table, copies):
    count, width = table.shape
    tokens = got.shape[2]
    span = 2048 + width // 2
    return pl.pallas_call(
        logits_kernel,
        grid_spec=pltpu.PrefetchScalarGridSpec(
            num_scalar_prefetch=1,
            grid=(count // CHUNK,),
            in_specs=[
                pl.BlockSpec((1, tokens), lambda i, s: (0, 0)),
                pl.BlockSpec(got.shape, lambda i, s: (0, 0, 0)),
                pl.BlockSpec((CHUNK, width), lambda i, s: (i, 0)),
            ],
            out_specs=[
                pl.BlockSpec((span, tokens), lambda i, s: (0, 0)),
                pl.BlockSpec((span, tokens), lambda i, s: (0, 0)),
                pl.BlockSpec((copies, 4, tokens), lambda i, s: (0, 0, 0)),
            ],
            scratch_shapes=[
                pltpu.VMEM((width, tokens), BF16),
                pltpu.VMEM((count, tokens), F32),
                pltpu.VMEM((8, tokens), F32),
            ],
        ),
        out_shape=[
            jax.ShapeDtypeStruct((span, tokens), BF16),
            jax.ShapeDtypeStruct((span, tokens), BF16),
            jax.ShapeDtypeStruct((copies, 4, tokens), F32),
        ],
        compiler_params=PARAMS,
        cost_estimate=cost(2 * count * width * tokens, 2 * count * width + 4 * span * tokens),
        name="logits",
    )(where, targets, got, table)


def part_kernel(where_ref, tgt_ref, e_ref, table_ref, soft_ref, hard_ref, lhs):
    tokens = tgt_ref.shape[1]
    count = table_ref.shape[0]

    @pl.when(pl.program_id(0) == 0)
    def _():
        index = lax.broadcasted_iota(I32, (count, tokens), 0) + where_ref[0]
        hit = jnp.where(index == tgt_ref[...], 1.0, 0.0).astype(BF16)
        lhs[0:tokens, :] = e_ref[...].T
        lhs[tokens:, :] = hit.T

    both = jnp.dot(lhs[...], table_ref[...], preferred_element_type=F32)
    soft = both[0:tokens, :].T
    hard = both[tokens:, :].T
    for k in range(soft.shape[0] // 32):
        z, x = k // 2, k % 2
        soft_ref[x, z * 32 : z * 32 + 32, :] = soft[k * 32 : k * 32 + 32, :]
        hard_ref[x, z * 32 : z * 32 + 32, :] = hard[k * 32 : k * 32 + 32, :].astype(BF16)


def part_call(where, targets, near, table):
    count, width = table.shape
    tokens = targets.shape[1]
    wide = 256
    spec = pl.BlockSpec((2, wide // 2, tokens), lambda j, s: (j // 2, j % 2, 0))
    return pl.pallas_call(
        part_kernel,
        grid_spec=pltpu.PrefetchScalarGridSpec(
            num_scalar_prefetch=1,
            grid=(width // wide,),
            in_specs=[
                pl.BlockSpec((1, tokens), lambda j, s: (0, 0)),
                pl.BlockSpec((count, tokens), lambda j, s: (0, 0)),
                pl.BlockSpec((count, wide), lambda j, s: (0, j)),
            ],
            out_specs=[spec, spec],
            scratch_shapes=[pltpu.VMEM((2 * tokens, count), BF16)],
        ),
        out_shape=[
            jax.ShapeDtypeStruct((8, width // 8, tokens), F32),
            jax.ShapeDtypeStruct((8, width // 8, tokens), BF16),
        ],
        compiler_params=PARAMS,
        cost_estimate=cost(4 * count * width * tokens, 2 * count * width + 6 * width * tokens),
        name="part",
    )(where, targets, near, table)


def scale_kernel(where_ref, tgt_ref, own_ref, stats_ref, soft_ref, hard_ref, out_ref, loss_ref, w_ref, keep):
    @pl.when(pl.program_id(0) == 0)
    def _():
        stats = stats_ref[...]
        peak = jnp.max(stats, axis=0)
        top = peak[0:1, :]
        sums = jnp.sum(stats[:, 1:2, :] * jnp.exp(stats[:, 0:1, :] - top[None]), axis=0)
        picks = jnp.sum(stats, axis=0)[2:3, :]
        loss_ref[...] = top + jnp.log(sums) - picks
        local_top, local_pick = own_ref[0, 0:1, :], own_ref[0, 2:3, :]
        w = jnp.exp(local_top - top) / sums
        prob = jnp.exp(local_pick - top) / sums
        soft = jnp.exp(local_pick - local_top).astype(BF16).astype(F32) * w
        gap = (prob - 1.0).astype(BF16).astype(F32) - soft
        keep[0:1, :] = w
        keep[1:2, :] = gap
        w_ref[...] = jnp.concatenate(
            [w, tgt_ref[...].astype(F32), jnp.zeros((6, w.shape[1]), F32)], axis=0
        )

    out_ref[...] = (
        soft_ref[...] * keep[0:1, :][None] + hard_ref[...].astype(F32) * keep[1:2, :][None]
    ).astype(BF16)


def scale_call(where, targets, own, stats, soft, hard):
    plane, depth, tokens = soft.shape
    spec = pl.BlockSpec((2, depth, tokens), lambda p, s: (p, 0, 0))
    return pl.pallas_call(
        scale_kernel,
        grid_spec=pltpu.PrefetchScalarGridSpec(
            num_scalar_prefetch=1,
            grid=(plane // 2,),
            in_specs=[
                pl.BlockSpec((1, tokens), lambda p, s: (0, 0)),
                pl.BlockSpec((1, 4, tokens), lambda p, s: (0, 0, 0)),
                pl.BlockSpec(stats.shape, lambda p, s: (0, 0, 0)),
                spec,
                spec,
            ],
            out_specs=[
                spec,
                pl.BlockSpec((1, tokens), lambda p, s: (0, 0)),
                pl.BlockSpec((8, tokens), lambda p, s: (0, 0)),
            ],
            scratch_shapes=[pltpu.VMEM((8, tokens), F32)],
        ),
        out_shape=[
            jax.ShapeDtypeStruct((plane, depth, tokens), BF16),
            jax.ShapeDtypeStruct((1, tokens), F32),
            jax.ShapeDtypeStruct((8, tokens), F32),
        ],
        compiler_params=PARAMS,
        cost_estimate=cost(4 * plane * depth * tokens, 8 * plane * depth * tokens),
        name="scale",
    )(where, targets, own, stats, soft, hard)


def table_kernel(where_ref, w_ref, place_ref, rows_ref, *refs):
    out_ref = refs[-1]
    count = out_ref.shape[0]
    first = pl.program_id(0) * count
    index = lax.broadcasted_iota(I32, (count, 256), 0) + first
    near = index + where_ref[0]
    slots = place_ref.shape[1]
    match = jnp.concatenate(
        [
            jnp.where(index == place_ref[:, k : k + 256], 1.0, 0.0).astype(BF16)
            for k in range(0, slots, 256)
        ],
        axis=1,
    )
    total = jnp.dot(match, rows_ref[...], preferred_element_type=F32)
    for g in range(4):
        e = refs[2 * g][...].astype(F32)
        w = w_ref[g, 0:1, :]
        target = w_ref[g, 1:2, :].astype(I32)
        res = (e * w - jnp.where(near == target, 1.0, 0.0)).astype(BF16)
        total += lax.dot_general(
            res, refs[2 * g + 1][...], (((1,), (1,)), ((), ())), preferred_element_type=F32
        )
    out_ref[...] = total.astype(BF16)


def table_call(where, w, place, rows, packs, count):
    tokens = packs[0].shape[1]
    block = rows.shape[1] // 128 * 128
    block = 512
    specs, operands = [], []
    for pack in packs:
        specs.append(pl.BlockSpec((CHUNK, tokens), lambda i, s: (i, 0)))
        specs.append(pl.BlockSpec((block, tokens), lambda i, s: (4 + s[2], 0)))
        operands += [pack, pack]
    return pl.pallas_call(
        table_kernel,
        grid_spec=pltpu.PrefetchScalarGridSpec(
            num_scalar_prefetch=1,
            grid=(count // CHUNK,),
            in_specs=[
                pl.BlockSpec(w.shape, lambda i, s: (0, 0, 0)),
                pl.BlockSpec(place.shape, lambda i, s: (0, 0)),
                pl.BlockSpec((rows.shape[0], block), lambda i, s: (0, 0)),
                *specs,
            ],
            out_specs=pl.BlockSpec((CHUNK, block), lambda i, s: (i, 0)),
        ),
        out_shape=jax.ShapeDtypeStruct((count, block), BF16),
        compiler_params=PARAMS,
        cost_estimate=cost(2 * count * block * 1536, 8 * count * 256 + 2 * count * block),
        name="table_grad",
    )(where, w, place, rows, *operands)


def body(hidden, table, targets, input_ids, cotangent):
    vocab_rows, width = table.shape
    ny, nz, nx = (lax.axis_size(a) for a in VOCAB)
    plane = ny * nx
    vocab_count = plane * nz
    data_count = lax.axis_size(DP)
    block = width // data_count
    xh, c = lax.axis_index("xh"), lax.axis_index("c")
    where = jnp.stack([lax.axis_index(VOCAB) * vocab_rows, xh, c]).astype(I32)
    tokens = hidden.shape[0]
    goal = targets.reshape(1, tokens)

    owners = input_ids // vocab_rows
    offsets = input_ids - owners * vocab_rows
    count = input_ids.shape[0]
    later = lax.broadcasted_iota(I32, (count, count), 0)
    early = lax.broadcasted_iota(I32, (count, count), 1)
    before = (owners[:, None] == owners[None, :]) & (early < later)
    slot = owners * 2 + jnp.sum(before.astype(I32), axis=1)
    chosen = lax.broadcasted_iota(I32, (2 * vocab_count, count), 0) == slot[None, :]
    sent = jnp.dot(chosen.astype(BF16), cotangent, preferred_element_type=F32).astype(BF16)
    spots = jnp.sum(jnp.where(chosen, offsets[None, :] + 1, 0), axis=1)
    lane = lax.broadcasted_iota(I32, (2 * vocab_count, 128), 1)
    code = jnp.where(lane == 0, (spots // 64)[:, None], jnp.where(lane == 1, (spots % 64)[:, None], 0))
    code = code.astype(BF16)
    sent = jnp.stack(
        [jnp.concatenate([sent[:, d * block : (d + 1) * block], code], axis=1) for d in range(data_count)]
    )
    sent = sent.reshape(data_count * vocab_count, 2, block + 128)

    mine = hidden.T
    stage = exchange(to_each(mine, nz), "z").reshape(-1, tokens)
    stage = exchange(to_each(stage, plane), PLANE)

    near, far, own = logits_call(where, goal, stage, table, vocab_count)
    stats = exchange(own, VOCAB)
    near_sib = swap(near, "c")
    far = swap(far, "xh")
    far_sib = swap(far, "c")
    soft, hard = part_call(where, goal, near, table)
    part, loss, w = scale_call(where, goal, own, stats, soft, hard)

    part = exchange(part, PLANE)
    part = jnp.sum(part.astype(F32), axis=0).reshape(nz, -1, tokens)
    part = jnp.sum(exchange(part, "z"), axis=0)
    hidden_grad = part.astype(BF16).T

    w_near = jnp.stack([w, swap(w, "c")])
    w_all = jnp.concatenate([w_near, swap(w_near, "xh")], axis=0)

    got = exchange(sent, ALL).reshape(-1, block + 128)
    code = got[:, block:].astype(F32)
    place = (code[:, 0] * 64 + code[:, 1]).astype(I32) - 1
    table_grad = table_call(
        where, w_all, place.reshape(1, -1), got, (near, near_sib, far, far_sib), vocab_rows
    )
    return loss.reshape(tokens), hidden_grad, table_grad


def solution(mesh):
    fine = Mesh(mesh.devices.reshape(2, 2, 4, 8, 2), ALL)
    placed = (P(DP, VOCAB), P(VOCAB, None), P(DP), P(ALL), P(ALL, None))
    return jax.shard_map(
        body,
        mesh=fine,
        in_specs=placed,
        out_specs=(P(DP), P(DP, VOCAB), P(VOCAB, DP)),
        check_vma=False,
    )
```

```python
import functools

import jax
import jax.numpy as jnp
from jax import lax
from jax.experimental import pallas as pl
from jax.experimental.pallas import tpu as pltpu
from jax.sharding import Mesh, PartitionSpec as P

BF16 = jnp.bfloat16
F32 = jnp.float32
I32 = jnp.int32
ALL = ("xh", "c", "y", "z", "xl")
DP = ("xh", "c")
VOCAB = ("y", "z", "xl")
PLANE = ("y", "xl")
CHUNK = 400
PARAMS = pltpu.CompilerParams(vmem_limit_bytes=24 * 1024 * 1024)


def exchange(pieces, axes):
    return lax.all_to_all(pieces, axes, 0, 0, tiled=True)


def to_each(value, count):
    return jnp.broadcast_to(value, (count, *value.shape))


def swap(value, axis):
    return lax.ppermute(value, axis, [(0, 1), (1, 0)])


def cost(flops, moved, special=0):
    return pl.CostEstimate(flops=flops, bytes_accessed=moved, transcendentals=special)


def shift(value, axis, by):
    size = lax.axis_size(axis)
    return lax.ppermute(value, axis, [(i, (i + by) % size) for i in range(size)])


def select_kernel(vocab_rows, where_ref, ids_ref, *refs):
    packs, outs = refs[:4], refs[4:]
    groups, count = ids_ref.shape
    total = groups * count
    line = jnp.concatenate([ids_ref[g : g + 1, :] for g in range(groups)], axis=1).astype(F32)
    tall = jnp.broadcast_to(line, (8, total)).T[:, 0:1]

    def parts(ids):
        owner = jnp.floor((ids + 0.5) * (1.0 / vocab_rows))
        spot = (ids - owner * vocab_rows).astype(I32) + 1
        owner = owner.astype(I32)
        plane = (owner >> 4) * 2 + (owner & 1)
        turn = (((owner >> 1) & 7) - where_ref[3]) & 7
        return owner, plane, turn, spot

    owner, plane, turn, _ = parts(line)
    owner_t, plane_t, turn_t, spot_t = parts(tall)
    early = lax.broadcasted_iota(I32, (total, total), 0)
    later = lax.broadcasted_iota(I32, (total, total), 1)
    before = (owner_t == owner) & (early < later) & ((early >> 6) == (later >> 6))
    rank = jnp.sum(jnp.where(before, 1.0, 0.0), axis=0, keepdims=True).astype(I32)
    token = lax.broadcasted_iota(I32, (1, total), 1)
    row = (token >> 6) * 2 + rank
    slots = turn * 64 + plane * 8 + row
    chosen = lax.broadcasted_iota(I32, (512, total), 0) == slots
    cot = jnp.concatenate([p[...] for p in packs], axis=0)
    picked = jnp.dot(jnp.where(chosen, 1.0, 0.0).astype(BF16), cot, preferred_element_type=F32)
    picked = picked.astype(BF16)
    lane = lax.broadcasted_iota(I32, (total, 128), 1)
    base = turn_t * 16 + plane_t
    digits = jnp.where(lane == base, spot_t >> 6, jnp.where(lane == base + 8, spot_t & 63, 0))
    mark = lax.broadcasted_iota(I32, (64, total), 0) == turn * 8 + row
    code = jnp.dot(
        jnp.where(mark, 1.0, 0.0).astype(BF16),
        digits.astype(F32).astype(BF16),
        preferred_element_type=F32,
    )
    width = cot.shape[1]
    code = jnp.concatenate([code, jnp.zeros((64, width - 128), F32)], axis=1).astype(BF16)
    for k, out in enumerate(outs):
        out[0:64, :] = picked[k * 64 : k * 64 + 64, :]
        out[64:72, :] = code[k * 8 : k * 8 + 8, :]


def select_call(where, ids, packs, vocab_rows):
    count, wide = packs[0].shape
    block = wide // 2
    out = pl.BlockSpec((72, block), lambda i, s: (0, 0))
    return pl.pallas_call(
        functools.partial(select_kernel, vocab_rows),
        grid_spec=pltpu.PrefetchScalarGridSpec(
            num_scalar_prefetch=1,
            grid=(1,),
            in_specs=[
                pl.BlockSpec(ids.shape, lambda i, s: (0, 0)),
                *[pl.BlockSpec((count, block), lambda i, s: (0, s[2]))] * 4,
            ],
            out_specs=[out] * 8,
        ),
        out_shape=[jax.ShapeDtypeStruct((72, block), BF16)] * 8,
        compiler_params=PARAMS,
        cost_estimate=cost(2 * 512 * 256 * block, 2**20),
        name="select",
    )(where, ids, *packs)


def regroup_kernel(*refs):
    turns, out_ref = refs[:-1], refs[-1]
    code = turns[0][64:72, :].astype(F32)
    for turn in turns[1:]:
        code += turn[64:72, :].astype(F32)
    for p in range(out_ref.shape[0]):
        for k, turn in enumerate(turns):
            out_ref[p, k * 8 : k * 8 + 8, :] = turn[p * 8 : p * 8 + 8, :]
        out_ref[p, 64:72, :] = code.astype(BF16)


def regroup_call(turns):
    return pl.pallas_call(
        regroup_kernel,
        out_shape=jax.ShapeDtypeStruct((8, *turns[0].shape), BF16),
        compiler_params=PARAMS,
        cost_estimate=cost(0, 2**20),
        name="regroup",
    )(*turns)


def logits_kernel(where_ref, tgt_ref, got_ref, table_ref, near_ref, far_ref, stats_ref, hid, log, acc):
    step = pl.program_id(0)
    rows, tokens = table_ref.shape[0], hid.shape[1]
    width = hid.shape[0]
    half = width // 2

    @pl.when(step == 0)
    def _():
        plane, depth, _ = got_ref.shape
        nz = depth // 32
        nx = 2
        for p in range(plane):
            y, x = p // nx, p % nx
            for z in range(nz):
                at = ((y * nz + z) * nx + x) * 32
                hid[at : at + 32, :] = got_ref[p, z * 32 : z * 32 + 32, :]
        acc[0:1, :] = jnp.full((1, tokens), -jnp.inf, F32)
        acc[1:2, :] = jnp.zeros((1, tokens), F32)

    values = jnp.dot(table_ref[...], hid[...], preferred_element_type=F32)
    log[pl.ds(pl.multiple_of(step * rows, rows), rows), :] = values
    index = lax.broadcasted_iota(I32, values.shape, 0) + (where_ref[0] + step * rows)
    acc[1:2, :] += jnp.sum(jnp.where(index == tgt_ref[...], values, 0.0), axis=0, keepdims=True)
    acc[0:1, :] = jnp.maximum(acc[0:1, :], jnp.max(values, axis=0, keepdims=True))

    @pl.when(step == pl.num_programs(0) - 1)
    def _():
        top = acc[0:1, :]
        piece = 80

        def one(i, total):
            at = pl.ds(pl.multiple_of(i * piece, piece), piece)
            e = jnp.exp(log[at, :] - top)
            near_ref[at, :] = e.astype(BF16)
            far_ref[at, :] = e.astype(BF16)
            return total + jnp.sum(e, axis=0, keepdims=True)

        count = log.shape[0]
        total = lax.fori_loop(0, count // piece, one, jnp.zeros((1, tokens), F32))
        base = near_ref.shape[0] - half
        near_ref[count:base, :] = jnp.zeros((base - count, tokens), BF16)
        far_ref[count:base, :] = jnp.zeros((base - count, tokens), BF16)
        near_ref[base:, :] = hid[pl.ds(pl.multiple_of(where_ref[1] * half, half), half), :]
        far_ref[base:, :] = hid[pl.ds(pl.multiple_of((1 - where_ref[1]) * half, half), half), :]
        line = jnp.concatenate([top, total, acc[1:2, :], jnp.zeros((1, tokens), F32)], axis=0)
        stats_ref[...] = jnp.broadcast_to(line[None], stats_ref.shape)


def logits_call(where, targets, got, table, copies):
    count, width = table.shape
    tokens = got.shape[2]
    span = 2048 + width // 2
    return pl.pallas_call(
        logits_kernel,
        grid_spec=pltpu.PrefetchScalarGridSpec(
            num_scalar_prefetch=1,
            grid=(count // CHUNK,),
            in_specs=[
                pl.BlockSpec((1, tokens), lambda i, s: (0, 0)),
                pl.BlockSpec(got.shape, lambda i, s: (0, 0, 0)),
                pl.BlockSpec((CHUNK, width), lambda i, s: (i, 0)),
            ],
            out_specs=[
                pl.BlockSpec((span, tokens), lambda i, s: (0, 0)),
                pl.BlockSpec((span, tokens), lambda i, s: (0, 0)),
                pl.BlockSpec((copies, 4, tokens), lambda i, s: (0, 0, 0)),
            ],
            scratch_shapes=[
                pltpu.VMEM((width, tokens), BF16),
                pltpu.VMEM((count, tokens), F32),
                pltpu.VMEM((8, tokens), F32),
            ],
        ),
        out_shape=[
            jax.ShapeDtypeStruct((span, tokens), BF16),
            jax.ShapeDtypeStruct((span, tokens), BF16),
            jax.ShapeDtypeStruct((copies, 4, tokens), F32),
        ],
        compiler_params=PARAMS,
        cost_estimate=cost(2 * count * width * tokens, 2 * count * width + 4 * span * tokens),
        name="logits",
    )(where, targets, got, table)


def part_kernel(where_ref, tgt_ref, e_ref, table_ref, soft_ref, hard_ref, lhs):
    tokens = tgt_ref.shape[1]
    count = table_ref.shape[0]

    @pl.when(pl.program_id(0) == 0)
    def _():
        index = lax.broadcasted_iota(I32, (count, tokens), 0) + where_ref[0]
        hit = jnp.where(index == tgt_ref[...], 1.0, 0.0).astype(BF16)
        lhs[0:tokens, :] = e_ref[...].T
        lhs[tokens:, :] = hit.T

    both = jnp.dot(lhs[...], table_ref[...], preferred_element_type=F32)
    soft = both[0:tokens, :].T
    hard = both[tokens:, :].T
    for k in range(soft.shape[0] // 32):
        z, x = k // 2, k % 2
        soft_ref[x, z * 32 : z * 32 + 32, :] = soft[k * 32 : k * 32 + 32, :]
        hard_ref[x, z * 32 : z * 32 + 32, :] = hard[k * 32 : k * 32 + 32, :].astype(BF16)


def part_call(where, targets, near, table):
    count, width = table.shape
    tokens = targets.shape[1]
    wide = 256
    spec = pl.BlockSpec((2, wide // 2, tokens), lambda j, s: (j // 2, j % 2, 0))
    return pl.pallas_call(
        part_kernel,
        grid_spec=pltpu.PrefetchScalarGridSpec(
            num_scalar_prefetch=1,
            grid=(width // wide,),
            in_specs=[
                pl.BlockSpec((1, tokens), lambda j, s: (0, 0)),
                pl.BlockSpec((count, tokens), lambda j, s: (0, 0)),
                pl.BlockSpec((count, wide), lambda j, s: (0, j)),
            ],
            out_specs=[spec, spec],
            scratch_shapes=[pltpu.VMEM((2 * tokens, count), BF16)],
        ),
        out_shape=[
            jax.ShapeDtypeStruct((8, width // 8, tokens), F32),
            jax.ShapeDtypeStruct((8, width // 8, tokens), BF16),
        ],
        compiler_params=PARAMS,
        cost_estimate=cost(4 * count * width * tokens, 2 * count * width + 6 * width * tokens),
        name="part",
    )(where, targets, near, table)


def scale_kernel(where_ref, tgt_ref, own_ref, stats_ref, soft_ref, hard_ref, out_ref, loss_ref, w_ref, keep):
    @pl.when(pl.program_id(0) == 0)
    def _():
        stats = stats_ref[...]
        peak = jnp.max(stats, axis=0)
        top = peak[0:1, :]
        sums = jnp.sum(stats[:, 1:2, :] * jnp.exp(stats[:, 0:1, :] - top[None]), axis=0)
        picks = jnp.sum(stats, axis=0)[2:3, :]
        loss_ref[...] = top + jnp.log(sums) - picks
        local_top, local_pick = own_ref[0, 0:1, :], own_ref[0, 2:3, :]
        w = jnp.exp(local_top - top) / sums
        prob = jnp.exp(local_pick - top) / sums
        soft = jnp.exp(local_pick - local_top).astype(BF16).astype(F32) * w
        gap = (prob - 1.0).astype(BF16).astype(F32) - soft
        keep[0:1, :] = w
        keep[1:2, :] = gap
        w_ref[...] = jnp.concatenate(
            [w, tgt_ref[...].astype(F32), jnp.zeros((6, w.shape[1]), F32)], axis=0
        )

    out_ref[...] = (
        soft_ref[...] * keep[0:1, :][None] + hard_ref[...].astype(F32) * keep[1:2, :][None]
    ).astype(BF16)


def scale_call(where, targets, own, stats, soft, hard):
    plane, depth, tokens = soft.shape
    spec = pl.BlockSpec((2, depth, tokens), lambda p, s: (p, 0, 0))
    return pl.pallas_call(
        scale_kernel,
        grid_spec=pltpu.PrefetchScalarGridSpec(
            num_scalar_prefetch=1,
            grid=(plane // 2,),
            in_specs=[
                pl.BlockSpec((1, tokens), lambda p, s: (0, 0)),
                pl.BlockSpec((1, 4, tokens), lambda p, s: (0, 0, 0)),
                pl.BlockSpec(stats.shape, lambda p, s: (0, 0, 0)),
                spec,
                spec,
            ],
            out_specs=[
                spec,
                pl.BlockSpec((1, tokens), lambda p, s: (0, 0)),
                pl.BlockSpec((8, tokens), lambda p, s: (0, 0)),
            ],
            scratch_shapes=[pltpu.VMEM((8, tokens), F32)],
        ),
        out_shape=[
            jax.ShapeDtypeStruct((plane, depth, tokens), BF16),
            jax.ShapeDtypeStruct((1, tokens), F32),
            jax.ShapeDtypeStruct((8, tokens), F32),
        ],
        compiler_params=PARAMS,
        cost_estimate=cost(4 * plane * depth * tokens, 8 * plane * depth * tokens),
        name="scale",
    )(where, targets, own, stats, soft, hard)


def table_kernel(where_ref, w_ref, place_ref, rows_ref, *refs):
    out_ref = refs[-1]
    count = out_ref.shape[0]
    first = pl.program_id(0) * count
    near = lax.broadcasted_iota(I32, (count, 256), 0) + (first + where_ref[0])
    spots = lax.broadcasted_iota(I32, (count, place_ref.shape[1]), 0) + first
    match = jnp.where(spots == place_ref[...], 1.0, 0.0).astype(BF16)
    total = jnp.dot(match, rows_ref[...], preferred_element_type=F32)
    for g in range(4):
        e = refs[2 * g][...].astype(F32)
        w = w_ref[g, 0:1, :]
        target = w_ref[g, 1:2, :].astype(I32)
        res = (e * w - jnp.where(near == target, 1.0, 0.0)).astype(BF16)
        total += lax.dot_general(
            res, refs[2 * g + 1][...], (((1,), (1,)), ((), ())), preferred_element_type=F32
        )
    out_ref[...] = total.astype(BF16)


def table_call(where, w, place, rows, packs, count):
    tokens = packs[0].shape[1]
    block = rows.shape[1]
    specs, operands = [], []
    for pack in packs:
        specs.append(pl.BlockSpec((CHUNK, tokens), lambda i, s: (i, 0)))
        specs.append(pl.BlockSpec((block, tokens), lambda i, s: (4 + s[2], 0)))
        operands += [pack, pack]
    return pl.pallas_call(
        table_kernel,
        grid_spec=pltpu.PrefetchScalarGridSpec(
            num_scalar_prefetch=1,
            grid=(count // CHUNK,),
            in_specs=[
                pl.BlockSpec(w.shape, lambda i, s: (0, 0, 0)),
                pl.BlockSpec(place.shape, lambda i, s: (0, 0)),
                pl.BlockSpec((rows.shape[0], block), lambda i, s: (0, 0)),
                *specs,
            ],
            out_specs=pl.BlockSpec((CHUNK, block), lambda i, s: (i, 0)),
        ),
        out_shape=jax.ShapeDtypeStruct((count, block), BF16),
        compiler_params=PARAMS,
        cost_estimate=cost(2 * count * block * 1536, 8 * count * 256 + 2 * count * block),
        name="table_grad",
    )(where, w, place, rows, *operands)


def inner(hidden, table, targets, input_ids, cotangent):
    vocab_rows, width = table.shape
    ny, nz, nx = (lax.axis_size(a) for a in VOCAB)
    plane = ny * nx
    vocab_count = plane * nz
    block = width // lax.axis_size(DP)
    xh, c = lax.axis_index("xh"), lax.axis_index("c")
    where = jnp.stack([lax.axis_index(VOCAB) * vocab_rows, xh, c, lax.axis_index("z")]).astype(I32)
    tokens = hidden.shape[0]
    goal = targets.reshape(1, tokens)

    half = width // 2
    near_rows = lax.dynamic_slice_in_dim(cotangent, xh * half, half, 1)
    far_rows = lax.dynamic_slice_in_dim(cotangent, (1 - xh) * half, half, 1)
    far_rows = swap(far_rows, "xh")
    ids = input_ids.reshape(1, -1)
    ids = jnp.concatenate([ids, swap(ids, "c")], axis=0)
    ids = jnp.concatenate([ids, swap(ids, "xh")], axis=0)
    packs = (near_rows, swap(near_rows, "c"), far_rows, swap(far_rows, "c"))
    turns = select_call(where, ids, packs, vocab_rows)

    mine = hidden.T
    stage = exchange(to_each(mine, nz), "z").reshape(-1, tokens)
    stage, *turns = lax.optimization_barrier((stage, *turns))
    stage = exchange(to_each(stage, plane), PLANE)
    turns = [shift(turn, "z", k) if k else turn for k, turn in enumerate(turns)]
    mixed = regroup_call(turns)
    stage, mixed = lax.optimization_barrier((stage, mixed))
    got = exchange(mixed, PLANE)
    near, far, own = logits_call(where, goal, stage, table, vocab_count)
    own, got = lax.optimization_barrier((own, got))

    stats = exchange(own, VOCAB)
    far = swap(far, "xh")
    near_sib = swap(near, "c")
    far_sib = swap(far, "c")
    soft, hard = part_call(where, goal, near, table)
    part, loss, w = scale_call(where, goal, own, stats, soft, hard)

    part = exchange(part, PLANE)
    part = jnp.sum(part.astype(F32), axis=0).reshape(nz, -1, tokens)
    part = jnp.sum(exchange(part, "z"), axis=0)
    hidden_grad = part.astype(BF16).T

    w_near = jnp.stack([w, swap(w, "c")])
    w_all = jnp.concatenate([w_near, swap(w_near, "xh")], axis=0)
    code = got[:, -8:, :128].astype(F32).reshape(plane, 8, nz, 2, plane)
    spot = lax.axis_index("y") * nx + lax.axis_index("xl")
    here = lax.broadcasted_iota(I32, code.shape, 4) == spot
    code = jnp.sum(jnp.where(here, code, 0.0), axis=4)
    place = (code[..., 0] * 64 + code[..., 1]).astype(I32) - 1
    place = place.transpose(0, 2, 1).reshape(plane, -1)
    place = jnp.concatenate([place, jnp.full((plane, 8), -1, I32)], axis=1).reshape(1, -1)
    table_grad = table_call(
        where, w_all, place, got.reshape(-1, block), (near, near_sib, far, far_sib), vocab_rows
    )
    return loss.reshape(tokens), hidden_grad, table_grad


def solution(mesh):
    fine = Mesh(mesh.devices.reshape(2, 2, 4, 8, 2), ALL)
    placed = (P(DP, VOCAB), P(VOCAB, None), P(DP), P(ALL), P(ALL, None))
    return jax.shard_map(
        inner,
        mesh=fine,
        in_specs=placed,
        out_specs=(P(DP), P(DP, VOCAB), P(VOCAB, DP)),
        check_vma=False,
    )
```

```python
import functools

import jax
import jax.numpy as jnp
from jax import lax
from jax.experimental import pallas as pl
from jax.experimental.pallas import tpu as pltpu
from jax.sharding import Mesh, PartitionSpec as P

BF16 = jnp.bfloat16
F32 = jnp.float32
I32 = jnp.int32
ALL = ("xh", "c", "y", "z", "xl")
DP = ("xh", "c")
VOCAB = ("y", "z", "xl")
PLANE = ("y", "xl")
CHUNK = 400
PARAMS = pltpu.CompilerParams(vmem_limit_bytes=16 * 1024 * 1024)


def exchange(pieces, axes):
    return lax.all_to_all(pieces, axes, 0, 0, tiled=True)


def to_each(value, count):
    return jnp.broadcast_to(value, (count, *value.shape))


def swap(value, axis):
    return lax.ppermute(value, axis, [(0, 1), (1, 0)])


def cost(flops, moved, special=0):
    return pl.CostEstimate(flops=flops, bytes_accessed=moved, transcendentals=special)


def partner(value, bit):
    size = lax.axis_size("z")
    return lax.ppermute(value, "z", [(i, i ^ bit) for i in range(size)])


def join_kernel(cuts, *refs):
    out, at = refs[-1], 0
    for ref, (first, size) in zip(refs, cuts):
        out[at : at + size, :] = ref[first : first + size, :]
        at += size


def join_call(*parts):
    cuts = tuple((first, size) for _, first, size in parts)
    shape = (sum(size for _, size in cuts), parts[0][0].shape[1])
    return pl.pallas_call(
        functools.partial(join_kernel, cuts),
        out_shape=jax.ShapeDtypeStruct(shape, BF16),
        compiler_params=PARAMS,
        cost_estimate=cost(10**6, 2**19),
        name="join",
    )(*(array for array, _, _ in parts))


def select_kernel(vocab_rows, where_ref, *refs):
    packs = refs[:4]
    outs = refs[4:]
    count = packs[0].shape[0] - 8
    total = 4 * count
    line = jnp.concatenate(
        [
            p[count : count + 8, 0:128].astype(F32)[:, 0:count]
            for p in packs
        ],
        axis=1,
    )
    line = line[0:1, :] * 16384.0 + line[1:2, :] * 128.0 + line[2:3, :]
    tall = jnp.broadcast_to(line, (8, total)).T[:, 0:1]

    def parts(ids):
        owner = jnp.floor((ids + 0.5) * (1.0 / vocab_rows))
        spot = (ids - owner * vocab_rows).astype(I32) + 1
        owner = owner.astype(I32)
        plane = (owner >> 4) * 2 + (owner & 1)
        turn = ((owner >> 1) & 7) ^ where_ref[3]
        return owner, plane, turn, spot

    owner, plane, turn, _ = parts(line)
    owner_t, plane_t, turn_t, spot_t = parts(tall)
    early = lax.broadcasted_iota(I32, (total, total), 0)
    later = lax.broadcasted_iota(I32, (total, total), 1)
    before = (owner_t == owner) & (early < later) & ((early >> 6) == (later >> 6))
    rank = jnp.sum(jnp.where(before, 1.0, 0.0), axis=0, keepdims=True).astype(I32)
    token = lax.broadcasted_iota(I32, (1, total), 1)
    row = (token >> 6) * 2 + rank
    slots = turn * 64 + plane * 8 + row
    chosen = lax.broadcasted_iota(I32, (512, total), 0) == slots
    cot = jnp.concatenate([p[0:count, :] for p in packs], axis=0)
    picked = jnp.dot(jnp.where(chosen, 1.0, 0.0).astype(BF16), cot, preferred_element_type=F32)
    lane = lax.broadcasted_iota(I32, (total, 128), 1)
    base = turn_t * 16 + plane_t
    digits = jnp.where(lane == base, spot_t >> 6, jnp.where(lane == base + 8, spot_t & 63, 0))
    mark = lax.broadcasted_iota(I32, (16, total), 0) == row
    code = jnp.dot(
        jnp.where(mark, 1.0, 0.0).astype(BF16),
        digits.astype(F32).astype(BF16),
        preferred_element_type=F32,
    )
    code = jnp.concatenate([code, jnp.zeros((16, 128), F32)], axis=1).astype(BF16)
    far, middle, one, own, mine = outs
    for q in range(8):
        out, at = ((own, 0), (one, 0), (middle, 0), (middle, 128))[q] if q < 4 else (far, (q - 4) * 128)
        for p in range(8):
            piece = picked[q * 64 + p * 8 : q * 64 + p * 8 + 8, :]
            piece = jnp.concatenate([piece[:, 0:256], piece[:, 256:512]], axis=0)
            out[at + p * 16 : at + p * 16 + 16, :] = piece.astype(BF16)
    far[512:528, :] = code
    mine[...] = code


def select_call(where, packs, vocab_rows):
    rows, wide = packs[0].shape
    block = wide // 2
    sizes = (528, 256, 128, 128, 16)
    return pl.pallas_call(
        functools.partial(select_kernel, vocab_rows),
        grid_spec=pltpu.PrefetchScalarGridSpec(
            num_scalar_prefetch=1,
            grid=(1,),
            in_specs=[pl.BlockSpec((rows, block), lambda i, s: (0, s[2]))] * 4,
            out_specs=[pl.BlockSpec((n, 256), lambda i, s: (0, 0)) for n in sizes],
        ),
        out_shape=[jax.ShapeDtypeStruct((n, 256), BF16) for n in sizes],
        compiler_params=PARAMS,
        cost_estimate=cost(2 * 512 * 256 * block, 2**20),
        name="select",
    )(where, *packs)


def logits_kernel(where_ref, tgt_ref, got_ref, table_ref, near_ref, far_ref, stats_ref, hid, log, acc):
    step = pl.program_id(0)
    rows, tokens = table_ref.shape[0], hid.shape[1]
    width = hid.shape[0]
    half = width // 2

    @pl.when(step == 0)
    def _():
        plane, depth, _ = got_ref.shape
        nz = depth // 32
        nx = 2
        for p in range(plane):
            y, x = p // nx, p % nx
            for z in range(nz):
                at = ((y * nz + z) * nx + x) * 32
                hid[at : at + 32, :] = got_ref[p, z * 32 : z * 32 + 32, :]
        acc[0:1, :] = jnp.full((1, tokens), -jnp.inf, F32)
        acc[1:2, :] = jnp.zeros((1, tokens), F32)

    values = jnp.dot(table_ref[...], hid[...], preferred_element_type=F32)
    log[pl.ds(pl.multiple_of(step * rows, rows), rows), :] = values
    index = lax.broadcasted_iota(I32, values.shape, 0) + (where_ref[0] + step * rows)
    acc[1:2, :] += jnp.sum(jnp.where(index == tgt_ref[...], values, 0.0), axis=0, keepdims=True)
    acc[0:1, :] = jnp.maximum(acc[0:1, :], jnp.max(values, axis=0, keepdims=True))

    @pl.when(step == pl.num_programs(0) - 1)
    def _():
        top = acc[0:1, :]
        piece = 80

        def one(i, total):
            at = pl.ds(pl.multiple_of(i * piece, piece), piece)
            e = jnp.exp(log[at, :] - top)
            near_ref[at, :] = e.astype(BF16)
            far_ref[at, :] = e.astype(BF16)
            return total + jnp.sum(e, axis=0, keepdims=True)

        count = log.shape[0]
        total = lax.fori_loop(0, count // piece, one, jnp.zeros((1, tokens), F32))
        base = near_ref.shape[0] - half
        near_ref[count:base, :] = jnp.zeros((base - count, tokens), BF16)
        far_ref[count:base, :] = jnp.zeros((base - count, tokens), BF16)
        near_ref[base:, :] = hid[pl.ds(pl.multiple_of(where_ref[1] * half, half), half), :]
        far_ref[base:, :] = hid[pl.ds(pl.multiple_of((1 - where_ref[1]) * half, half), half), :]
        line = jnp.concatenate([top, total, acc[1:2, :], jnp.zeros((1, tokens), F32)], axis=0)
        stats_ref[...] = jnp.broadcast_to(line[None], stats_ref.shape)


def logits_call(where, targets, got, table, copies):
    count, width = table.shape
    tokens = got.shape[2]
    span = 2048 + width // 2
    return pl.pallas_call(
        logits_kernel,
        grid_spec=pltpu.PrefetchScalarGridSpec(
            num_scalar_prefetch=1,
            grid=(count // CHUNK,),
            in_specs=[
                pl.BlockSpec((1, tokens), lambda i, s: (0, 0)),
                pl.BlockSpec(got.shape, lambda i, s: (0, 0, 0)),
                pl.BlockSpec((CHUNK, width), lambda i, s: (i, 0)),
            ],
            out_specs=[
                pl.BlockSpec((span, tokens), lambda i, s: (0, 0)),
                pl.BlockSpec((span, tokens), lambda i, s: (0, 0)),
                pl.BlockSpec((copies, 4, tokens), lambda i, s: (0, 0, 0)),
            ],
            scratch_shapes=[
                pltpu.VMEM((width, tokens), BF16),
                pltpu.VMEM((count, tokens), F32),
                pltpu.VMEM((8, tokens), F32),
            ],
        ),
        out_shape=[
            jax.ShapeDtypeStruct((span, tokens), BF16),
            jax.ShapeDtypeStruct((span, tokens), BF16),
            jax.ShapeDtypeStruct((copies, 4, tokens), F32),
        ],
        compiler_params=PARAMS,
        cost_estimate=cost(2 * count * width * tokens, 2 * count * width + 4 * span * tokens),
        name="logits",
    )(where, targets, got, table)


def part_kernel(where_ref, tgt_ref, e_ref, table_ref, soft_ref, hard_ref, lhs):
    tokens = tgt_ref.shape[1]
    count = table_ref.shape[0]

    @pl.when(pl.program_id(0) == 0)
    def _():
        index = lax.broadcasted_iota(I32, (count, tokens), 0) + where_ref[0]
        hit = jnp.where(index == tgt_ref[...], 1.0, 0.0).astype(BF16)
        lhs[0:tokens, :] = e_ref[...].T
        lhs[tokens:, :] = hit.T

    both = jnp.dot(lhs[...], table_ref[...], preferred_element_type=F32)
    soft = both[0:tokens, :].T
    hard = both[tokens:, :].T
    for k in range(soft.shape[0] // 32):
        z, x = k // 2, k % 2
        soft_ref[x, z * 32 : z * 32 + 32, :] = soft[k * 32 : k * 32 + 32, :]
        hard_ref[x, z * 32 : z * 32 + 32, :] = hard[k * 32 : k * 32 + 32, :].astype(BF16)


def part_call(where, targets, near, table):
    count, width = table.shape
    tokens = targets.shape[1]
    wide = 256
    spec = pl.BlockSpec((2, wide // 2, tokens), lambda j, s: (j // 2, j % 2, 0))
    return pl.pallas_call(
        part_kernel,
        grid_spec=pltpu.PrefetchScalarGridSpec(
            num_scalar_prefetch=1,
            grid=(width // wide,),
            in_specs=[
                pl.BlockSpec((1, tokens), lambda j, s: (0, 0)),
                pl.BlockSpec((count, tokens), lambda j, s: (0, 0)),
                pl.BlockSpec((count, wide), lambda j, s: (0, j)),
            ],
            out_specs=[spec, spec],
            scratch_shapes=[pltpu.VMEM((2 * tokens, count), BF16)],
        ),
        out_shape=[
            jax.ShapeDtypeStruct((8, width // 8, tokens), F32),
            jax.ShapeDtypeStruct((8, width // 8, tokens), BF16),
        ],
        compiler_params=PARAMS,
        cost_estimate=cost(4 * count * width * tokens, 2 * count * width + 6 * width * tokens),
        name="part",
    )(where, targets, near, table)


QUOTA = (0, 4, 2, 6, 1, 5, 3, 7)


def scale_kernel(
    where_ref, tgt_ref, own_ref, stats_ref, soft_ref, hard_ref, x0, r1, r2, r3, c0,
    out_ref, loss_ref, w_ref, keep, code,
):
    step = pl.program_id(0)

    @pl.when(pl.program_id(0) == 0)
    def _():
        stats = stats_ref[...]
        peak = jnp.max(stats, axis=0)
        top = peak[0:1, :]
        sums = jnp.sum(stats[:, 1:2, :] * jnp.exp(stats[:, 0:1, :] - top[None]), axis=0)
        picks = jnp.sum(stats, axis=0)[2:3, :]
        loss_ref[...] = top + jnp.log(sums) - picks
        local_top, local_pick = own_ref[0, 0:1, :], own_ref[0, 2:3, :]
        w = jnp.exp(local_top - top) / sums
        prob = jnp.exp(local_pick - top) / sums
        soft = jnp.exp(local_pick - local_top).astype(BF16).astype(F32) * w
        gap = (prob - 1.0).astype(BF16).astype(F32) - soft
        keep[0:1, :] = w
        keep[1:2, :] = gap
        w_ref[...] = jnp.concatenate(
            [w, tgt_ref[...].astype(F32), jnp.zeros((6, w.shape[1]), F32)], axis=0
        )

        marks = [c0[...], r1[512:528, :], r2[512:528, :], r2[528:544, :]]
        marks += [r3[k : k + 16, :] for k in range(512, 576, 16)]
        group = lax.broadcasted_iota(I32, (16, 256), 1) >> 4
        mixed = jnp.zeros((16, 256), F32)
        for q, mark in zip(QUOTA, marks):
            mixed += jnp.where(group == q, mark.astype(F32), 0.0)
        code[...] = mixed.astype(BF16)

    depth = soft_ref.shape[1]
    out_ref[:, 0:depth, :] = (
        soft_ref[...] * keep[0:1, :][None] + hard_ref[...].astype(F32) * keep[1:2, :][None]
    ).astype(BF16)
    pieces = ((x0, 0), (r1, 0), (r2, 0), (r2, 256), (r3, 0), (r3, 128), (r3, 256), (r3, 384))
    for j in range(2):
        for i, (ref, at) in enumerate(pieces):
            from_row = pl.multiple_of((2 * step + j) * 16 + at, 16)
            out_ref[j, depth + 16 * i : depth + 16 * i + 16, :] = ref[pl.ds(from_row, 16), :]
        out_ref[j, depth + 128 : depth + 144, :] = code[...]


def scale_call(where, targets, own, stats, soft, hard, riders):
    plane, depth, tokens = soft.shape
    spec = pl.BlockSpec((2, depth, tokens), lambda p, s: (p, 0, 0))
    return pl.pallas_call(
        scale_kernel,
        grid_spec=pltpu.PrefetchScalarGridSpec(
            num_scalar_prefetch=1,
            grid=(plane // 2,),
            in_specs=[
                pl.BlockSpec((1, tokens), lambda p, s: (0, 0)),
                pl.BlockSpec((1, 4, tokens), lambda p, s: (0, 0, 0)),
                pl.BlockSpec(stats.shape, lambda p, s: (0, 0, 0)),
                spec,
                spec,
                *[pl.BlockSpec(rider.shape, lambda p, s: (0, 0)) for rider in riders],
            ],
            out_specs=[
                pl.BlockSpec((2, depth + 144, tokens), lambda p, s: (p, 0, 0)),
                pl.BlockSpec((1, tokens), lambda p, s: (0, 0)),
                pl.BlockSpec((8, tokens), lambda p, s: (0, 0)),
            ],
            scratch_shapes=[pltpu.VMEM((8, tokens), F32), pltpu.VMEM((16, tokens), BF16)],
        ),
        out_shape=[
            jax.ShapeDtypeStruct((plane, depth + 144, tokens), BF16),
            jax.ShapeDtypeStruct((1, tokens), F32),
            jax.ShapeDtypeStruct((8, tokens), F32),
        ],
        compiler_params=PARAMS,
        cost_estimate=cost(4 * plane * depth * tokens, 8 * plane * depth * tokens),
        name="scale",
    )(where, targets, own, stats, soft, hard, *riders)


def table_kernel(where_ref, w_ref, got_ref, *refs):
    out_ref, rows, place = refs[-3:]
    count = out_ref.shape[0]
    first = pl.program_id(0) * count

    @pl.when(pl.program_id(0) == 0)
    def _():
        plane = got_ref.shape[0]
        depth = got_ref.shape[1] - 144
        slots = rows.shape[0]
        mark = lax.broadcasted_iota(I32, (128, slots), 0)
        lane = lax.broadcasted_iota(I32, (128, slots), 1)
        i = (lane >> 3) & 7
        quota = ((i & 1) << 2) | (i & 2) | ((i >> 2) & 1)
        at = quota * 16 + where_ref[4]
        digit = jnp.where(mark == at, 64.0, jnp.where(mark == at + 8, 1.0, 0.0))
        found = jnp.zeros((16, slots), F32)
        for p in range(plane):
            for k in range(0, 8, 2):
                a = got_ref[p, depth + 16 * k : depth + 16 * k + 16, :].astype(F32)
                b = got_ref[p, depth + 16 * k + 16 : depth + 16 * k + 32, :].astype(F32)
                to = p * 64 + k * 8
                rows[to : to + 16, 0:256] = jnp.concatenate([a[0:8], b[0:8]], axis=0).astype(BF16)
                rows[to : to + 16, 256:512] = jnp.concatenate([a[8:16], b[8:16]], axis=0).astype(BF16)
            code = got_ref[p, depth + 128 : depth + 144, 0:128]
            these = jnp.where((lane >> 6) == p, digit, 0.0).astype(BF16)
            found += jnp.dot(code, these, preferred_element_type=F32)
        mine = lax.broadcasted_iota(I32, (16, slots), 0) == (
            lax.broadcasted_iota(I32, (16, slots), 1) & 7
        )
        spot = jnp.sum(jnp.where(mine, found, 0.0), axis=0, keepdims=True) - 1.0
        place[...] = jnp.broadcast_to(spot, place.shape).astype(I32)

    near = lax.broadcasted_iota(I32, (count, 256), 0) + (first + where_ref[0])
    spots = lax.broadcasted_iota(I32, (count, place.shape[1]), 0) + first
    match = jnp.where(spots == place[0:1, :], 1.0, 0.0).astype(BF16)
    total = jnp.dot(match, rows[...], preferred_element_type=F32)
    for g in range(4):
        e = refs[2 * g][...].astype(F32)
        w = w_ref[g, 0:1, :]
        target = w_ref[g, 1:2, :].astype(I32)
        res = (e * w - jnp.where(near == target, 1.0, 0.0)).astype(BF16)
        total += lax.dot_general(
            res, refs[2 * g + 1][...], (((1,), (1,)), ((), ())), preferred_element_type=F32
        )
    out_ref[...] = total.astype(BF16)


def table_call(where, w, got, packs, count):
    tokens = packs[0].shape[1]
    block = 512
    specs, operands = [], []
    for pack in packs:
        specs.append(pl.BlockSpec((CHUNK, tokens), lambda i, s: (i, 0)))
        specs.append(pl.BlockSpec((block, tokens), lambda i, s: (4 + s[2], 0)))
        operands += [pack, pack]
    return pl.pallas_call(
        table_kernel,
        grid_spec=pltpu.PrefetchScalarGridSpec(
            num_scalar_prefetch=1,
            grid=(count // CHUNK,),
            in_specs=[
                pl.BlockSpec(w.shape, lambda i, s: (0, 0, 0)),
                pl.BlockSpec(got.shape, lambda i, s: (0, 0, 0)),
                *specs,
            ],
            out_specs=pl.BlockSpec((CHUNK, block), lambda i, s: (i, 0)),
            scratch_shapes=[pltpu.VMEM((512, block), BF16), pltpu.VMEM((8, 512), I32)],
        ),
        out_shape=jax.ShapeDtypeStruct((count, block), BF16),
        compiler_params=PARAMS,
        cost_estimate=cost(2 * count * block * 1536, 8 * count * 256 + 2 * count * block),
        name="table_grad",
    )(where, w, got, *operands)


def inner(hidden, table, targets, input_ids, cotangent):
    vocab_rows, width = table.shape
    ny, nz, nx = (lax.axis_size(a) for a in VOCAB)
    plane = ny * nx
    vocab_count = plane * nz
    block = width // lax.axis_size(DP)
    xh, c = lax.axis_index("xh"), lax.axis_index("c")
    spot = lax.axis_index("y") * nx + lax.axis_index("xl")
    where = jnp.stack([lax.axis_index(VOCAB) * vocab_rows, xh, c, lax.axis_index("z"), spot]).astype(I32)
    tokens = hidden.shape[0]
    goal = targets.reshape(1, tokens)

    half = width // 2
    ids = jnp.stack([input_ids >> 14, (input_ids >> 7) & 127, input_ids & 127]).astype(BF16)
    ids = jnp.pad(ids, ((0, 5), (0, block - ids.shape[1])))
    ids = jnp.concatenate([ids, ids], axis=1)
    near_rows = lax.dynamic_slice_in_dim(cotangent, xh * half, half, 1)
    far_rows = lax.dynamic_slice_in_dim(cotangent, (1 - xh) * half, half, 1)
    near_rows = jnp.concatenate([near_rows, ids], axis=0)
    far_rows = swap(jnp.concatenate([far_rows, ids], axis=0), "xh")
    packs = (near_rows, swap(near_rows, "c"), far_rows, swap(far_rows, "c"))
    away, middle, one, x0, c0 = select_call(where, packs, vocab_rows)
    r1 = partner(away, 4)
    r2 = partner(join_call((middle, 0, 256), (r1, 256, 256), (c0, 0, 16), (r1, 512, 16)), 2)
    r3 = join_call(
        (one, 0, 128), (r1, 128, 128), (r2, 128, 128), (r2, 384, 128), (c0, 0, 16), (r1, 512, 16), (r2, 512, 32)
    )
    r3 = partner(r3, 1)

    mine = hidden.T
    stage = exchange(to_each(mine, nz), "z").reshape(-1, tokens)
    stage = exchange(to_each(stage, plane), PLANE)
    near, far, own = logits_call(where, goal, stage, table, vocab_count)

    stats = exchange(own, VOCAB)
    far = swap(far, "xh")
    near_sib = swap(near, "c")
    far_sib = swap(far, "c")
    soft, hard = part_call(where, goal, near, table)
    part, loss, w = scale_call(where, goal, own, stats, soft, hard, (x0, r1, r2, r3, c0))

    got = exchange(part, PLANE)
    part = jnp.sum(got[:, : width // plane].astype(F32), axis=0).reshape(nz, -1, tokens)
    part = jnp.sum(exchange(part, "z"), axis=0)
    hidden_grad = part.astype(BF16).T

    w_near = jnp.stack([w, swap(w, "c")])
    w_all = jnp.concatenate([w_near, swap(w_near, "xh")], axis=0)
    table_grad = table_call(
        where, w_all, got, (near, near_sib, far, far_sib), vocab_rows
    )
    return loss.reshape(tokens), hidden_grad, table_grad


def solution(mesh):
    fine = Mesh(mesh.devices.reshape(2, 2, 4, 8, 2), ALL)
    placed = (P(DP, VOCAB), P(VOCAB, None), P(DP), P(ALL), P(ALL, None))
    return jax.shard_map(
        inner,
        mesh=fine,
        in_specs=placed,
        out_specs=(P(DP), P(DP, VOCAB), P(VOCAB, DP)),
        check_vma=False,
    )
```

```python
import functools

import jax
import jax.numpy as jnp
from jax import lax
from jax.experimental import pallas as pl
from jax.experimental.pallas import tpu as pltpu
from jax.sharding import Mesh, PartitionSpec as P

BF16 = jnp.bfloat16
F32 = jnp.float32
I32 = jnp.int32
ALL = ("xh", "c", "y", "z", "xl")
DP = ("xh", "c")
VOCAB = ("y", "z", "xl")
PLANE = ("y", "xl")
CHUNK = 400
PARAMS = pltpu.CompilerParams(vmem_limit_bytes=60 * 1024 * 1024)


def exchange(pieces, axes):
    return lax.all_to_all(pieces, axes, 0, 0, tiled=True)


def to_each(value, count):
    return jnp.broadcast_to(value, (count, *value.shape))


def swap(value, axis):
    return lax.ppermute(value, axis, [(0, 1), (1, 0)])


def cost(flops, moved, special=0):
    return pl.CostEstimate(flops=flops, bytes_accessed=moved, transcendentals=special)


def partner(value, bit):
    size = lax.axis_size("z")
    return lax.ppermute(value, "z", [(i, i ^ bit) for i in range(size)])


def join_kernel(cuts, *refs):
    out, at = refs[-1], 0
    for ref, (first, size) in zip(refs, cuts):
        out[at : at + size, :] = ref[first : first + size, :]
        at += size


def join_call(*parts):
    cuts = tuple((first, size) for _, first, size in parts)
    shape = (sum(size for _, size in cuts), parts[0][0].shape[1])
    return pl.pallas_call(
        functools.partial(join_kernel, cuts),
        out_shape=jax.ShapeDtypeStruct(shape, BF16),
        compiler_params=PARAMS,
        cost_estimate=cost(10**6, 2**19),
        name="join",
    )(*(array for array, _, _ in parts))


def select_kernel(vocab_rows, where_ref, *refs):
    packs = refs[:4]
    outs = refs[4:]
    count = packs[0].shape[0] - 8
    total = 4 * count
    line = jnp.concatenate(
        [
            p[count : count + 8, 0:128].astype(F32)[:, 0:count]
            for p in packs
        ],
        axis=1,
    )
    line = line[0:1, :] * 16384.0 + line[1:2, :] * 128.0 + line[2:3, :]
    tall = jnp.broadcast_to(line, (8, total)).T[:, 0:1]

    def parts(ids):
        owner = jnp.floor((ids + 0.5) * (1.0 / vocab_rows))
        spot = (ids - owner * vocab_rows).astype(I32) + 1
        owner = owner.astype(I32)
        plane = (owner >> 4) * 2 + (owner & 1)
        turn = ((owner >> 1) & 7) ^ where_ref[3]
        return owner, plane, turn, spot

    owner, plane, turn, _ = parts(line)
    owner_t, plane_t, turn_t, spot_t = parts(tall)
    early = lax.broadcasted_iota(I32, (total, total), 0)
    later = lax.broadcasted_iota(I32, (total, total), 1)
    before = (owner_t == owner) & (early < later) & ((early >> 6) == (later >> 6))
    rank = jnp.sum(jnp.where(before, 1.0, 0.0), axis=0, keepdims=True).astype(I32)
    token = lax.broadcasted_iota(I32, (1, total), 1)
    row = (token >> 6) * 2 + rank
    slots = turn * 64 + plane * 8 + row
    chosen = lax.broadcasted_iota(I32, (512, total), 0) == slots
    cot = jnp.concatenate([p[0:count, :] for p in packs], axis=0)
    picked = jnp.dot(jnp.where(chosen, 1.0, 0.0).astype(BF16), cot, preferred_element_type=F32)
    lane = lax.broadcasted_iota(I32, (total, 128), 1)
    base = turn_t * 16 + plane_t
    digits = jnp.where(lane == base, spot_t >> 6, jnp.where(lane == base + 8, spot_t & 63, 0))
    mark = lax.broadcasted_iota(I32, (16, total), 0) == row
    code = jnp.dot(
        jnp.where(mark, 1.0, 0.0).astype(BF16),
        digits.astype(F32).astype(BF16),
        preferred_element_type=F32,
    )
    code = jnp.concatenate([code, jnp.zeros((16, 128), F32)], axis=1).astype(BF16)
    far, middle, one, own, mine = outs
    for q in range(8):
        out, at = ((own, 0), (one, 0), (middle, 0), (middle, 128))[q] if q < 4 else (far, (q - 4) * 128)
        for p in range(8):
            piece = picked[q * 64 + p * 8 : q * 64 + p * 8 + 8, :]
            piece = jnp.concatenate([piece[:, 0:256], piece[:, 256:512]], axis=0)
            out[at + p * 16 : at + p * 16 + 16, :] = piece.astype(BF16)
    far[512:528, :] = code
    mine[...] = code


def select_call(where, packs, vocab_rows):
    rows, wide = packs[0].shape
    block = wide // 2
    sizes = (528, 256, 128, 128, 16)
    return pl.pallas_call(
        functools.partial(select_kernel, vocab_rows),
        grid_spec=pltpu.PrefetchScalarGridSpec(
            num_scalar_prefetch=1,
            grid=(1,),
            in_specs=[pl.BlockSpec((rows, block), lambda i, s: (0, s[2]))] * 4,
            out_specs=[pl.BlockSpec((n, 256), lambda i, s: (0, 0)) for n in sizes],
        ),
        out_shape=[jax.ShapeDtypeStruct((n, 256), BF16) for n in sizes],
        compiler_params=PARAMS,
        cost_estimate=cost(2 * 512 * 256 * block, 2**20),
        name="select",
    )(where, *packs)


def logits_kernel(where_ref, tgt_ref, got_ref, table_ref, near_ref, far_ref, stats_ref, hid, log, acc):
    step = pl.program_id(0)
    rows, tokens = table_ref.shape[0], hid.shape[1]
    width = hid.shape[0]
    half = width // 2

    @pl.when(step == 0)
    def _():
        plane, depth, _ = got_ref.shape
        nz = depth // 32
        nx = 2
        for p in range(plane):
            y, x = p // nx, p % nx
            for z in range(nz):
                at = ((y * nz + z) * nx + x) * 32
                hid[at : at + 32, :] = got_ref[p, z * 32 : z * 32 + 32, :]
        acc[0:1, :] = jnp.full((1, tokens), -jnp.inf, F32)
        acc[1:2, :] = jnp.zeros((1, tokens), F32)

    values = jnp.dot(table_ref[...], hid[...], preferred_element_type=F32)
    log[pl.ds(pl.multiple_of(step * rows, rows), rows), :] = values
    index = lax.broadcasted_iota(I32, values.shape, 0) + (where_ref[0] + step * rows)
    acc[1:2, :] += jnp.sum(jnp.where(index == tgt_ref[...], values, 0.0), axis=0, keepdims=True)
    acc[0:1, :] = jnp.maximum(acc[0:1, :], jnp.max(values, axis=0, keepdims=True))

    @pl.when(step == pl.num_programs(0) - 1)
    def _():
        top = acc[0:1, :]
        piece = 80

        def one(i, total):
            at = pl.ds(pl.multiple_of(i * piece, piece), piece)
            e = jnp.exp(log[at, :] - top)
            near_ref[at, :] = e.astype(BF16)
            far_ref[at, :] = e.astype(BF16)
            return total + jnp.sum(e, axis=0, keepdims=True)

        count = log.shape[0]
        total = lax.fori_loop(0, count // piece, one, jnp.zeros((1, tokens), F32))
        base = near_ref.shape[0] - half
        near_ref[count:base, :] = jnp.zeros((base - count, tokens), BF16)
        far_ref[count:base, :] = jnp.zeros((base - count, tokens), BF16)
        near_ref[base:, :] = hid[pl.ds(pl.multiple_of(where_ref[1] * half, half), half), :]
        far_ref[base:, :] = hid[pl.ds(pl.multiple_of((1 - where_ref[1]) * half, half), half), :]
        line = jnp.concatenate([top, total, acc[1:2, :], jnp.zeros((1, tokens), F32)], axis=0)
        stats_ref[...] = jnp.broadcast_to(line[None], stats_ref.shape)


def logits_call(where, targets, got, table, copies):
    count, width = table.shape
    tokens = got.shape[2]
    span = 2048 + width // 2
    return pl.pallas_call(
        logits_kernel,
        grid_spec=pltpu.PrefetchScalarGridSpec(
            num_scalar_prefetch=1,
            grid=(count // CHUNK,),
            in_specs=[
                pl.BlockSpec((1, tokens), lambda i, s: (0, 0)),
                pl.BlockSpec(got.shape, lambda i, s: (0, 0, 0)),
                pl.BlockSpec((CHUNK, width), lambda i, s: (i, 0)),
            ],
            out_specs=[
                pl.BlockSpec((span, tokens), lambda i, s: (0, 0)),
                pl.BlockSpec((span, tokens), lambda i, s: (0, 0)),
                pl.BlockSpec((copies, 4, tokens), lambda i, s: (0, 0, 0)),
            ],
            scratch_shapes=[
                pltpu.VMEM((width, tokens), BF16),
                pltpu.VMEM((count, tokens), F32),
                pltpu.VMEM((8, tokens), F32),
            ],
        ),
        out_shape=[
            jax.ShapeDtypeStruct((span, tokens), BF16),
            jax.ShapeDtypeStruct((span, tokens), BF16),
            jax.ShapeDtypeStruct((copies, 4, tokens), F32),
        ],
        compiler_params=PARAMS,
        cost_estimate=cost(2 * count * width * tokens, 2 * count * width + 4 * span * tokens),
        name="logits",
    )(where, targets, got, table)


def part_kernel(hot, where_ref, side_ref, table_ref, out_ref, lhs):
    tokens = out_ref.shape[2]
    count = table_ref.shape[0]

    @pl.when(pl.program_id(0) == 0)
    def _():
        if hot:
            index = lax.broadcasted_iota(I32, (count, tokens), 0) + where_ref[0]
            lhs[...] = jnp.where(index == side_ref[...], 1.0, 0.0).astype(BF16).T
        else:
            lhs[...] = side_ref[...].T

    part = jnp.dot(lhs[...], table_ref[...], preferred_element_type=F32).T
    for k in range(part.shape[0] // 32):
        z, x = k // 2, k % 2
        out_ref[x, z * 32 : z * 32 + 32, :] = part[k * 32 : k * 32 + 32, :].astype(out_ref.dtype)


def part_call(hot, where, side, table):
    count, width = table.shape
    tokens = side.shape[1]
    wide = 256
    return pl.pallas_call(
        functools.partial(part_kernel, hot),
        grid_spec=pltpu.PrefetchScalarGridSpec(
            num_scalar_prefetch=1,
            grid=(width // wide,),
            in_specs=[
                pl.BlockSpec((1 if hot else count, tokens), lambda j, s: (0, 0)),
                pl.BlockSpec((count, wide), lambda j, s: (0, j)),
            ],
            out_specs=pl.BlockSpec((2, wide // 2, tokens), lambda j, s: (j // 2, j % 2, 0)),
            scratch_shapes=[pltpu.VMEM((tokens, count), BF16)],
        ),
        out_shape=jax.ShapeDtypeStruct((8, width // 8, tokens), BF16 if hot else F32),
        compiler_params=PARAMS,
        cost_estimate=cost(2 * count * width * tokens, 2 * count * width + 4 * width * tokens),
        name="hard" if hot else "soft",
    )(where, side, table)


QUOTA = (0, 4, 2, 6, 1, 5, 3, 7)


def scale_kernel(
    where_ref, tgt_ref, own_ref, stats_ref, soft_ref, hard_ref, x0, r1, r2, r3, c0,
    out_ref, loss_ref, w_ref, keep, code,
):
    step = pl.program_id(0)

    @pl.when(pl.program_id(0) == 0)
    def _():
        stats = stats_ref[...]
        peak = jnp.max(stats, axis=0)
        top = peak[0:1, :]
        sums = jnp.sum(stats[:, 1:2, :] * jnp.exp(stats[:, 0:1, :] - top[None]), axis=0)
        picks = jnp.sum(stats, axis=0)[2:3, :]
        loss_ref[...] = top + jnp.log(sums) - picks
        local_top, local_pick = own_ref[0, 0:1, :], own_ref[0, 2:3, :]
        w = jnp.exp(local_top - top) / sums
        prob = jnp.exp(local_pick - top) / sums
        soft = jnp.exp(local_pick - local_top).astype(BF16).astype(F32) * w
        gap = (prob - 1.0).astype(BF16).astype(F32) - soft
        keep[0:1, :] = w
        keep[1:2, :] = gap
        w_ref[...] = jnp.concatenate(
            [w, tgt_ref[...].astype(F32), jnp.zeros((6, w.shape[1]), F32)], axis=0
        )

        marks = [c0[...], r1[512:528, :], r2[512:528, :], r2[528:544, :]]
        marks += [r3[k : k + 16, :] for k in range(512, 576, 16)]
        group = lax.broadcasted_iota(I32, (16, 256), 1) >> 4
        mixed = jnp.zeros((16, 256), F32)
        for q, mark in zip(QUOTA, marks):
            mixed += jnp.where(group == q, mark.astype(F32), 0.0)
        code[...] = mixed.astype(BF16)

    depth = soft_ref.shape[1]
    out_ref[:, 0:depth, :] = (
        soft_ref[...] * keep[0:1, :][None] + hard_ref[...].astype(F32) * keep[1:2, :][None]
    ).astype(BF16)
    pieces = ((x0, 0), (r1, 0), (r2, 0), (r2, 256), (r3, 0), (r3, 128), (r3, 256), (r3, 384))
    for j in range(2):
        for i, (ref, at) in enumerate(pieces):
            from_row = pl.multiple_of((2 * step + j) * 16 + at, 16)
            out_ref[j, depth + 16 * i : depth + 16 * i + 16, :] = ref[pl.ds(from_row, 16), :]
        out_ref[j, depth + 128 : depth + 144, :] = code[...]


def scale_call(where, targets, own, stats, soft, hard, riders):
    plane, depth, tokens = soft.shape
    spec = pl.BlockSpec((2, depth, tokens), lambda p, s: (p, 0, 0))
    return pl.pallas_call(
        scale_kernel,
        grid_spec=pltpu.PrefetchScalarGridSpec(
            num_scalar_prefetch=1,
            grid=(plane // 2,),
            in_specs=[
                pl.BlockSpec((1, tokens), lambda p, s: (0, 0)),
                pl.BlockSpec((1, 4, tokens), lambda p, s: (0, 0, 0)),
                pl.BlockSpec(stats.shape, lambda p, s: (0, 0, 0)),
                spec,
                spec,
                *[pl.BlockSpec(rider.shape, lambda p, s: (0, 0)) for rider in riders],
            ],
            out_specs=[
                pl.BlockSpec((2, depth + 144, tokens), lambda p, s: (p, 0, 0)),
                pl.BlockSpec((1, tokens), lambda p, s: (0, 0)),
                pl.BlockSpec((8, tokens), lambda p, s: (0, 0)),
            ],
            scratch_shapes=[pltpu.VMEM((8, tokens), F32), pltpu.VMEM((16, tokens), BF16)],
        ),
        out_shape=[
            jax.ShapeDtypeStruct((plane, depth + 144, tokens), BF16),
            jax.ShapeDtypeStruct((1, tokens), F32),
            jax.ShapeDtypeStruct((8, tokens), F32),
        ],
        compiler_params=PARAMS,
        cost_estimate=cost(4 * plane * depth * tokens, 8 * plane * depth * tokens),
        name="scale",
    )(where, targets, own, stats, soft, hard, *riders)


def table_kernel(where_ref, w_ref, got_ref, *refs):
    out_ref, rows, place = refs[-3:]
    count = out_ref.shape[0]
    first = pl.program_id(0) * count

    @pl.when(pl.program_id(0) == 0)
    def _():
        plane = got_ref.shape[0]
        depth = got_ref.shape[1] - 144
        slots = rows.shape[0]
        mark = lax.broadcasted_iota(I32, (128, slots), 0)
        lane = lax.broadcasted_iota(I32, (128, slots), 1)
        i = (lane >> 3) & 7
        quota = ((i & 1) << 2) | (i & 2) | ((i >> 2) & 1)
        at = quota * 16 + where_ref[4]
        digit = jnp.where(mark == at, 64.0, jnp.where(mark == at + 8, 1.0, 0.0))
        found = jnp.zeros((16, slots), F32)
        for p in range(plane):
            for k in range(0, 8, 2):
                a = got_ref[p, depth + 16 * k : depth + 16 * k + 16, :].astype(F32)
                b = got_ref[p, depth + 16 * k + 16 : depth + 16 * k + 32, :].astype(F32)
                to = p * 64 + k * 8
                rows[to : to + 16, 0:256] = jnp.concatenate([a[0:8], b[0:8]], axis=0).astype(BF16)
                rows[to : to + 16, 256:512] = jnp.concatenate([a[8:16], b[8:16]], axis=0).astype(BF16)
            code = got_ref[p, depth + 128 : depth + 144, 0:128]
            these = jnp.where((lane >> 6) == p, digit, 0.0).astype(BF16)
            found += jnp.dot(code, these, preferred_element_type=F32)
        mine = lax.broadcasted_iota(I32, (16, slots), 0) == (
            lax.broadcasted_iota(I32, (16, slots), 1) & 7
        )
        spot = jnp.sum(jnp.where(mine, found, 0.0), axis=0, keepdims=True) - 1.0
        place[...] = jnp.broadcast_to(spot, place.shape).astype(I32)

    near = lax.broadcasted_iota(I32, (count, 256), 0) + (first + where_ref[0])
    spots = lax.broadcasted_iota(I32, (count, place.shape[1]), 0) + first
    match = jnp.where(spots == place[0:1, :], 1.0, 0.0).astype(BF16)
    total = jnp.dot(match, rows[...], preferred_element_type=F32)
    for g in range(4):
        e = refs[2 * g][...].astype(F32)
        w = w_ref[g, 0:1, :]
        target = w_ref[g, 1:2, :].astype(I32)
        res = (e * w - jnp.where(near == target, 1.0, 0.0)).astype(BF16)
        total += lax.dot_general(
            res, refs[2 * g + 1][...], (((1,), (1,)), ((), ())), preferred_element_type=F32
        )
    out_ref[...] = total.astype(BF16)


def table_call(where, w, got, packs, count):
    tokens = packs[0].shape[1]
    block = 512
    specs, operands = [], []
    for pack in packs:
        specs.append(pl.BlockSpec((CHUNK, tokens), lambda i, s: (i, 0)))
        specs.append(pl.BlockSpec((block, tokens), lambda i, s: (4 + s[2], 0)))
        operands += [pack, pack]
    return pl.pallas_call(
        table_kernel,
        grid_spec=pltpu.PrefetchScalarGridSpec(
            num_scalar_prefetch=1,
            grid=(count // CHUNK,),
            in_specs=[
                pl.BlockSpec(w.shape, lambda i, s: (0, 0, 0)),
                pl.BlockSpec(got.shape, lambda i, s: (0, 0, 0)),
                *specs,
            ],
            out_specs=pl.BlockSpec((CHUNK, block), lambda i, s: (i, 0)),
            scratch_shapes=[pltpu.VMEM((512, block), BF16), pltpu.VMEM((8, 512), I32)],
        ),
        out_shape=jax.ShapeDtypeStruct((count, block), BF16),
        compiler_params=PARAMS,
        cost_estimate=cost(2 * count * block * 1536, 8 * count * 256 + 2 * count * block),
        name="table_grad",
    )(where, w, got, *operands)


def inner(hidden, table, targets, input_ids, cotangent):
    vocab_rows, width = table.shape
    ny, nz, nx = (lax.axis_size(a) for a in VOCAB)
    plane = ny * nx
    vocab_count = plane * nz
    block = width // lax.axis_size(DP)
    xh, c = lax.axis_index("xh"), lax.axis_index("c")
    spot = lax.axis_index("y") * nx + lax.axis_index("xl")
    where = jnp.stack([lax.axis_index(VOCAB) * vocab_rows, xh, c, lax.axis_index("z"), spot]).astype(I32)
    tokens = hidden.shape[0]
    goal = targets.reshape(1, tokens)

    half = width // 2
    ids = jnp.stack([input_ids >> 14, (input_ids >> 7) & 127, input_ids & 127]).astype(BF16)
    ids = jnp.pad(ids, ((0, 5), (0, block - ids.shape[1])))
    ids = jnp.concatenate([ids, ids], axis=1)
    near_rows = lax.dynamic_slice_in_dim(cotangent, xh * half, half, 1)
    far_rows = lax.dynamic_slice_in_dim(cotangent, (1 - xh) * half, half, 1)
    near_rows = jnp.concatenate([near_rows, ids], axis=0)
    far_rows = swap(jnp.concatenate([far_rows, ids], axis=0), "xh")
    packs = (near_rows, swap(near_rows, "c"), far_rows, swap(far_rows, "c"))
    away, middle, one, x0, c0 = select_call(where, packs, vocab_rows)
    hard = part_call(True, where, goal, table)
    r1 = partner(away, 4)
    r2 = partner(join_call((middle, 0, 256), (r1, 256, 256), (c0, 0, 16), (r1, 512, 16)), 2)
    r3 = join_call(
        (one, 0, 128), (r1, 128, 128), (r2, 128, 128), (r2, 384, 128), (c0, 0, 16), (r1, 512, 16), (r2, 512, 32)
    )
    r3 = partner(r3, 1)

    mine = hidden.T
    stage = exchange(to_each(mine, nz), "z").reshape(-1, tokens)
    stage = exchange(to_each(stage, plane), PLANE)
    near, far, own = logits_call(where, goal, stage, table, vocab_count)

    stats = exchange(own, VOCAB)
    far = swap(far, "xh")
    near_sib = swap(near, "c")
    far_sib = swap(far, "c")
    soft = part_call(False, where, near, table)
    part, loss, w = scale_call(where, goal, own, stats, soft, hard, (x0, r1, r2, r3, c0))

    got = exchange(part, PLANE)
    part = jnp.sum(got[:, : width // plane].astype(F32), axis=0).reshape(nz, -1, tokens)
    part = jnp.sum(exchange(part, "z"), axis=0)
    hidden_grad = part.astype(BF16).T

    w_near = jnp.stack([w, swap(w, "c")])
    w_all = jnp.concatenate([w_near, swap(w_near, "xh")], axis=0)
    table_grad = table_call(
        where, w_all, got, (near, near_sib, far, far_sib), vocab_rows
    )
    return loss.reshape(tokens), hidden_grad, table_grad


def solution(mesh):
    fine = Mesh(mesh.devices.reshape(2, 2, 4, 8, 2), ALL)
    placed = (P(DP, VOCAB), P(VOCAB, None), P(DP), P(ALL), P(ALL, None))
    return jax.shard_map(
        inner,
        mesh=fine,
        in_specs=placed,
        out_specs=(P(DP), P(DP, VOCAB), P(VOCAB, DP)),
        check_vma=False,
    )
```

```python
import functools

import jax
import jax.numpy as jnp
from jax import lax
from jax.experimental import pallas as pl
from jax.experimental.pallas import tpu as pltpu
from jax.sharding import Mesh, PartitionSpec as P

BF16 = jnp.bfloat16
F32 = jnp.float32
I32 = jnp.int32
ALL = ("xh", "c", "y", "z", "xl")
DP = ("xh", "c")
VOCAB = ("y", "z", "xl")
PLANE = ("y", "xl")
CHUNK = 400
PARAMS = pltpu.CompilerParams(vmem_limit_bytes=16 * 1024 * 1024)
WIDE = pltpu.CompilerParams(vmem_limit_bytes=57 * 1024 * 1024)
FULL = pltpu.CompilerParams(vmem_limit_bytes=62 * 1024 * 1024)


def exchange(pieces, axes):
    return lax.all_to_all(pieces, axes, 0, 0, tiled=True)


def to_each(value, count):
    return jnp.broadcast_to(value, (count, *value.shape))


def swap(value, axis):
    return lax.ppermute(value, axis, [(0, 1), (1, 0)])


def cost(flops, moved, special=0):
    return pl.CostEstimate(flops=flops, bytes_accessed=moved, transcendentals=special)


def partner(value, bit):
    size = lax.axis_size("z")
    return lax.ppermute(value, "z", [(i, i ^ bit) for i in range(size)])


def join_kernel(cuts, *refs):
    out, at = refs[-1], 0
    for ref, (first, size) in zip(refs, cuts):
        out[at : at + size, :] = ref[first : first + size, :]
        at += size


def join_call(*parts):
    cuts = tuple((first, size) for _, first, size in parts)
    shape = (sum(size for _, size in cuts), parts[0][0].shape[1])
    return pl.pallas_call(
        functools.partial(join_kernel, cuts),
        out_shape=jax.ShapeDtypeStruct(shape, BF16),
        compiler_params=PARAMS,
        cost_estimate=cost(10**6, 2**19),
        name="join",
    )(*(array for array, _, _ in parts))


def select_kernel(vocab_rows, where_ref, *refs):
    packs = refs[:4]
    outs = refs[4:]
    count = packs[0].shape[0] - 8
    total = 4 * count
    line = jnp.concatenate(
        [
            p[count : count + 8, 0:128].astype(F32)[:, 0:count]
            for p in packs
        ],
        axis=1,
    )
    line = line[0:1, :] * 16384.0 + line[1:2, :] * 128.0 + line[2:3, :]
    tall = jnp.broadcast_to(line, (8, total)).T[:, 0:1]

    def parts(ids):
        owner = jnp.floor((ids + 0.5) * (1.0 / vocab_rows))
        spot = (ids - owner * vocab_rows).astype(I32) + 1
        owner = owner.astype(I32)
        plane = (owner >> 4) * 2 + (owner & 1)
        turn = ((owner >> 1) & 7) ^ where_ref[3]
        return owner, plane, turn, spot

    owner, plane, turn, _ = parts(line)
    owner_t, plane_t, turn_t, spot_t = parts(tall)
    early = lax.broadcasted_iota(I32, (total, total), 0)
    later = lax.broadcasted_iota(I32, (total, total), 1)
    before = (owner_t == owner) & (early < later) & ((early >> 6) == (later >> 6))
    rank = jnp.sum(jnp.where(before, 1.0, 0.0), axis=0, keepdims=True).astype(I32)
    token = lax.broadcasted_iota(I32, (1, total), 1)
    row = (token >> 6) * 2 + rank
    slots = turn * 64 + plane * 8 + row
    chosen = lax.broadcasted_iota(I32, (512, total), 0) == slots
    cot = jnp.concatenate([p[0:count, :] for p in packs], axis=0)
    picked = jnp.dot(jnp.where(chosen, 1.0, 0.0).astype(BF16), cot, preferred_element_type=F32)
    lane = lax.broadcasted_iota(I32, (total, 128), 1)
    base = turn_t * 16 + plane_t
    digits = jnp.where(lane == base, spot_t >> 6, jnp.where(lane == base + 8, spot_t & 63, 0))
    mark = lax.broadcasted_iota(I32, (16, total), 0) == row
    code = jnp.dot(
        jnp.where(mark, 1.0, 0.0).astype(BF16),
        digits.astype(F32).astype(BF16),
        preferred_element_type=F32,
    )
    code = jnp.concatenate([code, jnp.zeros((16, 128), F32)], axis=1).astype(BF16)
    far, middle, one, own, mine = outs
    for q in range(8):
        out, at = ((own, 0), (one, 0), (middle, 0), (middle, 128))[q] if q < 4 else (far, (q - 4) * 128)
        for p in range(8):
            piece = picked[q * 64 + p * 8 : q * 64 + p * 8 + 8, :]
            piece = jnp.concatenate([piece[:, 0:256], piece[:, 256:512]], axis=0)
            out[at + p * 16 : at + p * 16 + 16, :] = piece.astype(BF16)
    far[512:528, :] = code
    mine[...] = code


def select_call(where, packs, vocab_rows):
    rows, wide = packs[0].shape
    block = wide // 2
    sizes = (528, 256, 128, 128, 16)
    return pl.pallas_call(
        functools.partial(select_kernel, vocab_rows),
        grid_spec=pltpu.PrefetchScalarGridSpec(
            num_scalar_prefetch=1,
            grid=(1,),
            in_specs=[pl.BlockSpec((rows, block), lambda i, s: (0, s[2]))] * 4,
            out_specs=[pl.BlockSpec((n, 256), lambda i, s: (0, 0)) for n in sizes],
        ),
        out_shape=[jax.ShapeDtypeStruct((n, 256), BF16) for n in sizes],
        compiler_params=PARAMS,
        cost_estimate=cost(2 * 512 * 256 * block, 2**20),
        name="select",
    )(where, *packs)


def logits_kernel(where_ref, tgt_ref, got_ref, table_ref, pack_ref, stats_ref, hid, log, tab, sems):
    count, tokens = log.shape
    half = hid.shape[0] // 2
    plane, depth, _ = got_ref.shape
    loads = []
    for i in range(count // CHUNK):
        at = pl.ds(i * CHUNK, CHUNK)
        loads.append(pltpu.make_async_copy(table_ref.at[at], tab.at[at], sems.at[i]))
        loads[i].start()
    for p in range(plane):
        y, x = p // 2, p % 2
        for z in range(depth // 32):
            at = ((y * (depth // 32) + z) * 2 + x) * 32
            hid[at : at + 32, :] = got_ref[p, z * 32 : z * 32 + 32, :]
    top = jnp.full((1, tokens), -jnp.inf, F32)
    picked = jnp.zeros((1, tokens), F32)
    for i, load in enumerate(loads):
        load.wait()
        values = jnp.dot(tab[i * CHUNK : (i + 1) * CHUNK, :], hid[...], preferred_element_type=F32)
        log[i * CHUNK : (i + 1) * CHUNK, :] = values
        index = lax.broadcasted_iota(I32, values.shape, 0) + (where_ref[0] + i * CHUNK)
        picked += jnp.sum(jnp.where(index == tgt_ref[...], values, 0.0), axis=0, keepdims=True)
        top = jnp.maximum(top, jnp.max(values, axis=0, keepdims=True))
    piece = 80

    def one(i, total):
        at = pl.ds(pl.multiple_of(i * piece, piece), piece)
        e = jnp.exp(log[at, :] - top)
        pack_ref[at, :] = e.astype(BF16)
        return total + jnp.sum(e, axis=0, keepdims=True)

    total = lax.fori_loop(0, count // piece, one, jnp.zeros((1, tokens), F32))
    base = pack_ref.shape[0] - half
    pack_ref[count:base, :] = jnp.zeros((base - count, tokens), BF16)
    pack_ref[base:, :] = hid[pl.ds(pl.multiple_of(where_ref[1] * half, half), half), :]
    line = jnp.concatenate([top, total, picked, jnp.zeros((1, tokens), F32)], axis=0)
    stats_ref[...] = jnp.broadcast_to(line[None], stats_ref.shape)


def logits_call(where, targets, got, table, copies):
    count, width = table.shape
    tokens = got.shape[2]
    span = 2048 + width // 2
    whole = pl.BlockSpec(memory_space=pltpu.VMEM)
    return pl.pallas_call(
        logits_kernel,
        in_specs=[pl.BlockSpec(memory_space=pltpu.SMEM), whole, whole, pl.BlockSpec(memory_space=pl.ANY)],
        out_specs=[whole, whole],
        scratch_shapes=[
            pltpu.VMEM((width, tokens), BF16),
            pltpu.VMEM((count, tokens), F32),
            pltpu.VMEM((count, width), BF16),
            pltpu.SemaphoreType.DMA((count // CHUNK,)),
        ],
        out_shape=[
            jax.ShapeDtypeStruct((span, tokens), BF16),
            jax.ShapeDtypeStruct((copies, 4, tokens), F32),
        ],
        compiler_params=WIDE,
        cost_estimate=cost(2 * count * width * tokens, 2 * count * width + 4 * span * tokens),
        name="logits",
    )(where, targets, got, table)


QUOTA = (0, 4, 2, 6, 1, 5, 3, 7)


def part_kernel(
    where_ref, tgt_ref, own_ref, stats_ref, near_ref, x0, r1, r2, r3, c0, table_ref,
    out_ref, loss_ref, w_ref, lhs, tab, buf, sems, out_sems,
):
    tokens = tgt_ref.shape[1]
    count, width = table_ref.shape
    plane = buf.shape[0]
    depth = width // plane
    wide = tab.shape[2]
    loads = []
    for j in range(width // wide):
        at = table_ref.at[:, pl.ds(j * wide, wide)]
        loads.append(pltpu.make_async_copy(at, tab.at[j], sems.at[j]))
        loads[j].start()

    stats = stats_ref[...]
    top = jnp.max(stats, axis=0)[0:1, :]
    sums = jnp.sum(stats[:, 1:2, :] * jnp.exp(stats[:, 0:1, :] - top[None]), axis=0)
    picks = jnp.sum(stats, axis=0)[2:3, :]
    loss_ref[...] = top + jnp.log(sums) - picks
    w = jnp.exp(own_ref[0, 0:1, :] - top) / sums
    w_ref[...] = jnp.concatenate([w, tgt_ref[...].astype(F32), jnp.zeros((6, tokens), F32)], axis=0)
    for i in range(0, count, CHUNK):
        index = lax.broadcasted_iota(I32, (CHUNK, tokens), 0) + (where_ref[0] + i)
        e = near_ref[i : i + CHUNK, :].astype(F32)
        residual = e * w - jnp.where(index == tgt_ref[...], 1.0, 0.0)
        lhs[i : i + CHUNK, :] = residual.astype(BF16)
    rows = lhs[...].T

    marks = [c0[...], r1[512:528, :], r2[512:528, :], r2[528:544, :]]
    marks += [r3[k : k + 16, :] for k in range(512, 576, 16)]
    group = lax.broadcasted_iota(I32, (16, tokens), 1) >> 4
    mixed = jnp.zeros((16, tokens), F32)
    for q, mark in zip(QUOTA, marks):
        mixed += jnp.where(group == q, mark.astype(F32), 0.0)
    pieces = ((x0, 0), (r1, 0), (r2, 0), (r2, 256), (r3, 0), (r3, 128), (r3, 256), (r3, 384))
    for p in range(plane):
        for i, (ref, at) in enumerate(pieces):
            to = depth + 16 * i
            buf[p, to : to + 16, :] = ref[at + p * 16 : at + p * 16 + 16, :]
        buf[p, depth + 128 : depth + 144, :] = mixed.astype(BF16)

    stores = []
    for j, load in enumerate(loads):
        load.wait()
        part = jnp.dot(rows, tab[j], preferred_element_type=F32).T
        for k in range(wide // 32):
            z, x = k // 2, k % 2
            at = (j % 2) * 128 + z * 32
            buf[j // 2 * 2 + x, at : at + 32, :] = part[k * 32 : k * 32 + 32, :].astype(BF16)
        if j % 2:
            at = pl.ds(j // 2 * 2, 2)
            stores.append(pltpu.make_async_copy(buf.at[at], out_ref.at[at], out_sems.at[j // 2]))
            stores[-1].start()
    for store in stores:
        store.wait()


def part_call(where, targets, own, stats, near, riders, table):
    count, width = table.shape
    tokens = targets.shape[1]
    plane, wide = 8, 256
    whole = pl.BlockSpec(memory_space=pltpu.VMEM)
    anywhere = pl.BlockSpec(memory_space=pl.ANY)
    shape = (plane, width // plane + 144, tokens)
    return pl.pallas_call(
        part_kernel,
        in_specs=[pl.BlockSpec(memory_space=pltpu.SMEM), *[whole] * 9, anywhere],
        out_specs=[anywhere, whole, whole],
        scratch_shapes=[
            pltpu.VMEM((count, tokens), BF16),
            pltpu.VMEM((width // wide, count, wide), BF16),
            pltpu.VMEM(shape, BF16),
            pltpu.SemaphoreType.DMA((width // wide,)),
            pltpu.SemaphoreType.DMA((plane // 2,)),
        ],
        out_shape=[
            jax.ShapeDtypeStruct(shape, BF16),
            jax.ShapeDtypeStruct((1, tokens), F32),
            jax.ShapeDtypeStruct((8, tokens), F32),
        ],
        compiler_params=FULL,
        cost_estimate=cost(2 * count * width * tokens, 2 * count * width + 2 * width * tokens),
        name="part",
    )(where, targets, own, stats, near, *riders, table)


def table_kernel(where_ref, w_ref, got_ref, *refs):
    out_ref, rows, place = refs[-3:]
    count = out_ref.shape[0]
    first = pl.program_id(0) * count

    @pl.when(pl.program_id(0) == 0)
    def _():
        plane = got_ref.shape[0]
        depth = got_ref.shape[1] - 144
        slots = rows.shape[0]
        mark = lax.broadcasted_iota(I32, (128, slots), 0)
        lane = lax.broadcasted_iota(I32, (128, slots), 1)
        i = (lane >> 3) & 7
        quota = ((i & 1) << 2) | (i & 2) | ((i >> 2) & 1)
        at = quota * 16 + where_ref[4]
        digit = jnp.where(mark == at, 64.0, jnp.where(mark == at + 8, 1.0, 0.0))
        found = jnp.zeros((16, slots), F32)
        for p in range(plane):
            for k in range(0, 8, 2):
                a = got_ref[p, depth + 16 * k : depth + 16 * k + 16, :].astype(F32)
                b = got_ref[p, depth + 16 * k + 16 : depth + 16 * k + 32, :].astype(F32)
                to = p * 64 + k * 8
                rows[to : to + 16, 0:256] = jnp.concatenate([a[0:8], b[0:8]], axis=0).astype(BF16)
                rows[to : to + 16, 256:512] = jnp.concatenate([a[8:16], b[8:16]], axis=0).astype(BF16)
            code = got_ref[p, depth + 128 : depth + 144, 0:128]
            these = jnp.where((lane >> 6) == p, digit, 0.0).astype(BF16)
            found += jnp.dot(code, these, preferred_element_type=F32)
        mine = lax.broadcasted_iota(I32, (16, slots), 0) == (
            lax.broadcasted_iota(I32, (16, slots), 1) & 7
        )
        spot = jnp.sum(jnp.where(mine, found, 0.0), axis=0, keepdims=True) - 1.0
        place[...] = jnp.broadcast_to(spot, place.shape).astype(I32)

    near = lax.broadcasted_iota(I32, (count, 256), 0) + (first + where_ref[0])
    spots = lax.broadcasted_iota(I32, (count, place.shape[1]), 0) + first
    match = jnp.where(spots == place[0:1, :], 1.0, 0.0).astype(BF16)
    total = jnp.dot(match, rows[...], preferred_element_type=F32)
    for g in range(4):
        e = refs[2 * g][...].astype(F32)
        w = w_ref[g, 0:1, :]
        target = w_ref[g, 1:2, :].astype(I32)
        res = (e * w - jnp.where(near == target, 1.0, 0.0)).astype(BF16)
        total += lax.dot_general(
            res, refs[2 * g + 1][...], (((1,), (1,)), ((), ())), preferred_element_type=F32
        )
    out_ref[...] = total.astype(BF16)


def table_call(where, w, got, packs, count):
    tokens = packs[0].shape[1]
    block = 512
    specs, operands = [], []
    for pack in packs:
        specs.append(pl.BlockSpec((CHUNK, tokens), lambda i, s: (i, 0)))
        specs.append(pl.BlockSpec((block, tokens), lambda i, s: (4 + s[2], 0)))
        operands += [pack, pack]
    return pl.pallas_call(
        table_kernel,
        grid_spec=pltpu.PrefetchScalarGridSpec(
            num_scalar_prefetch=1,
            grid=(count // CHUNK,),
            in_specs=[
                pl.BlockSpec(w.shape, lambda i, s: (0, 0, 0)),
                pl.BlockSpec(got.shape, lambda i, s: (0, 0, 0)),
                *specs,
            ],
            out_specs=pl.BlockSpec((CHUNK, block), lambda i, s: (i, 0)),
            scratch_shapes=[pltpu.VMEM((512, block), BF16), pltpu.VMEM((8, 512), I32)],
        ),
        out_shape=jax.ShapeDtypeStruct((count, block), BF16),
        compiler_params=PARAMS,
        cost_estimate=cost(2 * count * block * 1536, 8 * count * 256 + 2 * count * block),
        name="table_grad",
    )(where, w, got, *operands)


def inner(hidden, table, targets, input_ids, cotangent):
    vocab_rows, width = table.shape
    ny, nz, nx = (lax.axis_size(a) for a in VOCAB)
    plane = ny * nx
    vocab_count = plane * nz
    block = width // lax.axis_size(DP)
    xh, c = lax.axis_index("xh"), lax.axis_index("c")
    spot = lax.axis_index("y") * nx + lax.axis_index("xl")
    where = jnp.stack([lax.axis_index(VOCAB) * vocab_rows, xh, c, lax.axis_index("z"), spot]).astype(I32)
    tokens = hidden.shape[0]
    goal = targets.reshape(1, tokens)

    half = width // 2
    ids = jnp.stack([input_ids >> 14, (input_ids >> 7) & 127, input_ids & 127]).astype(BF16)
    ids = jnp.pad(ids, ((0, 5), (0, block - ids.shape[1])))
    ids = jnp.concatenate([ids, ids], axis=1)
    near_rows = lax.dynamic_slice_in_dim(cotangent, xh * half, half, 1)
    far_rows = lax.dynamic_slice_in_dim(cotangent, (1 - xh) * half, half, 1)
    near_rows = jnp.concatenate([near_rows, ids], axis=0)
    far_rows = jnp.concatenate([far_rows, ids], axis=0)
    far_rows = swap(far_rows, "xh")
    packs = (near_rows, swap(near_rows, "c"), far_rows, swap(far_rows, "c"))
    away, middle, one, x0, c0 = select_call(where, packs, vocab_rows)
    r1 = partner(away, 4)
    r2 = partner(join_call((middle, 0, 256), (r1, 256, 256), (c0, 0, 16), (r1, 512, 16)), 2)
    r3 = join_call(
        (one, 0, 128), (r1, 128, 128), (r2, 128, 128), (r2, 384, 128), (c0, 0, 16), (r1, 512, 16), (r2, 512, 32)
    )
    r3 = partner(r3, 1)

    mine = hidden.T
    stage = exchange(to_each(mine, nz), "z").reshape(-1, tokens)
    stage = exchange(to_each(stage, plane), PLANE)
    far_stage = swap(stage, "xh")
    near, own = logits_call(where, goal, stage, table, vocab_count)

    stats = exchange(own, VOCAB)
    far, _ = logits_call(where, goal, far_stage, table, 1)
    near_sib = swap(near, "c")
    far_sib = swap(far, "c")
    part, loss, w = part_call(where, goal, own[0:1], stats, near, (x0, r1, r2, r3, c0), table)

    got = exchange(part, PLANE)
    part = jnp.sum(got[:, : width // plane].astype(F32), axis=0).reshape(nz, -1, tokens)
    part = jnp.sum(exchange(part, "z"), axis=0)
    hidden_grad = part.astype(BF16).T

    w_near = jnp.stack([w, swap(w, "c")])
    w_all = jnp.concatenate([w_near, swap(w_near, "xh")], axis=0)
    table_grad = table_call(
        where, w_all, got, (near, near_sib, far, far_sib), vocab_rows
    )
    return loss.reshape(tokens), hidden_grad, table_grad


def solution(mesh):
    fine = Mesh(mesh.devices.reshape(2, 2, 4, 8, 2), ALL)
    placed = (P(DP, VOCAB), P(VOCAB, None), P(DP), P(ALL), P(ALL, None))
    return jax.shard_map(
        inner,
        mesh=fine,
        in_specs=placed,
        out_specs=(P(DP), P(DP, VOCAB), P(VOCAB, DP)),
        check_vma=False,
    )
```

```python
import functools

import jax
import jax.numpy as jnp
from jax import lax
from jax.experimental import pallas as pl
from jax.experimental.pallas import tpu as pltpu
from jax.sharding import Mesh, PartitionSpec as P

BF16 = jnp.bfloat16
F32 = jnp.float32
I32 = jnp.int32
ALL = ("xh", "c", "y", "z", "xl")
DP = ("xh", "c")
VOCAB = ("y", "z", "xl")
PLANE = ("y", "xl")
CHUNK = 400
DEPTH = 3
PARAMS = pltpu.CompilerParams(vmem_limit_bytes=16 * 1024 * 1024)
WIDE = pltpu.CompilerParams(vmem_limit_bytes=57 * 1024 * 1024)
FULL = pltpu.CompilerParams(vmem_limit_bytes=62 * 1024 * 1024)


def exchange(pieces, axes):
    return lax.all_to_all(pieces, axes, 0, 0, tiled=True)


def to_each(value, count):
    return jnp.broadcast_to(value, (count, *value.shape))


def swap(value, axis):
    return lax.ppermute(value, axis, [(0, 1), (1, 0)])


def cost(flops, moved, special=0):
    return pl.CostEstimate(flops=flops, bytes_accessed=moved, transcendentals=special)


def partner(value, bit):
    size = lax.axis_size("z")
    return lax.ppermute(value, "z", [(i, i ^ bit) for i in range(size)])


def join_kernel(cuts, *refs):
    out, at = refs[-1], 0
    for ref, (first, size) in zip(refs, cuts):
        out[at : at + size, :] = ref[first : first + size, :]
        at += size


def join_call(*parts):
    cuts = tuple((first, size) for _, first, size in parts)
    shape = (sum(size for _, size in cuts), parts[0][0].shape[1])
    return pl.pallas_call(
        functools.partial(join_kernel, cuts),
        out_shape=jax.ShapeDtypeStruct(shape, BF16),
        compiler_params=PARAMS,
        cost_estimate=cost(10**6, 2**19),
        name="join",
    )(*(array for array, _, _ in parts))


def select_kernel(vocab_rows, where_ref, *refs):
    packs = refs[:4]
    outs = refs[4:]
    count = packs[0].shape[0] - 8
    total = 4 * count
    line = jnp.concatenate(
        [
            p[count : count + 8, 0:128].astype(F32)[:, 0:count]
            for p in packs
        ],
        axis=1,
    )
    line = line[0:1, :] * 16384.0 + line[1:2, :] * 128.0 + line[2:3, :]
    tall = jnp.broadcast_to(line, (8, total)).T[:, 0:1]

    def parts(ids):
        owner = jnp.floor((ids + 0.5) * (1.0 / vocab_rows))
        spot = (ids - owner * vocab_rows).astype(I32) + 1
        owner = owner.astype(I32)
        plane = (owner >> 4) * 2 + (owner & 1)
        turn = ((owner >> 1) & 7) ^ where_ref[3]
        return owner, plane, turn, spot

    owner, plane, turn, _ = parts(line)
    owner_t, plane_t, turn_t, spot_t = parts(tall)
    early = lax.broadcasted_iota(I32, (total, total), 0)
    later = lax.broadcasted_iota(I32, (total, total), 1)
    before = (owner_t == owner) & (early < later) & ((early >> 6) == (later >> 6))
    rank = jnp.sum(jnp.where(before, 1.0, 0.0), axis=0, keepdims=True).astype(I32)
    token = lax.broadcasted_iota(I32, (1, total), 1)
    row = (token >> 6) * 2 + rank
    slots = turn * 64 + plane * 8 + row
    chosen = lax.broadcasted_iota(I32, (512, total), 0) == slots
    cot = jnp.concatenate([p[0:count, :] for p in packs], axis=0)
    picked = jnp.dot(jnp.where(chosen, 1.0, 0.0).astype(BF16), cot, preferred_element_type=F32)
    lane = lax.broadcasted_iota(I32, (total, 128), 1)
    base = turn_t * 16 + plane_t
    digits = jnp.where(lane == base, spot_t >> 6, jnp.where(lane == base + 8, spot_t & 63, 0))
    mark = lax.broadcasted_iota(I32, (16, total), 0) == row
    code = jnp.dot(
        jnp.where(mark, 1.0, 0.0).astype(BF16),
        digits.astype(F32).astype(BF16),
        preferred_element_type=F32,
    )
    code = jnp.concatenate([code, jnp.zeros((16, 128), F32)], axis=1).astype(BF16)
    far, middle, one, own, mine = outs
    for q in range(8):
        out, at = ((own, 0), (one, 0), (middle, 0), (middle, 128))[q] if q < 4 else (far, (q - 4) * 128)
        for p in range(8):
            piece = picked[q * 64 + p * 8 : q * 64 + p * 8 + 8, :]
            piece = jnp.concatenate([piece[:, 0:256], piece[:, 256:512]], axis=0)
            out[at + p * 16 : at + p * 16 + 16, :] = piece.astype(BF16)
    far[512:528, :] = code
    mine[...] = code


def select_call(where, packs, vocab_rows):
    rows, wide = packs[0].shape
    block = wide // 2
    sizes = (528, 256, 128, 128, 16)
    return pl.pallas_call(
        functools.partial(select_kernel, vocab_rows),
        grid_spec=pltpu.PrefetchScalarGridSpec(
            num_scalar_prefetch=1,
            grid=(1,),
            in_specs=[pl.BlockSpec((rows, block), lambda i, s: (0, s[2]))] * 4,
            out_specs=[pl.BlockSpec((n, 256), lambda i, s: (0, 0)) for n in sizes],
        ),
        out_shape=[jax.ShapeDtypeStruct((n, 256), BF16) for n in sizes],
        compiler_params=PARAMS,
        cost_estimate=cost(2 * 512 * 256 * block, 2**20),
        name="select",
    )(where, *packs)


def logits_kernel(
    where_ref, tgt_ref, got_ref, table_ref, pack_ref, stats_ref, own_ref, hid, tab, buf, sems, out_sems
):
    count, width = tab.shape
    tokens = hid.shape[1]
    half = width // 2
    plane, depth, _ = got_ref.shape
    chunks = count // CHUNK

    def load(i):
        at = pl.ds(pl.multiple_of(i * CHUNK, CHUNK), CHUNK)
        return pltpu.make_async_copy(table_ref.at[at], tab.at[at], sems.at[i])

    def store(i):
        at = pl.ds(pl.multiple_of(i * CHUNK, CHUNK), CHUNK)
        return pltpu.make_async_copy(buf.at[at], pack_ref.at[at], out_sems.at[i])

    for i in range(DEPTH):
        load(i).start()
    for p in range(plane):
        y, x = p // 2, p % 2
        for z in range(depth // 32):
            at = ((y * (depth // 32) + z) * 2 + x) * 32
            hid[at : at + 32, :] = got_ref[p, z * 32 : z * 32 + 32, :]
    base = buf.shape[0] - half
    buf[base:, :] = hid[pl.ds(pl.multiple_of(where_ref[1] * half, half), half), :]
    at = pl.ds(base, half)
    side = pltpu.make_async_copy(buf.at[at], pack_ref.at[at], out_sems.at[chunks])
    side.start()
    own_ref[...] = jnp.zeros(own_ref.shape, F32)

    def one(i, carry):
        top, total, picked = carry
        load(i).wait()

        @pl.when(i + DEPTH < chunks)
        def _():
            load(i + DEPTH).start()

        at = pl.ds(pl.multiple_of(i * CHUNK, CHUNK), CHUNK)
        values = jnp.dot(tab[at, :], hid[...], preferred_element_type=F32)
        index = lax.broadcasted_iota(I32, values.shape, 0) + (where_ref[0] + i * CHUNK)
        picked += jnp.sum(jnp.where(index == tgt_ref[...], values, 0.0), axis=0, keepdims=True)
        peak = jnp.max(values, axis=0, keepdims=True)
        e = jnp.exp(values - peak)
        buf[at, :] = e.astype(BF16)
        store(i).start()
        own_ref[pl.ds(i, 1), :] = peak
        higher = jnp.maximum(top, peak)
        total = total * jnp.exp(top - higher)
        total += jnp.sum(e, axis=0, keepdims=True) * jnp.exp(peak - higher)
        return higher, total, picked

    blank = jnp.zeros((1, tokens), F32)
    start = (jnp.full((1, tokens), -jnp.inf, F32), blank, blank)
    line = jnp.concatenate([*lax.fori_loop(0, chunks, one, start), blank], axis=0)
    stats_ref[...] = jnp.broadcast_to(line[None], stats_ref.shape)
    side.wait()

    def end(i, carry):
        store(i).wait()
        return carry

    lax.fori_loop(0, chunks, end, 0)


def logits_call(where, targets, got, table, copies):
    count, width = table.shape
    tokens = got.shape[2]
    span = 2048 + width // 2
    whole = pl.BlockSpec(memory_space=pltpu.VMEM)
    return pl.pallas_call(
        logits_kernel,
        in_specs=[pl.BlockSpec(memory_space=pltpu.SMEM), whole, whole, pl.BlockSpec(memory_space=pl.ANY)],
        out_specs=[pl.BlockSpec(memory_space=pltpu.HBM), whole, whole],
        scratch_shapes=[
            pltpu.VMEM((width, tokens), BF16),
            pltpu.VMEM((count, width), BF16),
            pltpu.VMEM((span, tokens), BF16),
            pltpu.SemaphoreType.DMA((count // CHUNK,)),
            pltpu.SemaphoreType.DMA((count // CHUNK + 1,)),
        ],
        out_shape=[
            pltpu.HBM((span, tokens), BF16),
            jax.ShapeDtypeStruct((copies, 4, tokens), F32),
            jax.ShapeDtypeStruct((8, tokens), F32),
        ],
        compiler_params=WIDE,
        cost_estimate=cost(2 * count * width * tokens, 2 * count * width + 4 * span * tokens),
        name="logits",
    )(where, targets, got, table)


QUOTA = (0, 4, 2, 6, 1, 5, 3, 7)


def part_kernel(
    where_ref, tgt_ref, own_ref, stats_ref, near_ref, x0, r1, r2, r3, c0, table_ref,
    out_ref, loss_ref, w_ref, lhs, tab, buf, sems, out_sems,
):
    tokens = tgt_ref.shape[1]
    count, width = table_ref.shape
    plane = buf.shape[0]
    depth = width // plane
    turns, _, wide = tab.shape

    def load(j):
        at = table_ref.at[:, pl.ds(pl.multiple_of(j * wide, wide), wide)]
        return pltpu.make_async_copy(at, tab.at[j], sems.at[j])

    def store(j):
        at = pl.ds(j * 2, 2)
        return pltpu.make_async_copy(buf.at[at], out_ref.at[at], out_sems.at[j])

    for j in range(DEPTH):
        load(j).start()

    stats = stats_ref[...]
    top = jnp.max(stats, axis=0)[0:1, :]
    sums = jnp.sum(stats[:, 1:2, :] * jnp.exp(stats[:, 0:1, :] - top[None]), axis=0)
    picks = jnp.sum(stats, axis=0)[2:3, :]
    loss_ref[...] = top + jnp.log(sums) - picks
    chunks = count // CHUNK
    w = jnp.exp(own_ref[0:chunks, :] - top) / sums
    w_ref[...] = jnp.concatenate(
        [w, tgt_ref[...].astype(F32), jnp.zeros((7 - chunks, tokens), F32)], axis=0
    )
    for i in range(chunks):
        index = lax.broadcasted_iota(I32, (CHUNK, tokens), 0) + (where_ref[0] + i * CHUNK)
        e = near_ref[i * CHUNK : (i + 1) * CHUNK, :].astype(F32)
        residual = e * w[i : i + 1, :] - jnp.where(index == tgt_ref[...], 1.0, 0.0)
        lhs[i * CHUNK : (i + 1) * CHUNK, :] = residual.astype(BF16)

    marks = [c0[...], r1[512:528, :], r2[512:528, :], r2[528:544, :]]
    marks += [r3[k : k + 16, :] for k in range(512, 576, 16)]
    group = lax.broadcasted_iota(I32, (16, tokens), 1) >> 4
    mixed = jnp.zeros((16, tokens), F32)
    for q, mark in zip(QUOTA, marks):
        mixed += jnp.where(group == q, mark.astype(F32), 0.0)
    pieces = ((x0, 0), (r1, 0), (r2, 0), (r2, 256), (r3, 0), (r3, 128), (r3, 256), (r3, 384))
    for p in range(plane):
        for i, (ref, at) in enumerate(pieces):
            to = depth + 16 * i
            buf[p, to : to + 16, :] = ref[at + p * 16 : at + p * 16 + 16, :]
        buf[p, depth + 128 : depth + 144, :] = mixed.astype(BF16)

    def one(j, carry):
        load(j).wait()

        @pl.when(j + DEPTH < turns)
        def _():
            load(j + DEPTH).start()

        part = lax.dot_general(
            tab[j], lhs[...], (((0,), (0,)), ((), ())), preferred_element_type=F32
        )
        for k in range(wide // 32):
            z, x = k // 2, k % 2
            buf[j * 2 + x, z * 32 : z * 32 + 32, :] = part[k * 32 : k * 32 + 32, :].astype(BF16)
        store(j).start()
        return carry

    lax.fori_loop(0, turns, one, 0)

    def end(j, carry):
        store(j).wait()
        return carry

    lax.fori_loop(0, turns, end, 0)


def part_call(where, targets, own, stats, near, riders, table):
    count, width = table.shape
    tokens = targets.shape[1]
    plane, wide = 8, 512
    whole = pl.BlockSpec(memory_space=pltpu.VMEM)
    anywhere = pl.BlockSpec(memory_space=pl.ANY)
    shape = (plane, width // plane + 144, tokens)
    return pl.pallas_call(
        part_kernel,
        in_specs=[pl.BlockSpec(memory_space=pltpu.SMEM), *[whole] * 9, anywhere],
        out_specs=[pl.BlockSpec(memory_space=pltpu.HBM), whole, whole],
        scratch_shapes=[
            pltpu.VMEM((count, tokens), BF16),
            pltpu.VMEM((width // wide, count, wide), BF16),
            pltpu.VMEM(shape, BF16),
            pltpu.SemaphoreType.DMA((width // wide,)),
            pltpu.SemaphoreType.DMA((plane // 2,)),
        ],
        out_shape=[
            pltpu.HBM(shape, BF16),
            jax.ShapeDtypeStruct((1, tokens), F32),
            jax.ShapeDtypeStruct((8, tokens), F32),
        ],
        compiler_params=FULL,
        cost_estimate=cost(2 * count * width * tokens, 2 * count * width + 2 * width * tokens),
        name="part",
    )(where, targets, own, stats, near, *riders, table)


def table_kernel(where_ref, w_ref, got_ref, *refs):
    out_ref, rows, place = refs[-3:]
    count = out_ref.shape[0]
    first = pl.program_id(0) * count

    @pl.when(pl.program_id(0) == 0)
    def _():
        plane = got_ref.shape[0]
        depth = got_ref.shape[1] - 144
        slots = rows.shape[0]
        mark = lax.broadcasted_iota(I32, (128, slots), 0)
        lane = lax.broadcasted_iota(I32, (128, slots), 1)
        i = (lane >> 3) & 7
        quota = ((i & 1) << 2) | (i & 2) | ((i >> 2) & 1)
        at = quota * 16 + where_ref[4]
        digit = jnp.where(mark == at, 64.0, jnp.where(mark == at + 8, 1.0, 0.0))
        found = jnp.zeros((16, slots), F32)
        for p in range(plane):
            for k in range(0, 8, 2):
                a = got_ref[p, depth + 16 * k : depth + 16 * k + 16, :].astype(F32)
                b = got_ref[p, depth + 16 * k + 16 : depth + 16 * k + 32, :].astype(F32)
                to = p * 64 + k * 8
                rows[to : to + 16, 0:256] = jnp.concatenate([a[0:8], b[0:8]], axis=0).astype(BF16)
                rows[to : to + 16, 256:512] = jnp.concatenate([a[8:16], b[8:16]], axis=0).astype(BF16)
            code = got_ref[p, depth + 128 : depth + 144, 0:128]
            these = jnp.where((lane >> 6) == p, digit, 0.0).astype(BF16)
            found += jnp.dot(code, these, preferred_element_type=F32)
        mine = lax.broadcasted_iota(I32, (16, slots), 0) == (
            lax.broadcasted_iota(I32, (16, slots), 1) & 7
        )
        spot = jnp.sum(jnp.where(mine, found, 0.0), axis=0, keepdims=True) - 1.0
        place[...] = jnp.broadcast_to(spot, place.shape).astype(I32)

    near = lax.broadcasted_iota(I32, (count, 256), 0) + (first + where_ref[0])
    spots = lax.broadcasted_iota(I32, (count, place.shape[1]), 0) + first
    match = jnp.where(spots == place[0:1, :], 1.0, 0.0).astype(BF16)
    total = jnp.dot(match, rows[...], preferred_element_type=F32)
    for g in range(4):
        e = refs[2 * g][...].astype(F32)
        w = w_ref[g, pl.ds(pl.program_id(0), 1), :]
        target = w_ref[g, 5:6, :].astype(I32)
        res = (e * w - jnp.where(near == target, 1.0, 0.0)).astype(BF16)
        total += lax.dot_general(
            res, refs[2 * g + 1][...], (((1,), (1,)), ((), ())), preferred_element_type=F32
        )
    out_ref[...] = total.astype(BF16)


def table_call(where, w, got, packs, count):
    tokens = packs[0].shape[1]
    block = 512
    specs, operands = [], []
    for pack in packs:
        specs.append(pl.BlockSpec((CHUNK, tokens), lambda i, s: (i, 0)))
        specs.append(pl.BlockSpec((block, tokens), lambda i, s: (4 + s[2], 0)))
        operands += [pack, pack]
    return pl.pallas_call(
        table_kernel,
        grid_spec=pltpu.PrefetchScalarGridSpec(
            num_scalar_prefetch=1,
            grid=(count // CHUNK,),
            in_specs=[
                pl.BlockSpec(w.shape, lambda i, s: (0, 0, 0)),
                pl.BlockSpec(got.shape, lambda i, s: (0, 0, 0)),
                *specs,
            ],
            out_specs=pl.BlockSpec((CHUNK, block), lambda i, s: (i, 0)),
            scratch_shapes=[pltpu.VMEM((512, block), BF16), pltpu.VMEM((8, 512), I32)],
        ),
        out_shape=jax.ShapeDtypeStruct((count, block), BF16),
        compiler_params=PARAMS,
        cost_estimate=cost(2 * count * block * 1536, 8 * count * 256 + 2 * count * block),
        name="table_grad",
    )(where, w, got, *operands)


def inner(hidden, table, targets, input_ids, cotangent):
    vocab_rows, width = table.shape
    ny, nz, nx = (lax.axis_size(a) for a in VOCAB)
    plane = ny * nx
    vocab_count = plane * nz
    block = width // lax.axis_size(DP)
    xh, c = lax.axis_index("xh"), lax.axis_index("c")
    spot = lax.axis_index("y") * nx + lax.axis_index("xl")
    where = jnp.stack([lax.axis_index(VOCAB) * vocab_rows, xh, c, lax.axis_index("z"), spot]).astype(I32)
    tokens = hidden.shape[0]
    goal = targets.reshape(1, tokens)

    half = width // 2
    ids = jnp.stack([input_ids >> 14, (input_ids >> 7) & 127, input_ids & 127]).astype(BF16)
    ids = jnp.pad(ids, ((0, 5), (0, block - ids.shape[1])))
    ids = jnp.concatenate([ids, ids], axis=1)
    near_rows = lax.dynamic_slice_in_dim(cotangent, xh * half, half, 1)
    far_rows = lax.dynamic_slice_in_dim(cotangent, (1 - xh) * half, half, 1)
    near_rows = jnp.concatenate([near_rows, ids], axis=0)
    far_rows = jnp.concatenate([far_rows, ids], axis=0)
    far_rows = swap(far_rows, "xh")
    packs = (near_rows, swap(near_rows, "c"), far_rows, swap(far_rows, "c"))
    away, middle, one, x0, c0 = select_call(where, packs, vocab_rows)
    r1 = partner(away, 4)
    r2 = partner(join_call((middle, 0, 256), (r1, 256, 256), (c0, 0, 16), (r1, 512, 16)), 2)
    r3 = join_call(
        (one, 0, 128), (r1, 128, 128), (r2, 128, 128), (r2, 384, 128), (c0, 0, 16), (r1, 512, 16), (r2, 512, 32)
    )
    r3 = partner(r3, 1)

    mine = hidden.T
    stage = exchange(to_each(mine, nz), "z").reshape(-1, tokens)
    stage = exchange(to_each(stage, plane), PLANE)
    far_stage = swap(stage, "xh")
    near, sums, own = logits_call(where, goal, stage, table, vocab_count)

    stats = exchange(sums, VOCAB)
    far, _, _ = logits_call(where, goal, far_stage, table, 1)
    near_sib = swap(near, "c")
    far_sib = swap(far, "c")
    part, loss, w = part_call(where, goal, own, stats, near, (x0, r1, r2, r3, c0), table)

    got = exchange(part, PLANE)
    part = jnp.sum(got[:, : width // plane].astype(F32), axis=0).reshape(nz, -1, tokens)
    part = jnp.sum(exchange(part, "z"), axis=0)
    hidden_grad = part.astype(BF16).T

    w_near = jnp.stack([w, swap(w, "c")])
    w_all = jnp.concatenate([w_near, swap(w_near, "xh")], axis=0)
    table_grad = table_call(
        where, w_all, got, (near, near_sib, far, far_sib), vocab_rows
    )
    return loss.reshape(tokens), hidden_grad, table_grad


def solution(mesh):
    fine = Mesh(mesh.devices.reshape(2, 2, 4, 8, 2), ALL)
    placed = (P(DP, VOCAB), P(VOCAB, None), P(DP), P(ALL), P(ALL, None))
    return jax.shard_map(
        inner,
        mesh=fine,
        in_specs=placed,
        out_specs=(P(DP), P(DP, VOCAB), P(VOCAB, DP)),
        check_vma=False,
    )
```

```python
import functools

import jax
import jax.numpy as jnp
from jax import lax
from jax.experimental import pallas as pl
from jax.experimental.pallas import tpu as pltpu
from jax.sharding import Mesh, PartitionSpec as P

BF16 = jnp.bfloat16
F32 = jnp.float32
I32 = jnp.int32
ALL = ("xh", "c", "y", "z", "xl")
DP = ("xh", "c")
VOCAB = ("y", "z", "xl")
PLANE = ("y", "xl")
CHUNK = 400
DEPTH = 3
PARAMS = pltpu.CompilerParams(vmem_limit_bytes=16 * 1024 * 1024)
WIDE = pltpu.CompilerParams(vmem_limit_bytes=57 * 1024 * 1024)
FULL = pltpu.CompilerParams(vmem_limit_bytes=62 * 1024 * 1024)


def exchange(pieces, axes):
    return lax.all_to_all(pieces, axes, 0, 0, tiled=True)


def to_each(value, count):
    return jnp.broadcast_to(value, (count, *value.shape))


def swap(value, axis):
    return lax.ppermute(value, axis, [(0, 1), (1, 0)])


def cost(flops, moved, special=0):
    return pl.CostEstimate(flops=flops, bytes_accessed=moved, transcendentals=special)


def partner(value, bit):
    size = lax.axis_size("z")
    return lax.ppermute(value, "z", [(i, i ^ bit) for i in range(size)])


def join_kernel(cuts, *refs):
    out, at = refs[-1], 0
    for ref, (first, size) in zip(refs, cuts):
        out[at : at + size, :] = ref[first : first + size, :]
        at += size


def join_call(*parts):
    cuts = tuple((first, size) for _, first, size in parts)
    shape = (sum(size for _, size in cuts), parts[0][0].shape[1])
    return pl.pallas_call(
        functools.partial(join_kernel, cuts),
        out_shape=jax.ShapeDtypeStruct(shape, BF16),
        compiler_params=PARAMS,
        cost_estimate=cost(10**6, 2**19),
        name="join",
    )(*(array for array, _, _ in parts))


def select_kernel(vocab_rows, where_ref, *refs):
    packs = refs[:4]
    outs = refs[4:]
    count = packs[0].shape[0] - 8
    total = 4 * count
    line = jnp.concatenate(
        [
            p[count : count + 8, 0:128].astype(F32)[:, 0:count]
            for p in packs
        ],
        axis=1,
    )
    line = line[0:1, :] * 16384.0 + line[1:2, :] * 128.0 + line[2:3, :]
    tall = jnp.broadcast_to(line, (8, total)).T[:, 0:1]

    def parts(ids):
        owner = jnp.floor((ids + 0.5) * (1.0 / vocab_rows))
        spot = (ids - owner * vocab_rows).astype(I32) + 1
        owner = owner.astype(I32)
        plane = (owner >> 4) * 2 + (owner & 1)
        turn = ((owner >> 1) & 7) ^ where_ref[3]
        return owner, plane, turn, spot

    owner, plane, turn, _ = parts(line)
    owner_t, plane_t, turn_t, spot_t = parts(tall)
    early = lax.broadcasted_iota(I32, (total, total), 0)
    later = lax.broadcasted_iota(I32, (total, total), 1)
    before = (owner_t == owner) & (early < later) & ((early >> 6) == (later >> 6))
    rank = jnp.sum(jnp.where(before, 1.0, 0.0), axis=0, keepdims=True).astype(I32)
    token = lax.broadcasted_iota(I32, (1, total), 1)
    row = (token >> 6) * 2 + rank
    slots = turn * 64 + plane * 8 + row
    chosen = lax.broadcasted_iota(I32, (512, total), 0) == slots
    cot = jnp.concatenate([p[0:count, :] for p in packs], axis=0)
    picked = jnp.dot(jnp.where(chosen, 1.0, 0.0).astype(BF16), cot, preferred_element_type=F32)
    lane = lax.broadcasted_iota(I32, (total, 128), 1)
    base = turn_t * 16 + plane_t
    digits = jnp.where(lane == base, spot_t >> 6, jnp.where(lane == base + 8, spot_t & 63, 0))
    mark = lax.broadcasted_iota(I32, (16, total), 0) == row
    code = jnp.dot(
        jnp.where(mark, 1.0, 0.0).astype(BF16),
        digits.astype(F32).astype(BF16),
        preferred_element_type=F32,
    )
    code = jnp.concatenate([code, jnp.zeros((16, 128), F32)], axis=1).astype(BF16)
    far, middle, one, own, mine = outs
    for q in range(8):
        out, at = ((own, 0), (one, 0), (middle, 0), (middle, 128))[q] if q < 4 else (far, (q - 4) * 128)
        for p in range(8):
            piece = picked[q * 64 + p * 8 : q * 64 + p * 8 + 8, :]
            piece = jnp.concatenate([piece[:, 0:256], piece[:, 256:512]], axis=0)
            out[at + p * 16 : at + p * 16 + 16, :] = piece.astype(BF16)
    far[512:528, :] = code
    mine[...] = code


def select_call(where, packs, vocab_rows):
    rows, wide = packs[0].shape
    block = wide // 2
    sizes = (528, 256, 128, 128, 16)
    return pl.pallas_call(
        functools.partial(select_kernel, vocab_rows),
        grid_spec=pltpu.PrefetchScalarGridSpec(
            num_scalar_prefetch=1,
            grid=(1,),
            in_specs=[pl.BlockSpec((rows, block), lambda i, s: (0, s[2]))] * 4,
            out_specs=[pl.BlockSpec((n, 256), lambda i, s: (0, 0)) for n in sizes],
        ),
        out_shape=[jax.ShapeDtypeStruct((n, 256), BF16) for n in sizes],
        compiler_params=PARAMS,
        cost_estimate=cost(2 * 512 * 256 * block, 2**20),
        name="select",
    )(where, *packs)


def logits_kernel(
    where_ref, tgt_ref, got_ref, table_ref, pack_ref, stats_ref, own_ref, hid, tab, buf, sems, out_sems
):
    count, width = tab.shape
    tokens = hid.shape[1]
    half = width // 2
    plane, depth, _ = got_ref.shape
    chunks = count // CHUNK

    def load(i):
        at = pl.ds(pl.multiple_of(i * CHUNK, CHUNK), CHUNK)
        return pltpu.make_async_copy(table_ref.at[at], tab.at[at], sems.at[i])

    def store(i):
        at = pl.ds(pl.multiple_of(i * CHUNK, CHUNK), CHUNK)
        return pltpu.make_async_copy(buf.at[at], pack_ref.at[at], out_sems.at[i])

    for i in range(DEPTH):
        load(i).start()
    for p in range(plane):
        y, x = p // 2, p % 2
        for z in range(depth // 32):
            at = ((y * (depth // 32) + z) * 2 + x) * 32
            hid[at : at + 32, :] = got_ref[p, z * 32 : z * 32 + 32, :]
    base = buf.shape[0] - half
    buf[base:, :] = hid[pl.ds(pl.multiple_of(where_ref[1] * half, half), half), :]
    at = pl.ds(base, half)
    side = pltpu.make_async_copy(buf.at[at], pack_ref.at[at], out_sems.at[chunks])
    side.start()
    own_ref[...] = jnp.zeros(own_ref.shape, F32)

    def one(i, carry):
        top, total, picked = carry
        load(i).wait()

        @pl.when(i + DEPTH < chunks)
        def _():
            load(i + DEPTH).start()

        at = pl.ds(pl.multiple_of(i * CHUNK, CHUNK), CHUNK)
        values = jnp.dot(tab[at, :], hid[...], preferred_element_type=F32)
        index = lax.broadcasted_iota(I32, values.shape, 0) + (where_ref[0] + i * CHUNK)
        picked += jnp.sum(jnp.where(index == tgt_ref[...], values, 0.0), axis=0, keepdims=True)
        peak = jnp.max(values, axis=0, keepdims=True)
        e = jnp.exp(values - peak)
        buf[at, :] = e.astype(BF16)
        store(i).start()
        own_ref[pl.ds(i, 1), :] = peak
        higher = jnp.maximum(top, peak)
        total = total * jnp.exp(top - higher)
        total += jnp.sum(e, axis=0, keepdims=True) * jnp.exp(peak - higher)
        return higher, total, picked

    blank = jnp.zeros((1, tokens), F32)
    start = (jnp.full((1, tokens), -jnp.inf, F32), blank, blank)
    line = jnp.concatenate([*lax.fori_loop(0, chunks, one, start), blank], axis=0)
    stats_ref[...] = jnp.broadcast_to(line[None], stats_ref.shape)
    side.wait()

    def end(i, carry):
        store(i).wait()
        return carry

    lax.fori_loop(0, chunks, end, 0)


def logits_call(where, targets, got, table, copies):
    count, width = table.shape
    tokens = got.shape[2]
    span = 2048 + width // 2
    whole = pl.BlockSpec(memory_space=pltpu.VMEM)
    return pl.pallas_call(
        logits_kernel,
        in_specs=[pl.BlockSpec(memory_space=pltpu.SMEM), whole, whole, pl.BlockSpec(memory_space=pl.ANY)],
        out_specs=[pl.BlockSpec(memory_space=pltpu.HBM), whole, whole],
        scratch_shapes=[
            pltpu.VMEM((width, tokens), BF16),
            pltpu.VMEM((count, width), BF16),
            pltpu.VMEM((span, tokens), BF16),
            pltpu.SemaphoreType.DMA((count // CHUNK,)),
            pltpu.SemaphoreType.DMA((count // CHUNK + 1,)),
        ],
        out_shape=[
            pltpu.HBM((span, tokens), BF16),
            jax.ShapeDtypeStruct((copies, 4, tokens), F32),
            jax.ShapeDtypeStruct((8, tokens), F32),
        ],
        compiler_params=WIDE,
        cost_estimate=cost(2 * count * width * tokens, 2 * count * width + 4 * span * tokens),
        name="logits",
    )(where, targets, got, table)


QUOTA = (0, 4, 2, 6, 1, 5, 3, 7)


def part_kernel(
    where_ref, tgt_ref, own_ref, stats_ref, near_ref, x0, r1, r2, r3, c0, table_ref,
    out_ref, loss_ref, w_ref, lhs, tab, buf, sems, out_sems,
):
    tokens = tgt_ref.shape[1]
    count, width = table_ref.shape
    plane = buf.shape[0]
    depth = width // plane
    turns, _, wide = tab.shape

    def load(j):
        at = table_ref.at[:, pl.ds(pl.multiple_of(j * wide, wide), wide)]
        return pltpu.make_async_copy(at, tab.at[j], sems.at[j])

    def store(j):
        at = pl.ds(j * 2, 2)
        return pltpu.make_async_copy(buf.at[at], out_ref.at[at], out_sems.at[j])

    for j in range(DEPTH):
        load(j).start()

    stats = stats_ref[...]
    top = jnp.max(stats, axis=0)[0:1, :]
    sums = jnp.sum(stats[:, 1:2, :] * jnp.exp(stats[:, 0:1, :] - top[None]), axis=0)
    picks = jnp.sum(stats, axis=0)[2:3, :]
    loss_ref[...] = top + jnp.log(sums) - picks
    chunks = count // CHUNK
    w = jnp.exp(own_ref[0:chunks, :] - top) / sums
    w_ref[...] = jnp.concatenate(
        [w, tgt_ref[...].astype(F32), jnp.zeros((7 - chunks, tokens), F32)], axis=0
    )
    for i in range(chunks):
        index = lax.broadcasted_iota(I32, (CHUNK, tokens), 0) + (where_ref[0] + i * CHUNK)
        e = near_ref[i * CHUNK : (i + 1) * CHUNK, :].astype(F32)
        residual = e * w[i : i + 1, :] - jnp.where(index == tgt_ref[...], 1.0, 0.0)
        lhs[i * CHUNK : (i + 1) * CHUNK, :] = residual.astype(BF16)

    marks = [c0[...], r1[512:528, :], r2[512:528, :], r2[528:544, :]]
    marks += [r3[k : k + 16, :] for k in range(512, 576, 16)]
    group = lax.broadcasted_iota(I32, (16, tokens), 1) >> 4
    mixed = jnp.zeros((16, tokens), F32)
    for q, mark in zip(QUOTA, marks):
        mixed += jnp.where(group == q, mark.astype(F32), 0.0)
    pieces = ((x0, 0), (r1, 0), (r2, 0), (r2, 256), (r3, 0), (r3, 128), (r3, 256), (r3, 384))
    for p in range(plane):
        for i, (ref, at) in enumerate(pieces):
            to = depth + 16 * i
            buf[p, to : to + 16, :] = ref[at + p * 16 : at + p * 16 + 16, :]
        buf[p, depth + 128 : depth + 144, :] = mixed.astype(BF16)

    def one(j, carry):
        load(j).wait()

        @pl.when(j + DEPTH < turns)
        def _():
            load(j + DEPTH).start()

        part = lax.dot_general(
            tab[j], lhs[...], (((0,), (0,)), ((), ())), preferred_element_type=F32
        )
        for k in range(wide // 32):
            z, x = k // 2, k % 2
            buf[j * 2 + x, z * 32 : z * 32 + 32, :] = part[k * 32 : k * 32 + 32, :].astype(BF16)
        store(j).start()
        return carry

    lax.fori_loop(0, turns, one, 0)

    def end(j, carry):
        store(j).wait()
        return carry

    lax.fori_loop(0, turns, end, 0)


def part_call(where, targets, own, stats, near, riders, table):
    count, width = table.shape
    tokens = targets.shape[1]
    plane, wide = 8, 512
    whole = pl.BlockSpec(memory_space=pltpu.VMEM)
    anywhere = pl.BlockSpec(memory_space=pl.ANY)
    shape = (plane, width // plane + 144, tokens)
    return pl.pallas_call(
        part_kernel,
        in_specs=[pl.BlockSpec(memory_space=pltpu.SMEM), *[whole] * 9, anywhere],
        out_specs=[pl.BlockSpec(memory_space=pltpu.HBM), whole, whole],
        scratch_shapes=[
            pltpu.VMEM((count, tokens), BF16),
            pltpu.VMEM((width // wide, count, wide), BF16),
            pltpu.VMEM(shape, BF16),
            pltpu.SemaphoreType.DMA((width // wide,)),
            pltpu.SemaphoreType.DMA((plane // 2,)),
        ],
        out_shape=[
            pltpu.HBM(shape, BF16),
            jax.ShapeDtypeStruct((1, tokens), F32),
            jax.ShapeDtypeStruct((8, tokens), F32),
        ],
        compiler_params=FULL,
        cost_estimate=cost(2 * count * width * tokens, 2 * count * width + 2 * width * tokens),
        name="part",
    )(where, targets, own, stats, near, *riders, table)


def table_kernel(where_ref, w_ref, got_ref, *refs):
    out_ref, rows, place = refs[-3:]
    count = out_ref.shape[0]
    first = pl.program_id(0) * count

    @pl.when(pl.program_id(0) == 0)
    def _():
        plane = got_ref.shape[0]
        depth = got_ref.shape[1] - 144
        slots = rows.shape[0]
        mark = lax.broadcasted_iota(I32, (128, slots), 0)
        lane = lax.broadcasted_iota(I32, (128, slots), 1)
        i = (lane >> 3) & 7
        quota = ((i & 1) << 2) | (i & 2) | ((i >> 2) & 1)
        at = quota * 16 + where_ref[4]
        digit = jnp.where(mark == at, 64.0, jnp.where(mark == at + 8, 1.0, 0.0))
        found = jnp.zeros((16, slots), F32)
        for p in range(plane):
            for k in range(0, 8, 2):
                a = got_ref[p, depth + 16 * k : depth + 16 * k + 16, :].astype(F32)
                b = got_ref[p, depth + 16 * k + 16 : depth + 16 * k + 32, :].astype(F32)
                to = p * 64 + k * 8
                rows[to : to + 16, 0:256] = jnp.concatenate([a[0:8], b[0:8]], axis=0).astype(BF16)
                rows[to : to + 16, 256:512] = jnp.concatenate([a[8:16], b[8:16]], axis=0).astype(BF16)
            code = got_ref[p, depth + 128 : depth + 144, 0:128]
            these = jnp.where((lane >> 6) == p, digit, 0.0).astype(BF16)
            found += jnp.dot(code, these, preferred_element_type=F32)
        mine = lax.broadcasted_iota(I32, (16, slots), 0) == (
            lax.broadcasted_iota(I32, (16, slots), 1) & 7
        )
        spot = jnp.sum(jnp.where(mine, found, 0.0), axis=0, keepdims=True) - 1.0
        place[...] = jnp.broadcast_to(spot, place.shape).astype(I32)

    near = lax.broadcasted_iota(I32, (count, 256), 0) + (first + where_ref[0])
    spots = lax.broadcasted_iota(I32, (count, place.shape[1]), 0) + first
    match = jnp.where(spots == place[0:1, :], 1.0, 0.0).astype(BF16)
    total = jnp.dot(match, rows[...], preferred_element_type=F32)
    for g in range(4):
        e = refs[2 * g][...].astype(F32)
        w = w_ref[g, pl.ds(pl.program_id(0), 1), :]
        target = w_ref[g, 5:6, :].astype(I32)
        res = (e * w - jnp.where(near == target, 1.0, 0.0)).astype(BF16)
        total += lax.dot_general(
            res, refs[2 * g + 1][...], (((1,), (1,)), ((), ())), preferred_element_type=F32
        )
    out_ref[...] = total.astype(BF16)


def table_call(where, w, got, packs, count):
    tokens = packs[0].shape[1]
    block = 512
    specs, operands = [], []
    for pack in packs:
        specs.append(pl.BlockSpec((CHUNK, tokens), lambda i, s: (i, 0)))
        specs.append(pl.BlockSpec((block, tokens), lambda i, s: (4 + s[2], 0)))
        operands += [pack, pack]
    return pl.pallas_call(
        table_kernel,
        grid_spec=pltpu.PrefetchScalarGridSpec(
            num_scalar_prefetch=1,
            grid=(count // CHUNK,),
            in_specs=[
                pl.BlockSpec(w.shape, lambda i, s: (0, 0, 0)),
                pl.BlockSpec(got.shape, lambda i, s: (0, 0, 0)),
                *specs,
            ],
            out_specs=pl.BlockSpec((CHUNK, block), lambda i, s: (i, 0)),
            scratch_shapes=[pltpu.VMEM((512, block), BF16), pltpu.VMEM((8, 512), I32)],
        ),
        out_shape=jax.ShapeDtypeStruct((count, block), BF16),
        compiler_params=WIDE,
        cost_estimate=cost(2 * count * block * 1536, 8 * count * 256 + 2 * count * block),
        name="table_grad",
    )(where, w, got, *operands)


def inner(hidden, table, targets, input_ids, cotangent):
    vocab_rows, width = table.shape
    ny, nz, nx = (lax.axis_size(a) for a in VOCAB)
    plane = ny * nx
    vocab_count = plane * nz
    block = width // lax.axis_size(DP)
    xh, c = lax.axis_index("xh"), lax.axis_index("c")
    spot = lax.axis_index("y") * nx + lax.axis_index("xl")
    where = jnp.stack([lax.axis_index(VOCAB) * vocab_rows, xh, c, lax.axis_index("z"), spot]).astype(I32)
    tokens = hidden.shape[0]
    goal = targets.reshape(1, tokens)

    half = width // 2
    ids = jnp.stack([input_ids >> 14, (input_ids >> 7) & 127, input_ids & 127]).astype(BF16)
    ids = jnp.pad(ids, ((0, 5), (0, block - ids.shape[1])))
    ids = jnp.concatenate([ids, ids], axis=1)
    near_rows = lax.dynamic_slice_in_dim(cotangent, xh * half, half, 1)
    far_rows = lax.dynamic_slice_in_dim(cotangent, (1 - xh) * half, half, 1)
    near_rows = jnp.concatenate([near_rows, ids], axis=0)
    far_rows = jnp.concatenate([far_rows, ids], axis=0)
    far_rows = swap(far_rows, "xh")
    packs = (near_rows, swap(near_rows, "c"), far_rows, swap(far_rows, "c"))
    away, middle, one, x0, c0 = select_call(where, packs, vocab_rows)
    r1 = partner(away, 4)
    r2 = partner(join_call((middle, 0, 256), (r1, 256, 256), (c0, 0, 16), (r1, 512, 16)), 2)
    r3 = join_call(
        (one, 0, 128), (r1, 128, 128), (r2, 128, 128), (r2, 384, 128), (c0, 0, 16), (r1, 512, 16), (r2, 512, 32)
    )
    r3 = partner(r3, 1)

    mine = hidden.T
    stage = exchange(to_each(mine, nz), "z").reshape(-1, tokens)
    stage = exchange(to_each(stage, plane), PLANE)
    far_stage = swap(stage, "xh")
    near, sums, own = logits_call(where, goal, stage, table, vocab_count)

    stats = exchange(sums, VOCAB)
    far, _, _ = logits_call(where, goal, far_stage, table, 1)
    near_sib = swap(near, "c")
    far_sib = swap(far, "c")
    part, loss, w = part_call(where, goal, own, stats, near, (x0, r1, r2, r3, c0), table)

    got = exchange(part, PLANE)
    part = jnp.sum(got[:, : width // plane].astype(F32), axis=0).reshape(nz, -1, tokens)
    part = jnp.sum(exchange(part, "z"), axis=0)
    hidden_grad = part.astype(BF16).T

    w_far = swap(w, "xh")
    w_all = jnp.stack([w, swap(w, "c"), w_far, swap(w_far, "c")])
    table_grad = table_call(
        where, w_all, got, (near, near_sib, far, far_sib), vocab_rows
    )
    return loss.reshape(tokens), hidden_grad, table_grad


def solution(mesh):
    fine = Mesh(mesh.devices.reshape(2, 2, 4, 8, 2), ALL)
    placed = (P(DP, VOCAB), P(VOCAB, None), P(DP), P(ALL), P(ALL, None))
    return jax.shard_map(
        inner,
        mesh=fine,
        in_specs=placed,
        out_specs=(P(DP), P(DP, VOCAB), P(VOCAB, DP)),
        check_vma=False,
    )
```

```python
import functools

import jax
import jax.numpy as jnp
from jax import lax
from jax.experimental import pallas as pl
from jax.experimental.pallas import tpu as pltpu
from jax.sharding import Mesh, PartitionSpec as P

BF16 = jnp.bfloat16
F32 = jnp.float32
I32 = jnp.int32
ALL = ("xh", "c", "y", "z", "xl")
DP = ("xh", "c")
VOCAB = ("y", "z", "xl")
PLANE = ("y", "xl")
CHUNK = 400
DEPTH = 3
PARAMS = pltpu.CompilerParams(vmem_limit_bytes=16 * 1024 * 1024)
WIDE = pltpu.CompilerParams(vmem_limit_bytes=57 * 1024 * 1024)
BASE = pltpu.CompilerParams(vmem_limit_bytes=60 * 1024 * 1024)
FULL = pltpu.CompilerParams(vmem_limit_bytes=62 * 1024 * 1024)


def exchange(pieces, axes):
    return lax.all_to_all(pieces, axes, 0, 0, tiled=True)


def to_each(value, count):
    return jnp.broadcast_to(value, (count, *value.shape))


def swap(value, axis):
    return lax.ppermute(value, axis, [(0, 1), (1, 0)])


def cost(flops, moved, special=0):
    return pl.CostEstimate(flops=flops, bytes_accessed=moved, transcendentals=special)


def partner(value, bit):
    size = lax.axis_size("z")
    return lax.ppermute(value, "z", [(i, i ^ bit) for i in range(size)])


def join_kernel(cuts, *refs):
    out, at = refs[-1], 0
    for ref, (first, size) in zip(refs, cuts):
        out[at : at + size, :] = ref[first : first + size, :]
        at += size


def join_call(*parts):
    cuts = tuple((first, size) for _, first, size in parts)
    shape = (sum(size for _, size in cuts), parts[0][0].shape[1])
    return pl.pallas_call(
        functools.partial(join_kernel, cuts),
        out_shape=jax.ShapeDtypeStruct(shape, BF16),
        compiler_params=PARAMS,
        cost_estimate=cost(10**6, 2**19),
        name="join",
    )(*(array for array, _, _ in parts))


def select_kernel(vocab_rows, where_ref, *refs):
    packs = refs[:4]
    outs = refs[4:]
    count = packs[0].shape[0] - 8
    total = 4 * count
    line = jnp.concatenate(
        [
            p[count : count + 8, 0:128].astype(F32)[:, 0:count]
            for p in packs
        ],
        axis=1,
    )
    line = line[0:1, :] * 16384.0 + line[1:2, :] * 128.0 + line[2:3, :]
    tall = jnp.broadcast_to(line, (8, total)).T[:, 0:1]

    def parts(ids):
        owner = jnp.floor((ids + 0.5) * (1.0 / vocab_rows))
        spot = (ids - owner * vocab_rows).astype(I32) + 1
        owner = owner.astype(I32)
        plane = (owner >> 4) * 2 + (owner & 1)
        turn = ((owner >> 1) & 7) ^ where_ref[3]
        return owner, plane, turn, spot

    owner, plane, turn, _ = parts(line)
    owner_t, plane_t, turn_t, spot_t = parts(tall)
    early = lax.broadcasted_iota(I32, (total, total), 0)
    later = lax.broadcasted_iota(I32, (total, total), 1)
    before = (owner_t == owner) & (early < later) & ((early >> 6) == (later >> 6))
    rank = jnp.sum(jnp.where(before, 1.0, 0.0), axis=0, keepdims=True).astype(I32)
    token = lax.broadcasted_iota(I32, (1, total), 1)
    row = (token >> 6) * 2 + rank
    slots = turn * 64 + plane * 8 + row
    chosen = lax.broadcasted_iota(I32, (512, total), 0) == slots
    cot = jnp.concatenate([p[0:count, :] for p in packs], axis=0)
    picked = jnp.dot(jnp.where(chosen, 1.0, 0.0).astype(BF16), cot, preferred_element_type=F32)
    lane = lax.broadcasted_iota(I32, (total, 128), 1)
    base = turn_t * 16 + plane_t
    digits = jnp.where(lane == base, spot_t >> 6, jnp.where(lane == base + 8, spot_t & 63, 0))
    mark = lax.broadcasted_iota(I32, (16, total), 0) == row
    code = jnp.dot(
        jnp.where(mark, 1.0, 0.0).astype(BF16),
        digits.astype(F32).astype(BF16),
        preferred_element_type=F32,
    )
    code = jnp.concatenate([code, jnp.zeros((16, 128), F32)], axis=1).astype(BF16)
    far, middle, one, own, mine = outs
    for q in range(8):
        out, at = ((own, 0), (one, 0), (middle, 0), (middle, 128))[q] if q < 4 else (far, (q - 4) * 128)
        for p in range(8):
            piece = picked[q * 64 + p * 8 : q * 64 + p * 8 + 8, :]
            piece = jnp.concatenate([piece[:, 0:256], piece[:, 256:512]], axis=0)
            out[at + p * 16 : at + p * 16 + 16, :] = piece.astype(BF16)
    far[512:528, :] = code
    mine[...] = code


def select_call(where, packs, vocab_rows):
    rows, wide = packs[0].shape
    block = wide // 2
    sizes = (528, 256, 128, 128, 16)
    return pl.pallas_call(
        functools.partial(select_kernel, vocab_rows),
        grid_spec=pltpu.PrefetchScalarGridSpec(
            num_scalar_prefetch=1,
            grid=(1,),
            in_specs=[pl.BlockSpec((rows, block), lambda i, s: (0, s[2]))] * 4,
            out_specs=[pl.BlockSpec((n, 256), lambda i, s: (0, 0)) for n in sizes],
        ),
        out_shape=[jax.ShapeDtypeStruct((n, 256), BF16) for n in sizes],
        compiler_params=PARAMS,
        cost_estimate=cost(2 * 512 * 256 * block, 2**20),
        name="select",
    )(where, *packs)


def logits_kernel(
    where_ref, tgt_ref, got_ref, table_ref, pack_ref, stats_ref, own_ref, hid, tab, buf, sems, out_sems
):
    count, width = tab.shape
    tokens = hid.shape[1]
    half = width // 2
    plane, depth, _ = got_ref.shape
    chunks = count // CHUNK

    def load(i):
        at = pl.ds(pl.multiple_of(i * CHUNK, CHUNK), CHUNK)
        return pltpu.make_async_copy(table_ref.at[at], tab.at[at], sems.at[i])

    def store(i):
        at = pl.ds(pl.multiple_of(i * CHUNK, CHUNK), CHUNK)
        return pltpu.make_async_copy(buf.at[at], pack_ref.at[at], out_sems.at[i])

    for i in range(DEPTH):
        load(i).start()
    for p in range(plane):
        y, x = p // 2, p % 2
        for z in range(depth // 32):
            at = ((y * (depth // 32) + z) * 2 + x) * 32
            hid[at : at + 32, :] = got_ref[p, z * 32 : z * 32 + 32, :]
    base = buf.shape[0] - half
    buf[base:, :] = hid[pl.ds(pl.multiple_of(where_ref[1] * half, half), half), :]
    at = pl.ds(base, half)
    side = pltpu.make_async_copy(buf.at[at], pack_ref.at[at], out_sems.at[chunks])
    side.start()
    own_ref[...] = jnp.zeros(own_ref.shape, F32)

    def one(i, carry):
        top, total, picked = carry
        load(i).wait()

        @pl.when(i + DEPTH < chunks)
        def _():
            load(i + DEPTH).start()

        at = pl.ds(pl.multiple_of(i * CHUNK, CHUNK), CHUNK)
        values = jnp.dot(tab[at, :], hid[...], preferred_element_type=F32)
        index = lax.broadcasted_iota(I32, values.shape, 0) + (where_ref[0] + i * CHUNK)
        picked += jnp.sum(jnp.where(index == tgt_ref[...], values, 0.0), axis=0, keepdims=True)
        peak = jnp.max(values, axis=0, keepdims=True)
        e = jnp.exp(values - peak)
        buf[at, :] = e.astype(BF16)
        store(i).start()
        own_ref[pl.ds(i, 1), :] = peak
        higher = jnp.maximum(top, peak)
        total = total * jnp.exp(top - higher)
        total += jnp.sum(e, axis=0, keepdims=True) * jnp.exp(peak - higher)
        return higher, total, picked

    blank = jnp.zeros((1, tokens), F32)
    start = (jnp.full((1, tokens), -jnp.inf, F32), blank, blank)
    line = jnp.concatenate([*lax.fori_loop(0, chunks, one, start), blank], axis=0)
    stats_ref[...] = jnp.broadcast_to(line[None], stats_ref.shape)
    side.wait()

    def end(i, carry):
        store(i).wait()
        return carry

    lax.fori_loop(0, chunks, end, 0)


def logits_call(where, targets, got, table, copies):
    count, width = table.shape
    tokens = got.shape[2]
    span = 2048 + width // 2
    whole = pl.BlockSpec(memory_space=pltpu.VMEM)
    return pl.pallas_call(
        logits_kernel,
        in_specs=[pl.BlockSpec(memory_space=pltpu.SMEM), whole, whole, pl.BlockSpec(memory_space=pl.ANY)],
        out_specs=[pl.BlockSpec(memory_space=pltpu.HBM), whole, whole],
        scratch_shapes=[
            pltpu.VMEM((width, tokens), BF16),
            pltpu.VMEM((count, width), BF16),
            pltpu.VMEM((span, tokens), BF16),
            pltpu.SemaphoreType.DMA((count // CHUNK,)),
            pltpu.SemaphoreType.DMA((count // CHUNK + 1,)),
        ],
        out_shape=[
            pltpu.HBM((span, tokens), BF16),
            jax.ShapeDtypeStruct((copies, 4, tokens), F32),
            jax.ShapeDtypeStruct((8, tokens), F32),
        ],
        compiler_params=WIDE,
        cost_estimate=cost(2 * count * width * tokens, 2 * count * width + 4 * span * tokens),
        name="logits",
    )(where, targets, got, table)


QUOTA = (0, 4, 2, 6, 1, 5, 3, 7)


def part_kernel(
    where_ref, tgt_ref, own_ref, stats_ref, near_ref, x0, r1, r2, r3, c0, table_ref,
    out_ref, loss_ref, w_ref, near, lhs, tab, buf, sems, out_sems,
):
    tokens = tgt_ref.shape[1]
    count, width = table_ref.shape
    plane = buf.shape[0]
    depth = width // plane
    turns, _, wide = tab.shape

    def load(j):
        at = table_ref.at[:, pl.ds(pl.multiple_of(j * wide, wide), wide)]
        return pltpu.make_async_copy(at, tab.at[j], sems.at[j])

    def store(j):
        at = pl.ds(j * 2, 2)
        return pltpu.make_async_copy(buf.at[at], out_ref.at[at], out_sems.at[j])

    given = pltpu.make_async_copy(near_ref.at[pl.ds(0, count)], near, sems.at[turns])
    given.start()
    for j in range(DEPTH):
        load(j).start()

    stats = stats_ref[...]
    top = jnp.max(stats, axis=0)[0:1, :]
    sums = jnp.sum(stats[:, 1:2, :] * jnp.exp(stats[:, 0:1, :] - top[None]), axis=0)
    picks = jnp.sum(stats, axis=0)[2:3, :]
    loss_ref[...] = top + jnp.log(sums) - picks
    chunks = count // CHUNK
    w = jnp.exp(own_ref[0:chunks, :] - top) / sums
    w_ref[...] = jnp.concatenate(
        [w, tgt_ref[...].astype(F32), jnp.zeros((7 - chunks, tokens), F32)], axis=0
    )
    given.wait()
    for i in range(chunks):
        index = lax.broadcasted_iota(I32, (CHUNK, tokens), 0) + (where_ref[0] + i * CHUNK)
        e = near[i * CHUNK : (i + 1) * CHUNK, :].astype(F32)
        residual = e * w[i : i + 1, :] - jnp.where(index == tgt_ref[...], 1.0, 0.0)
        lhs[i * CHUNK : (i + 1) * CHUNK, :] = residual.astype(BF16)

    marks = [c0[...], r1[512:528, :], r2[512:528, :], r2[528:544, :]]
    marks += [r3[k : k + 16, :] for k in range(512, 576, 16)]
    group = lax.broadcasted_iota(I32, (16, tokens), 1) >> 4
    mixed = jnp.zeros((16, tokens), F32)
    for q, mark in zip(QUOTA, marks):
        mixed += jnp.where(group == q, mark.astype(F32), 0.0)
    pieces = ((x0, 0), (r1, 0), (r2, 0), (r2, 256), (r3, 0), (r3, 128), (r3, 256), (r3, 384))
    for p in range(plane):
        for i, (ref, at) in enumerate(pieces):
            to = depth + 16 * i
            buf[p, to : to + 16, :] = ref[at + p * 16 : at + p * 16 + 16, :]
        buf[p, depth + 128 : depth + 144, :] = mixed.astype(BF16)

    def one(j, carry):
        load(j).wait()

        @pl.when(j + DEPTH < turns)
        def _():
            load(j + DEPTH).start()

        part = lax.dot_general(
            tab[j], lhs[...], (((0,), (0,)), ((), ())), preferred_element_type=F32
        )
        for k in range(wide // 32):
            z, x = k // 2, k % 2
            buf[j * 2 + x, z * 32 : z * 32 + 32, :] = part[k * 32 : k * 32 + 32, :].astype(BF16)
        store(j).start()
        return carry

    lax.fori_loop(0, turns, one, 0)

    def end(j, carry):
        store(j).wait()
        return carry

    lax.fori_loop(0, turns, end, 0)


def part_call(where, targets, own, stats, near, riders, table):
    count, width = table.shape
    tokens = targets.shape[1]
    plane, wide = 8, 512
    whole = pl.BlockSpec(memory_space=pltpu.VMEM)
    anywhere = pl.BlockSpec(memory_space=pl.ANY)
    shape = (plane, width // plane + 144, tokens)
    return pl.pallas_call(
        part_kernel,
        in_specs=[
            pl.BlockSpec(memory_space=pltpu.SMEM), *[whole] * 3, anywhere, *[whole] * 5, anywhere
        ],
        out_specs=[pl.BlockSpec(memory_space=pltpu.HBM), whole, whole],
        scratch_shapes=[
            pltpu.VMEM((count, tokens), BF16),
            pltpu.VMEM((count, tokens), BF16),
            pltpu.VMEM((width // wide, count, wide), BF16),
            pltpu.VMEM(shape, BF16),
            pltpu.SemaphoreType.DMA((width // wide + 1,)),
            pltpu.SemaphoreType.DMA((plane // 2,)),
        ],
        out_shape=[
            pltpu.HBM(shape, BF16),
            jax.ShapeDtypeStruct((1, tokens), F32),
            jax.ShapeDtypeStruct((8, tokens), F32),
        ],
        compiler_params=FULL,
        cost_estimate=cost(2 * count * width * tokens, 2 * count * width + 2 * width * tokens),
        name="part",
    )(where, targets, own, stats, near, *riders, table)


def table_kernel(where_ref, got_ref, base_ref, *refs):
    out_ref, rows, place = refs[-3:]
    count = out_ref.shape[0]
    first = pl.program_id(0) * count

    @pl.when(pl.program_id(0) == 0)
    def _():
        plane = got_ref.shape[0]
        depth = got_ref.shape[1] - 144
        slots = rows.shape[0]
        mark = lax.broadcasted_iota(I32, (128, slots), 0)
        lane = lax.broadcasted_iota(I32, (128, slots), 1)
        i = (lane >> 3) & 7
        quota = ((i & 1) << 2) | (i & 2) | ((i >> 2) & 1)
        at = quota * 16 + where_ref[4]
        digit = jnp.where(mark == at, 64.0, jnp.where(mark == at + 8, 1.0, 0.0))
        found = jnp.zeros((16, slots), F32)
        for p in range(plane):
            for k in range(0, 8, 2):
                a = got_ref[p, depth + 16 * k : depth + 16 * k + 16, :].astype(F32)
                b = got_ref[p, depth + 16 * k + 16 : depth + 16 * k + 32, :].astype(F32)
                to = p * 64 + k * 8
                rows[to : to + 16, 0:256] = jnp.concatenate([a[0:8], b[0:8]], axis=0).astype(BF16)
                rows[to : to + 16, 256:512] = jnp.concatenate([a[8:16], b[8:16]], axis=0).astype(BF16)
            code = got_ref[p, depth + 128 : depth + 144, 0:128]
            these = jnp.where((lane >> 6) == p, digit, 0.0).astype(BF16)
            found += jnp.dot(code, these, preferred_element_type=F32)
        mine = lax.broadcasted_iota(I32, (16, slots), 0) == (
            lax.broadcasted_iota(I32, (16, slots), 1) & 7
        )
        spot = jnp.sum(jnp.where(mine, found, 0.0), axis=0, keepdims=True) - 1.0
        place[...] = jnp.broadcast_to(spot, place.shape).astype(I32)

    spots = lax.broadcasted_iota(I32, (count, place.shape[1]), 0) + first
    match = jnp.where(spots == place[0:1, :], 1.0, 0.0).astype(BF16)
    total = base_ref[...] + jnp.dot(match, rows[...], preferred_element_type=F32)
    out_ref[...] = total.astype(BF16)


def table_call(where, got, base):
    count, block = base.shape
    part = pl.BlockSpec((CHUNK, block), lambda i, s: (i, 0))
    return pl.pallas_call(
        table_kernel,
        grid_spec=pltpu.PrefetchScalarGridSpec(
            num_scalar_prefetch=1,
            grid=(count // CHUNK,),
            in_specs=[pl.BlockSpec(got.shape, lambda i, s: (0, 0, 0)), part],
            out_specs=part,
            scratch_shapes=[pltpu.VMEM((512, block), BF16), pltpu.VMEM((8, 512), I32)],
        ),
        out_shape=jax.ShapeDtypeStruct((count, block), BF16),
        compiler_params=FULL,
        cost_estimate=cost(2 * count * block * 512, 6 * count * block),
        name="table_grad",
    )(where, got, base)


def base_kernel(where_ref, w_ref, *refs):
    out_ref = refs[-1]
    count = out_ref.shape[0]
    first = where_ref[0] + pl.program_id(0) * count
    near = lax.broadcasted_iota(I32, (count, 256), 0) + first
    total = jnp.zeros(out_ref.shape, F32)
    for g in range(4):
        e = refs[2 * g][...].astype(F32)
        w = w_ref[g, pl.ds(pl.program_id(0), 1), :]
        target = w_ref[g, 5:6, :].astype(I32)
        res = (e * w - jnp.where(near == target, 1.0, 0.0)).astype(BF16)
        total += lax.dot_general(
            res, refs[2 * g + 1][...], (((1,), (1,)), ((), ())), preferred_element_type=F32
        )
    out_ref[...] = total


def base_call(where, w, packs, count):
    tokens = packs[0].shape[1]
    block = 512
    specs, operands = [], []
    for pack in packs:
        specs.append(pl.BlockSpec((CHUNK, tokens), lambda i, s: (i, 0)))
        specs.append(pl.BlockSpec((block, tokens), lambda i, s: (4 + s[2], 0)))
        operands += [pack, pack]
    return pl.pallas_call(
        base_kernel,
        grid_spec=pltpu.PrefetchScalarGridSpec(
            num_scalar_prefetch=1,
            grid=(count // CHUNK,),
            in_specs=[pl.BlockSpec(w.shape, lambda i, s: (0, 0, 0)), *specs],
            out_specs=pl.BlockSpec((CHUNK, block), lambda i, s: (i, 0)),
        ),
        out_shape=jax.ShapeDtypeStruct((count, block), F32),
        compiler_params=BASE,
        cost_estimate=cost(2 * count * block * 1024, 8 * count * 256 + 4 * count * block),
        name="base",
    )(where, w, *operands)


def inner(hidden, table, targets, input_ids, cotangent):
    vocab_rows, width = table.shape
    ny, nz, nx = (lax.axis_size(a) for a in VOCAB)
    plane = ny * nx
    vocab_count = plane * nz
    block = width // lax.axis_size(DP)
    xh, c = lax.axis_index("xh"), lax.axis_index("c")
    spot = lax.axis_index("y") * nx + lax.axis_index("xl")
    where = jnp.stack([lax.axis_index(VOCAB) * vocab_rows, xh, c, lax.axis_index("z"), spot]).astype(I32)
    tokens = hidden.shape[0]
    goal = targets.reshape(1, tokens)

    half = width // 2
    ids = jnp.stack([input_ids >> 14, (input_ids >> 7) & 127, input_ids & 127]).astype(BF16)
    ids = jnp.pad(ids, ((0, 5), (0, block - ids.shape[1])))
    ids = jnp.concatenate([ids, ids], axis=1)
    near_rows = lax.dynamic_slice_in_dim(cotangent, xh * half, half, 1)
    far_rows = lax.dynamic_slice_in_dim(cotangent, (1 - xh) * half, half, 1)
    near_rows = jnp.concatenate([near_rows, ids], axis=0)
    far_rows = jnp.concatenate([far_rows, ids], axis=0)
    far_rows = swap(far_rows, "xh")
    packs = (near_rows, swap(near_rows, "c"), far_rows, swap(far_rows, "c"))
    away, middle, one, x0, c0 = select_call(where, packs, vocab_rows)
    r1 = partner(away, 4)
    r2 = partner(join_call((middle, 0, 256), (r1, 256, 256), (c0, 0, 16), (r1, 512, 16)), 2)
    r3 = join_call(
        (one, 0, 128), (r1, 128, 128), (r2, 128, 128), (r2, 384, 128), (c0, 0, 16), (r1, 512, 16), (r2, 512, 32)
    )
    r3 = partner(r3, 1)

    mine = hidden.T
    stage = exchange(to_each(mine, nz), "z").reshape(-1, tokens)
    stage = exchange(to_each(stage, plane), PLANE)
    far_stage = swap(stage, "xh")
    near, sums, own = logits_call(where, goal, stage, table, vocab_count)

    stats = exchange(sums, VOCAB)
    far, _, _ = logits_call(where, goal, far_stage, table, 1)
    near_sib = swap(near, "c")
    far_sib = swap(far, "c")
    part, loss, w = part_call(where, goal, own, stats, near, (x0, r1, r2, r3, c0), table)

    got = exchange(part, PLANE)
    part = jnp.sum(got[:, : width // plane].astype(F32), axis=0).reshape(nz, -1, tokens)
    part = jnp.sum(exchange(part, "z"), axis=0)
    hidden_grad = part.astype(BF16).T

    w_far = swap(w, "xh")
    w_all = jnp.stack([w, swap(w, "c"), w_far, swap(w_far, "c")])
    base = base_call(where, w_all, (near, near_sib, far, far_sib), vocab_rows)
    table_grad = table_call(where, got, base)
    return loss.reshape(tokens), hidden_grad, table_grad


def solution(mesh):
    fine = Mesh(mesh.devices.reshape(2, 2, 4, 8, 2), ALL)
    placed = (P(DP, VOCAB), P(VOCAB, None), P(DP), P(ALL), P(ALL, None))
    return jax.shard_map(
        inner,
        mesh=fine,
        in_specs=placed,
        out_specs=(P(DP), P(DP, VOCAB), P(VOCAB, DP)),
        check_vma=False,
    )
```

```python
import functools

import jax
import jax.numpy as jnp
from jax import lax
from jax.experimental import pallas as pl
from jax.experimental.pallas import tpu as pltpu
from jax.sharding import Mesh, PartitionSpec as P

BF16 = jnp.bfloat16
F32 = jnp.float32
I32 = jnp.int32
ALL = ("xh", "c", "y", "z", "xl")
DP = ("xh", "c")
VOCAB = ("y", "z", "xl")
PLANE = ("y", "xl")
CHUNK = 400
DEPTH = 3
PARAMS = pltpu.CompilerParams(vmem_limit_bytes=16 * 1024 * 1024)
SIDE = pltpu.CompilerParams(vmem_limit_bytes=57 * 1024 * 1024)
WIDE = pltpu.CompilerParams(vmem_limit_bytes=63 * 1024 * 1024)
FULL = pltpu.CompilerParams(vmem_limit_bytes=62 * 1024 * 1024)


def exchange(pieces, axes):
    return lax.all_to_all(pieces, axes, 0, 0, tiled=True)


def to_each(value, count):
    return jnp.broadcast_to(value, (count, *value.shape))


def swap(value, axis):
    return lax.ppermute(value, axis, [(0, 1), (1, 0)])


def cost(flops, moved, special=0):
    return pl.CostEstimate(flops=flops, bytes_accessed=moved, transcendentals=special)


def partner(value, bit):
    size = lax.axis_size("z")
    return lax.ppermute(value, "z", [(i, i ^ bit) for i in range(size)])


def join_kernel(one, middle, r1, c0, *outs):
    for k, out in enumerate(outs):
        source, at = ((one, 0), (middle, 0), (middle, 128))[k]
        out[0:128, :] = source[at : at + 128, :]
        out[128:256, :] = r1[128 * (k + 1) : 128 * (k + 2), :]
        out[256:272, :] = c0[...]
        out[272:288, :] = r1[512:528, :]


def join_call(one, middle, r1, c0):
    return pl.pallas_call(
        join_kernel,
        out_shape=[jax.ShapeDtypeStruct((288, 256), BF16)] * 3,
        compiler_params=PARAMS,
        cost_estimate=cost(10**6, 2**19),
        name="join",
    )(one, middle, r1, c0)


def select_kernel(vocab_rows, where_ref, *refs):
    packs = refs[:4]
    outs = refs[4:]
    count = packs[0].shape[0] - 8
    total = 4 * count
    line = jnp.concatenate(
        [
            p[count : count + 8, 0:128].astype(F32)[:, 0:count]
            for p in packs
        ],
        axis=1,
    )
    line = line[0:1, :] * 16384.0 + line[1:2, :] * 128.0 + line[2:3, :]
    tall = jnp.broadcast_to(line, (8, total)).T[:, 0:1]

    def parts(ids):
        owner = jnp.floor((ids + 0.5) * (1.0 / vocab_rows))
        spot = (ids - owner * vocab_rows).astype(I32) + 1
        owner = owner.astype(I32)
        plane = (owner >> 4) * 2 + (owner & 1)
        turn = ((owner >> 1) & 7) ^ where_ref[3]
        return owner, plane, turn, spot

    owner, plane, turn, _ = parts(line)
    owner_t, plane_t, turn_t, spot_t = parts(tall)
    early = lax.broadcasted_iota(I32, (total, total), 0)
    later = lax.broadcasted_iota(I32, (total, total), 1)
    before = (owner_t == owner) & (early < later) & ((early >> 6) == (later >> 6))
    rank = jnp.sum(jnp.where(before, 1.0, 0.0), axis=0, keepdims=True).astype(I32)
    token = lax.broadcasted_iota(I32, (1, total), 1)
    row = (token >> 6) * 2 + rank
    slots = turn * 64 + plane * 8 + row
    chosen = lax.broadcasted_iota(I32, (512, total), 0) == slots
    cot = jnp.concatenate([p[0:count, :] for p in packs], axis=0)
    picked = jnp.dot(jnp.where(chosen, 1.0, 0.0).astype(BF16), cot, preferred_element_type=F32)
    lane = lax.broadcasted_iota(I32, (total, 128), 1)
    base = turn_t * 16 + plane_t
    digits = jnp.where(lane == base, spot_t >> 6, jnp.where(lane == base + 8, spot_t & 63, 0))
    mark = lax.broadcasted_iota(I32, (16, total), 0) == row
    code = jnp.dot(
        jnp.where(mark, 1.0, 0.0).astype(BF16),
        digits.astype(F32).astype(BF16),
        preferred_element_type=F32,
    )
    code = jnp.concatenate([code, jnp.zeros((16, 128), F32)], axis=1).astype(BF16)
    far, middle, one, own, mine = outs
    for q in range(8):
        out, at = ((own, 0), (one, 0), (middle, 0), (middle, 128))[q] if q < 4 else (far, (q - 4) * 128)
        for p in range(8):
            piece = picked[q * 64 + p * 8 : q * 64 + p * 8 + 8, :]
            piece = jnp.concatenate([piece[:, 0:256], piece[:, 256:512]], axis=0)
            out[at + p * 16 : at + p * 16 + 16, :] = piece.astype(BF16)
    far[512:528, :] = code
    mine[...] = code


def select_call(where, packs, vocab_rows):
    rows, wide = packs[0].shape
    block = wide // 2
    sizes = (528, 256, 128, 128, 16)
    return pl.pallas_call(
        functools.partial(select_kernel, vocab_rows),
        grid_spec=pltpu.PrefetchScalarGridSpec(
            num_scalar_prefetch=1,
            grid=(1,),
            in_specs=[pl.BlockSpec((rows, block), lambda i, s: (0, s[2]))] * 4,
            out_specs=[pl.BlockSpec((n, 256), lambda i, s: (0, 0)) for n in sizes],
        ),
        out_shape=[jax.ShapeDtypeStruct((n, 256), BF16) for n in sizes],
        compiler_params=PARAMS,
        cost_estimate=cost(2 * 512 * 256 * block, 2**20),
        name="select",
    )(where, *packs)


def logits_kernel(
    where_ref, tgt_ref, got_ref, table_ref, pack_ref, stats_ref, own_ref, hid, tab, buf, sems, out_sems
):
    count, width = tab.shape
    tokens = hid.shape[1]
    half = width // 2
    plane, depth, _ = got_ref.shape
    chunks = count // CHUNK

    def load(i):
        at = pl.ds(pl.multiple_of(i * CHUNK, CHUNK), CHUNK)
        return pltpu.make_async_copy(table_ref.at[at], tab.at[at], sems.at[i])

    def store(i):
        at = pl.ds(pl.multiple_of(i * CHUNK, CHUNK), CHUNK)
        return pltpu.make_async_copy(buf.at[at], pack_ref.at[at], out_sems.at[i])

    for i in range(DEPTH):
        load(i).start()
    for p in range(plane):
        y, x = p // 2, p % 2
        for z in range(depth // 32):
            at = ((y * (depth // 32) + z) * 2 + x) * 32
            hid[at : at + 32, :] = got_ref[p, z * 32 : z * 32 + 32, :]
    base = buf.shape[0] - half
    buf[base:, :] = hid[pl.ds(pl.multiple_of(where_ref[1] * half, half), half), :]
    at = pl.ds(base, half)
    side = pltpu.make_async_copy(buf.at[at], pack_ref.at[at], out_sems.at[chunks])
    side.start()
    own_ref[...] = jnp.zeros(own_ref.shape, F32)

    def one(i, carry):
        top, total, picked = carry
        load(i).wait()

        @pl.when(i + DEPTH < chunks)
        def _():
            load(i + DEPTH).start()

        at = pl.ds(pl.multiple_of(i * CHUNK, CHUNK), CHUNK)
        values = jnp.dot(tab[at, :], hid[...], preferred_element_type=F32)
        index = lax.broadcasted_iota(I32, values.shape, 0) + (where_ref[0] + i * CHUNK)
        picked += jnp.sum(jnp.where(index == tgt_ref[...], values, 0.0), axis=0, keepdims=True)
        peak = jnp.max(values, axis=0, keepdims=True)
        e = jnp.exp(values - peak)
        buf[at, :] = e.astype(BF16)
        store(i).start()
        own_ref[pl.ds(i, 1), :] = peak
        higher = jnp.maximum(top, peak)
        total = total * jnp.exp(top - higher)
        total += jnp.sum(e, axis=0, keepdims=True) * jnp.exp(peak - higher)
        return higher, total, picked

    blank = jnp.zeros((1, tokens), F32)
    start = (jnp.full((1, tokens), -jnp.inf, F32), blank, blank)
    line = jnp.concatenate([*lax.fori_loop(0, chunks, one, start), blank], axis=0)
    stats_ref[...] = jnp.broadcast_to(line[None], stats_ref.shape)
    side.wait()

    def end(i, carry):
        store(i).wait()
        return carry

    lax.fori_loop(0, chunks, end, 0)


def logits_call(where, targets, got, table, copies):
    count, width = table.shape
    tokens = got.shape[2]
    span = 2048 + width // 2
    whole = pl.BlockSpec(memory_space=pltpu.VMEM)
    return pl.pallas_call(
        logits_kernel,
        in_specs=[pl.BlockSpec(memory_space=pltpu.SMEM), whole, whole, pl.BlockSpec(memory_space=pl.ANY)],
        out_specs=[pl.BlockSpec(memory_space=pltpu.HBM), whole, whole],
        scratch_shapes=[
            pltpu.VMEM((width, tokens), BF16),
            pltpu.VMEM((count, width), BF16),
            pltpu.VMEM((span, tokens), BF16),
            pltpu.SemaphoreType.DMA((count // CHUNK,)),
            pltpu.SemaphoreType.DMA((count // CHUNK + 1,)),
        ],
        out_shape=[
            pltpu.HBM((span, tokens), BF16),
            jax.ShapeDtypeStruct((copies, 4, tokens), F32),
            jax.ShapeDtypeStruct((8, tokens), F32),
        ],
        compiler_params=WIDE,
        cost_estimate=cost(2 * count * width * tokens, 2 * count * width + 4 * span * tokens),
        name="logits",
    )(where, targets, got, table)


QUOTA = (0, 4, 1, 5, 2, 6, 3, 7)


def part_kernel(
    where_ref, tgt_ref, own_ref, stats_ref, near_ref, x0, r1, p1, p2, p3, c0, table_ref,
    out_ref, loss_ref, w_ref, lhs, tab, buf, sems, out_sems,
):
    tokens = tgt_ref.shape[1]
    count, width = table_ref.shape
    plane = buf.shape[0]
    depth = width // plane
    turns, _, wide = tab.shape

    def load(j):
        at = table_ref.at[:, pl.ds(pl.multiple_of(j * wide, wide), wide)]
        return pltpu.make_async_copy(at, tab.at[j], sems.at[j])

    def store(j):
        at = pl.ds(j * 2, 2)
        return pltpu.make_async_copy(buf.at[at], out_ref.at[at], out_sems.at[j])

    for j in range(DEPTH):
        load(j).start()

    stats = stats_ref[...]
    top = jnp.max(stats, axis=0)[0:1, :]
    sums = jnp.sum(stats[:, 1:2, :] * jnp.exp(stats[:, 0:1, :] - top[None]), axis=0)
    picks = jnp.sum(stats, axis=0)[2:3, :]
    loss_ref[...] = top + jnp.log(sums) - picks
    chunks = count // CHUNK
    w = jnp.exp(own_ref[0:chunks, :] - top) / sums
    w_ref[...] = jnp.concatenate(
        [w, tgt_ref[...].astype(F32), jnp.zeros((7 - chunks, tokens), F32)], axis=0
    )
    for i in range(chunks):
        index = lax.broadcasted_iota(I32, (CHUNK, tokens), 0) + (where_ref[0] + i * CHUNK)
        e = near_ref[i * CHUNK : (i + 1) * CHUNK, :].astype(F32)
        residual = e * w[i : i + 1, :] - jnp.where(index == tgt_ref[...], 1.0, 0.0)
        lhs[i * CHUNK : (i + 1) * CHUNK, :] = residual.astype(BF16)

    marks = [c0[...], r1[512:528, :]]
    marks += [ref[k : k + 16, :] for ref in (p1, p2, p3) for k in (256, 272)]
    group = lax.broadcasted_iota(I32, (16, tokens), 1) >> 4
    mixed = jnp.zeros((16, tokens), F32)
    for q, mark in zip(QUOTA, marks):
        mixed += jnp.where(group == q, mark.astype(F32), 0.0)
    pieces = ((x0, 0), (r1, 0), (p1, 0), (p1, 128), (p2, 0), (p2, 128), (p3, 0), (p3, 128))
    for p in range(plane):
        for i, (ref, at) in enumerate(pieces):
            to = depth + 16 * i
            buf[p, to : to + 16, :] = ref[at + p * 16 : at + p * 16 + 16, :]
        buf[p, depth + 128 : depth + 144, :] = mixed.astype(BF16)

    def one(j, carry):
        load(j).wait()

        @pl.when(j + DEPTH < turns)
        def _():
            load(j + DEPTH).start()

        part = lax.dot_general(
            tab[j], lhs[...], (((0,), (0,)), ((), ())), preferred_element_type=F32
        )
        for k in range(wide // 32):
            z, x = k // 2, k % 2
            buf[j * 2 + x, z * 32 : z * 32 + 32, :] = part[k * 32 : k * 32 + 32, :].astype(BF16)
        store(j).start()
        return carry

    lax.fori_loop(0, turns, one, 0)

    def end(j, carry):
        store(j).wait()
        return carry

    lax.fori_loop(0, turns, end, 0)


def part_call(where, targets, own, stats, near, riders, table):
    count, width = table.shape
    tokens = targets.shape[1]
    plane, wide = 8, 512
    whole = pl.BlockSpec(memory_space=pltpu.VMEM)
    anywhere = pl.BlockSpec(memory_space=pl.ANY)
    shape = (plane, width // plane + 144, tokens)
    return pl.pallas_call(
        part_kernel,
        in_specs=[pl.BlockSpec(memory_space=pltpu.SMEM), *[whole] * 10, anywhere],
        out_specs=[pl.BlockSpec(memory_space=pltpu.HBM), whole, whole],
        scratch_shapes=[
            pltpu.VMEM((count, tokens), BF16),
            pltpu.VMEM((width // wide, count, wide), BF16),
            pltpu.VMEM(shape, BF16),
            pltpu.SemaphoreType.DMA((width // wide,)),
            pltpu.SemaphoreType.DMA((plane // 2,)),
        ],
        out_shape=[
            pltpu.HBM(shape, BF16),
            jax.ShapeDtypeStruct((1, tokens), F32),
            jax.ShapeDtypeStruct((8, tokens), F32),
        ],
        compiler_params=FULL,
        cost_estimate=cost(2 * count * width * tokens, 2 * count * width + 2 * width * tokens),
        name="part",
    )(where, targets, own, stats, near, *riders, table)


def table_kernel(where_ref, w_ref, got_ref, *refs):
    out_ref, rows, place = refs[-3:]
    count = out_ref.shape[0]
    first = pl.program_id(0) * count

    @pl.when(pl.program_id(0) == 0)
    def _():
        plane = got_ref.shape[0]
        depth = got_ref.shape[1] - 144
        slots = rows.shape[0]
        mark = lax.broadcasted_iota(I32, (128, slots), 0)
        lane = lax.broadcasted_iota(I32, (128, slots), 1)
        i = (lane >> 3) & 7
        quota = ((i & 1) << 2) | (i >> 1)
        at = quota * 16 + where_ref[4]
        digit = jnp.where(mark == at, 64.0, jnp.where(mark == at + 8, 1.0, 0.0))
        found = jnp.zeros((16, slots), F32)
        for p in range(plane):
            for k in range(0, 8, 2):
                a = got_ref[p, depth + 16 * k : depth + 16 * k + 16, :].astype(F32)
                b = got_ref[p, depth + 16 * k + 16 : depth + 16 * k + 32, :].astype(F32)
                to = p * 64 + k * 8
                rows[to : to + 16, 0:256] = jnp.concatenate([a[0:8], b[0:8]], axis=0).astype(BF16)
                rows[to : to + 16, 256:512] = jnp.concatenate([a[8:16], b[8:16]], axis=0).astype(BF16)
            code = got_ref[p, depth + 128 : depth + 144, 0:128]
            these = jnp.where((lane >> 6) == p, digit, 0.0).astype(BF16)
            found += jnp.dot(code, these, preferred_element_type=F32)
        mine = lax.broadcasted_iota(I32, (16, slots), 0) == (
            lax.broadcasted_iota(I32, (16, slots), 1) & 7
        )
        spot = jnp.sum(jnp.where(mine, found, 0.0), axis=0, keepdims=True) - 1.0
        place[...] = jnp.broadcast_to(spot, place.shape).astype(I32)

    near = lax.broadcasted_iota(I32, (count, 256), 0) + (first + where_ref[0])
    spots = lax.broadcasted_iota(I32, (count, place.shape[1]), 0) + first
    match = jnp.where(spots == place[0:1, :], 1.0, 0.0).astype(BF16)
    total = jnp.dot(match, rows[...], preferred_element_type=F32)
    for g in range(4):
        e = refs[2 * g][...].astype(F32)
        w = w_ref[g, pl.ds(pl.program_id(0), 1), :]
        target = w_ref[g, 5:6, :].astype(I32)
        res = (e * w - jnp.where(near == target, 1.0, 0.0)).astype(BF16)
        total += lax.dot_general(
            res, refs[2 * g + 1][...], (((1,), (1,)), ((), ())), preferred_element_type=F32
        )
    out_ref[...] = total.astype(BF16)


def table_call(where, w, got, packs, count):
    tokens = packs[0].shape[1]
    block = 512
    specs, operands = [], []
    for pack in packs:
        specs.append(pl.BlockSpec((CHUNK, tokens), lambda i, s: (i, 0)))
        specs.append(pl.BlockSpec((block, tokens), lambda i, s: (4 + s[2], 0)))
        operands += [pack, pack]
    return pl.pallas_call(
        table_kernel,
        grid_spec=pltpu.PrefetchScalarGridSpec(
            num_scalar_prefetch=1,
            grid=(count // CHUNK,),
            in_specs=[
                pl.BlockSpec(w.shape, lambda i, s: (0, 0, 0)),
                pl.BlockSpec(got.shape, lambda i, s: (0, 0, 0)),
                *specs,
            ],
            out_specs=pl.BlockSpec((CHUNK, block), lambda i, s: (i, 0)),
            scratch_shapes=[pltpu.VMEM((512, block), BF16), pltpu.VMEM((8, 512), I32)],
        ),
        out_shape=jax.ShapeDtypeStruct((count, block), BF16),
        compiler_params=SIDE,
        cost_estimate=cost(2 * count * block * 1536, 8 * count * 256 + 2 * count * block),
        name="table_grad",
    )(where, w, got, *operands)


def inner(hidden, table, targets, input_ids, cotangent):
    vocab_rows, width = table.shape
    ny, nz, nx = (lax.axis_size(a) for a in VOCAB)
    plane = ny * nx
    vocab_count = plane * nz
    block = width // lax.axis_size(DP)
    xh, c = lax.axis_index("xh"), lax.axis_index("c")
    spot = lax.axis_index("y") * nx + lax.axis_index("xl")
    where = jnp.stack([lax.axis_index(VOCAB) * vocab_rows, xh, c, lax.axis_index("z"), spot]).astype(I32)
    tokens = hidden.shape[0]
    goal = targets.reshape(1, tokens)

    half = width // 2
    ids = jnp.stack([input_ids >> 14, (input_ids >> 7) & 127, input_ids & 127]).astype(BF16)
    ids = jnp.pad(ids, ((0, 5), (0, block - ids.shape[1])))
    ids = jnp.concatenate([ids, ids], axis=1)
    near_rows = lax.dynamic_slice_in_dim(cotangent, xh * half, half, 1)
    far_rows = lax.dynamic_slice_in_dim(cotangent, (1 - xh) * half, half, 1)
    near_rows = jnp.concatenate([near_rows, ids], axis=0)
    far_rows = jnp.concatenate([far_rows, ids], axis=0)
    far_rows = swap(far_rows, "xh")
    packs = (near_rows, swap(near_rows, "c"), far_rows, swap(far_rows, "c"))
    away, middle, one, x0, c0 = select_call(where, packs, vocab_rows)
    r1 = partner(away, 4)
    sent = join_call(one, middle, r1, c0)
    got1, got2, got3 = (partner(value, k + 1) for k, value in enumerate(sent))

    mine = hidden.T
    stage = exchange(to_each(mine, nz), "z").reshape(-1, tokens)
    stage = exchange(to_each(stage, plane), PLANE)
    far_stage = swap(stage, "xh")
    near, sums, own = logits_call(where, goal, stage, table, vocab_count)

    stats = exchange(sums, VOCAB)
    far, _, _ = logits_call(where, goal, far_stage, table, 1)
    near_sib = swap(near, "c")
    far_sib = swap(far, "c")
    part, loss, w = part_call(where, goal, own, stats, near, (x0, r1, got1, got2, got3, c0), table)

    got = exchange(part, PLANE)
    part = jnp.sum(got[:, : width // plane].astype(F32), axis=0).reshape(nz, -1, tokens)
    part = jnp.sum(exchange(part, "z"), axis=0)
    hidden_grad = part.astype(BF16).T

    w_far = swap(w, "xh")
    w_all = jnp.stack([w, swap(w, "c"), w_far, swap(w_far, "c")])
    table_grad = table_call(
        where, w_all, got, (near, near_sib, far, far_sib), vocab_rows
    )
    return loss.reshape(tokens), hidden_grad, table_grad


def solution(mesh):
    fine = Mesh(mesh.devices.reshape(2, 2, 4, 8, 2), ALL)
    placed = (P(DP, VOCAB), P(VOCAB, None), P(DP), P(ALL), P(ALL, None))
    return jax.shard_map(
        inner,
        mesh=fine,
        in_specs=placed,
        out_specs=(P(DP), P(DP, VOCAB), P(VOCAB, DP)),
        check_vma=False,
    )
```

```python
import functools

import jax
import jax.numpy as jnp
from jax import lax
from jax.experimental import pallas as pl
from jax.experimental.pallas import tpu as pltpu
from jax.sharding import Mesh, PartitionSpec as P

BF16 = jnp.bfloat16
F32 = jnp.float32
I32 = jnp.int32
ALL = ("xh", "c", "y", "z", "xl")
DP = ("xh", "c")
VOCAB = ("y", "z", "xl")
PLANE = ("y", "xl")
CHUNK = 400
DEPTH = 3
PARAMS = pltpu.CompilerParams(vmem_limit_bytes=16 * 1024 * 1024)
SIDE = pltpu.CompilerParams(vmem_limit_bytes=16 * 1024 * 1024)
WIDE = pltpu.CompilerParams(vmem_limit_bytes=63 * 1024 * 1024)
FULL = pltpu.CompilerParams(vmem_limit_bytes=62 * 1024 * 1024)


def exchange(pieces, axes):
    return lax.all_to_all(pieces, axes, 0, 0, tiled=True)


def to_each(value, count):
    return jnp.broadcast_to(value, (count, *value.shape))


def swap(value, axis):
    return lax.ppermute(value, axis, [(0, 1), (1, 0)])


def cost(flops, moved, special=0):
    return pl.CostEstimate(flops=flops, bytes_accessed=moved, transcendentals=special)


def partner(value, bit):
    size = lax.axis_size("z")
    return lax.ppermute(value, "z", [(i, i ^ bit) for i in range(size)])


def join_kernel(one, middle, r1, c0, *outs):
    for k, out in enumerate(outs):
        source, at = ((one, 0), (middle, 0), (middle, 128))[k]
        out[0:128, :] = source[at : at + 128, :]
        out[128:256, :] = r1[128 * (k + 1) : 128 * (k + 2), :]
        out[256:272, :] = c0[...]
        out[272:288, :] = r1[512:528, :]


def join_call(one, middle, r1, c0):
    return pl.pallas_call(
        join_kernel,
        out_shape=[jax.ShapeDtypeStruct((288, 256), BF16)] * 3,
        compiler_params=PARAMS,
        cost_estimate=cost(10**6, 2**19),
        name="join",
    )(one, middle, r1, c0)


def select_kernel(vocab_rows, where_ref, *refs):
    packs = refs[:4]
    outs = refs[4:]
    count = packs[0].shape[0] - 8
    total = 4 * count
    line = jnp.concatenate(
        [
            p[count : count + 8, 0:128].astype(F32)[:, 0:count]
            for p in packs
        ],
        axis=1,
    )
    line = line[0:1, :] * 16384.0 + line[1:2, :] * 128.0 + line[2:3, :]
    tall = jnp.broadcast_to(line, (8, total)).T[:, 0:1]

    def parts(ids):
        owner = jnp.floor((ids + 0.5) * (1.0 / vocab_rows))
        spot = (ids - owner * vocab_rows).astype(I32) + 1
        owner = owner.astype(I32)
        plane = (owner >> 4) * 2 + (owner & 1)
        turn = ((owner >> 1) & 7) ^ where_ref[3]
        return owner, plane, turn, spot

    owner, plane, turn, _ = parts(line)
    owner_t, plane_t, turn_t, spot_t = parts(tall)
    early = lax.broadcasted_iota(I32, (total, total), 0)
    later = lax.broadcasted_iota(I32, (total, total), 1)
    before = (owner_t == owner) & (early < later) & ((early >> 6) == (later >> 6))
    rank = jnp.sum(jnp.where(before, 1.0, 0.0), axis=0, keepdims=True).astype(I32)
    token = lax.broadcasted_iota(I32, (1, total), 1)
    row = (token >> 6) * 2 + rank
    slots = turn * 64 + plane * 8 + row
    chosen = lax.broadcasted_iota(I32, (512, total), 0) == slots
    cot = jnp.concatenate([p[0:count, :] for p in packs], axis=0)
    picked = jnp.dot(jnp.where(chosen, 1.0, 0.0).astype(BF16), cot, preferred_element_type=F32)
    lane = lax.broadcasted_iota(I32, (total, 128), 1)
    base = turn_t * 16 + plane_t
    digits = jnp.where(lane == base, spot_t >> 6, jnp.where(lane == base + 8, spot_t & 63, 0))
    mark = lax.broadcasted_iota(I32, (16, total), 0) == row
    code = jnp.dot(
        jnp.where(mark, 1.0, 0.0).astype(BF16),
        digits.astype(F32).astype(BF16),
        preferred_element_type=F32,
    )
    code = jnp.concatenate([code, jnp.zeros((16, 128), F32)], axis=1).astype(BF16)
    far, middle, one, own, mine = outs
    for q in range(8):
        out, at = ((own, 0), (one, 0), (middle, 0), (middle, 128))[q] if q < 4 else (far, (q - 4) * 128)
        for p in range(8):
            piece = picked[q * 64 + p * 8 : q * 64 + p * 8 + 8, :]
            piece = jnp.concatenate([piece[:, 0:256], piece[:, 256:512]], axis=0)
            out[at + p * 16 : at + p * 16 + 16, :] = piece.astype(BF16)
    far[512:528, :] = code
    mine[...] = code


def select_call(where, packs, vocab_rows):
    rows, wide = packs[0].shape
    block = wide // 2
    sizes = (528, 256, 128, 128, 16)
    return pl.pallas_call(
        functools.partial(select_kernel, vocab_rows),
        grid_spec=pltpu.PrefetchScalarGridSpec(
            num_scalar_prefetch=1,
            grid=(1,),
            in_specs=[pl.BlockSpec((rows, block), lambda i, s: (0, s[2]))] * 4,
            out_specs=[pl.BlockSpec((n, 256), lambda i, s: (0, 0)) for n in sizes],
        ),
        out_shape=[jax.ShapeDtypeStruct((n, 256), BF16) for n in sizes],
        compiler_params=PARAMS,
        cost_estimate=cost(2 * 512 * 256 * block, 2**20),
        name="select",
    )(where, *packs)


def logits_kernel(
    where_ref, tgt_ref, got_ref, table_ref, pack_ref, stats_ref, own_ref, hid, tab, buf, sems, out_sems
):
    count, width = tab.shape
    tokens = hid.shape[1]
    half = width // 2
    plane, depth, _ = got_ref.shape
    chunks = count // CHUNK

    def load(i):
        at = pl.ds(pl.multiple_of(i * CHUNK, CHUNK), CHUNK)
        return pltpu.make_async_copy(table_ref.at[at], tab.at[at], sems.at[i])

    def store(i):
        at = pl.ds(pl.multiple_of(i * CHUNK, CHUNK), CHUNK)
        return pltpu.make_async_copy(buf.at[at], pack_ref.at[at], out_sems.at[i])

    for i in range(DEPTH):
        load(i).start()
    for p in range(plane):
        y, x = p // 2, p % 2
        for z in range(depth // 32):
            at = ((y * (depth // 32) + z) * 2 + x) * 32
            hid[at : at + 32, :] = got_ref[p, z * 32 : z * 32 + 32, :]
    base = buf.shape[0] - half
    buf[base:, :] = hid[pl.ds(pl.multiple_of(where_ref[1] * half, half), half), :]
    at = pl.ds(base, half)
    side = pltpu.make_async_copy(buf.at[at], pack_ref.at[at], out_sems.at[chunks])
    side.start()
    own_ref[...] = jnp.zeros(own_ref.shape, F32)

    def one(i, carry):
        top, total, picked = carry
        load(i).wait()

        @pl.when(i + DEPTH < chunks)
        def _():
            load(i + DEPTH).start()

        at = pl.ds(pl.multiple_of(i * CHUNK, CHUNK), CHUNK)
        values = jnp.dot(tab[at, :], hid[...], preferred_element_type=F32)
        index = lax.broadcasted_iota(I32, values.shape, 0) + (where_ref[0] + i * CHUNK)
        picked += jnp.sum(jnp.where(index == tgt_ref[...], values, 0.0), axis=0, keepdims=True)
        peak = jnp.max(values, axis=0, keepdims=True)
        e = jnp.exp(values - peak)
        buf[at, :] = e.astype(BF16)
        store(i).start()
        own_ref[pl.ds(i, 1), :] = peak
        higher = jnp.maximum(top, peak)
        total = total * jnp.exp(top - higher)
        total += jnp.sum(e, axis=0, keepdims=True) * jnp.exp(peak - higher)
        return higher, total, picked

    blank = jnp.zeros((1, tokens), F32)
    start = (jnp.full((1, tokens), -jnp.inf, F32), blank, blank)
    line = jnp.concatenate([*lax.fori_loop(0, chunks, one, start), blank], axis=0)
    stats_ref[...] = jnp.broadcast_to(line[None], stats_ref.shape)
    side.wait()

    def end(i, carry):
        store(i).wait()
        return carry

    lax.fori_loop(0, chunks, end, 0)


def logits_call(where, targets, got, table, copies):
    count, width = table.shape
    tokens = got.shape[2]
    span = 2048 + width // 2
    whole = pl.BlockSpec(memory_space=pltpu.VMEM)
    return pl.pallas_call(
        logits_kernel,
        in_specs=[pl.BlockSpec(memory_space=pltpu.SMEM), whole, whole, pl.BlockSpec(memory_space=pl.ANY)],
        out_specs=[pl.BlockSpec(memory_space=pltpu.HBM), whole, whole],
        scratch_shapes=[
            pltpu.VMEM((width, tokens), BF16),
            pltpu.VMEM((count, width), BF16),
            pltpu.VMEM((span, tokens), BF16),
            pltpu.SemaphoreType.DMA((count // CHUNK,)),
            pltpu.SemaphoreType.DMA((count // CHUNK + 1,)),
        ],
        out_shape=[
            pltpu.HBM((span, tokens), BF16),
            jax.ShapeDtypeStruct((copies, 4, tokens), F32),
            jax.ShapeDtypeStruct((8, tokens), F32),
        ],
        compiler_params=WIDE,
        cost_estimate=cost(2 * count * width * tokens, 2 * count * width + 4 * span * tokens),
        name="logits",
    )(where, targets, got, table)


QUOTA = (0, 4, 1, 5, 2, 6, 3, 7)


def part_kernel(
    where_ref, tgt_ref, own_ref, stats_ref, near_ref, x0, r1, p1, p2, p3, c0, table_ref,
    out_ref, loss_ref, w_ref, lhs, tab, buf, sems, out_sems,
):
    tokens = tgt_ref.shape[1]
    count, width = table_ref.shape
    plane = buf.shape[0]
    depth = width // plane
    turns, _, wide = tab.shape

    def load(j):
        at = table_ref.at[:, pl.ds(pl.multiple_of(j * wide, wide), wide)]
        return pltpu.make_async_copy(at, tab.at[j], sems.at[j])

    def store(j):
        at = pl.ds(j * 2, 2)
        return pltpu.make_async_copy(buf.at[at], out_ref.at[at], out_sems.at[j])

    for j in range(DEPTH):
        load(j).start()

    stats = stats_ref[...]
    top = jnp.max(stats, axis=0)[0:1, :]
    sums = jnp.sum(stats[:, 1:2, :] * jnp.exp(stats[:, 0:1, :] - top[None]), axis=0)
    picks = jnp.sum(stats, axis=0)[2:3, :]
    loss_ref[...] = top + jnp.log(sums) - picks
    chunks = count // CHUNK
    w = jnp.exp(own_ref[0:chunks, :] - top) / sums
    w_ref[...] = jnp.concatenate(
        [w, tgt_ref[...].astype(F32), jnp.zeros((7 - chunks, tokens), F32)], axis=0
    )
    for i in range(chunks):
        index = lax.broadcasted_iota(I32, (CHUNK, tokens), 0) + (where_ref[0] + i * CHUNK)
        e = near_ref[i * CHUNK : (i + 1) * CHUNK, :].astype(F32)
        residual = e * w[i : i + 1, :] - jnp.where(index == tgt_ref[...], 1.0, 0.0)
        lhs[i * CHUNK : (i + 1) * CHUNK, :] = residual.astype(BF16)

    marks = [c0[...], r1[512:528, :]]
    marks += [ref[k : k + 16, :] for ref in (p1, p2, p3) for k in (256, 272)]
    group = lax.broadcasted_iota(I32, (16, tokens), 1) >> 4
    mixed = jnp.zeros((16, tokens), F32)
    for q, mark in zip(QUOTA, marks):
        mixed += jnp.where(group == q, mark.astype(F32), 0.0)
    pieces = ((x0, 0), (r1, 0), (p1, 0), (p1, 128), (p2, 0), (p2, 128), (p3, 0), (p3, 128))
    for p in range(plane):
        for i, (ref, at) in enumerate(pieces):
            to = depth + 16 * i
            buf[p, to : to + 16, :] = ref[at + p * 16 : at + p * 16 + 16, :]
        buf[p, depth + 128 : depth + 144, :] = mixed.astype(BF16)

    def one(j, carry):
        load(j).wait()

        @pl.when(j + DEPTH < turns)
        def _():
            load(j + DEPTH).start()

        part = lax.dot_general(
            tab[j], lhs[...], (((0,), (0,)), ((), ())), preferred_element_type=F32
        )
        for k in range(wide // 32):
            z, x = k // 2, k % 2
            buf[j * 2 + x, z * 32 : z * 32 + 32, :] = part[k * 32 : k * 32 + 32, :].astype(BF16)
        store(j).start()
        return carry

    lax.fori_loop(0, turns, one, 0)

    def end(j, carry):
        store(j).wait()
        return carry

    lax.fori_loop(0, turns, end, 0)


def part_call(where, targets, own, stats, near, riders, table):
    count, width = table.shape
    tokens = targets.shape[1]
    plane, wide = 8, 512
    whole = pl.BlockSpec(memory_space=pltpu.VMEM)
    anywhere = pl.BlockSpec(memory_space=pl.ANY)
    shape = (plane, width // plane + 144, tokens)
    return pl.pallas_call(
        part_kernel,
        in_specs=[pl.BlockSpec(memory_space=pltpu.SMEM), *[whole] * 10, anywhere],
        out_specs=[pl.BlockSpec(memory_space=pltpu.HBM), whole, whole],
        scratch_shapes=[
            pltpu.VMEM((count, tokens), BF16),
            pltpu.VMEM((width // wide, count, wide), BF16),
            pltpu.VMEM(shape, BF16),
            pltpu.SemaphoreType.DMA((width // wide,)),
            pltpu.SemaphoreType.DMA((plane // 2,)),
        ],
        out_shape=[
            pltpu.HBM(shape, BF16),
            jax.ShapeDtypeStruct((1, tokens), F32),
            jax.ShapeDtypeStruct((8, tokens), F32),
        ],
        compiler_params=FULL,
        cost_estimate=cost(2 * count * width * tokens, 2 * count * width + 2 * width * tokens),
        name="part",
    )(where, targets, own, stats, near, *riders, table)


def table_kernel(where_ref, w_ref, got_ref, *refs):
    out_ref, rows, place = refs[-3:]
    count = out_ref.shape[0]
    first = pl.program_id(0) * count

    @pl.when(pl.program_id(0) == 0)
    def _():
        plane = got_ref.shape[0]
        depth = got_ref.shape[1] - 144
        slots = rows.shape[0]
        mark = lax.broadcasted_iota(I32, (128, slots), 0)
        lane = lax.broadcasted_iota(I32, (128, slots), 1)
        i = (lane >> 3) & 7
        quota = ((i & 1) << 2) | (i >> 1)
        at = quota * 16 + where_ref[4]
        digit = jnp.where(mark == at, 64.0, jnp.where(mark == at + 8, 1.0, 0.0))
        found = jnp.zeros((16, slots), F32)
        for p in range(plane):
            for k in range(0, 8, 2):
                a = got_ref[p, depth + 16 * k : depth + 16 * k + 16, :].astype(F32)
                b = got_ref[p, depth + 16 * k + 16 : depth + 16 * k + 32, :].astype(F32)
                to = p * 64 + k * 8
                rows[to : to + 16, 0:256] = jnp.concatenate([a[0:8], b[0:8]], axis=0).astype(BF16)
                rows[to : to + 16, 256:512] = jnp.concatenate([a[8:16], b[8:16]], axis=0).astype(BF16)
            code = got_ref[p, depth + 128 : depth + 144, 0:128]
            these = jnp.where((lane >> 6) == p, digit, 0.0).astype(BF16)
            found += jnp.dot(code, these, preferred_element_type=F32)
        mine = lax.broadcasted_iota(I32, (16, slots), 0) == (
            lax.broadcasted_iota(I32, (16, slots), 1) & 7
        )
        spot = jnp.sum(jnp.where(mine, found, 0.0), axis=0, keepdims=True) - 1.0
        place[...] = jnp.broadcast_to(spot, place.shape).astype(I32)

    near = lax.broadcasted_iota(I32, (count, 256), 0) + (first + where_ref[0])
    spots = lax.broadcasted_iota(I32, (count, place.shape[1]), 0) + first
    match = jnp.where(spots == place[0:1, :], 1.0, 0.0).astype(BF16)
    total = jnp.dot(match, rows[...], preferred_element_type=F32)
    for g in range(4):
        e = refs[2 * g][...].astype(F32)
        w = w_ref[g, pl.ds(pl.program_id(0), 1), :]
        target = w_ref[g, 5:6, :].astype(I32)
        res = (e * w - jnp.where(near == target, 1.0, 0.0)).astype(BF16)
        total += lax.dot_general(
            res, refs[2 * g + 1][...], (((1,), (1,)), ((), ())), preferred_element_type=F32
        )
    out_ref[...] = total.astype(BF16)


def table_call(where, w, got, packs, count):
    tokens = packs[0].shape[1]
    block = 512
    specs, operands = [], []
    for pack in packs:
        specs.append(pl.BlockSpec((CHUNK, tokens), lambda i, s: (i, 0)))
        specs.append(pl.BlockSpec((block, tokens), lambda i, s: (4 + s[2], 0)))
        operands += [pack, pack]
    return pl.pallas_call(
        table_kernel,
        grid_spec=pltpu.PrefetchScalarGridSpec(
            num_scalar_prefetch=1,
            grid=(count // CHUNK,),
            in_specs=[
                pl.BlockSpec(w.shape, lambda i, s: (0, 0, 0)),
                pl.BlockSpec(got.shape, lambda i, s: (0, 0, 0)),
                *specs,
            ],
            out_specs=pl.BlockSpec((CHUNK, block), lambda i, s: (i, 0)),
            scratch_shapes=[pltpu.VMEM((512, block), BF16), pltpu.VMEM((8, 512), I32)],
        ),
        out_shape=jax.ShapeDtypeStruct((count, block), BF16),
        compiler_params=SIDE,
        cost_estimate=cost(2 * count * block * 1536, 8 * count * 256 + 2 * count * block),
        name="table_grad",
    )(where, w, got, *operands)


def inner(hidden, table, targets, input_ids, cotangent):
    vocab_rows, width = table.shape
    ny, nz, nx = (lax.axis_size(a) for a in VOCAB)
    plane = ny * nx
    vocab_count = plane * nz
    block = width // lax.axis_size(DP)
    xh, c = lax.axis_index("xh"), lax.axis_index("c")
    spot = lax.axis_index("y") * nx + lax.axis_index("xl")
    where = jnp.stack([lax.axis_index(VOCAB) * vocab_rows, xh, c, lax.axis_index("z"), spot]).astype(I32)
    tokens = hidden.shape[0]
    goal = targets.reshape(1, tokens)

    half = width // 2
    ids = jnp.stack([input_ids >> 14, (input_ids >> 7) & 127, input_ids & 127]).astype(BF16)
    ids = jnp.pad(ids, ((0, 5), (0, block - ids.shape[1])))
    ids = jnp.concatenate([ids, ids], axis=1)
    near_rows = lax.dynamic_slice_in_dim(cotangent, xh * half, half, 1)
    far_rows = lax.dynamic_slice_in_dim(cotangent, (1 - xh) * half, half, 1)
    near_rows = jnp.concatenate([near_rows, ids], axis=0)
    far_rows = jnp.concatenate([far_rows, ids], axis=0)
    far_rows = swap(far_rows, "xh")
    packs = (near_rows, swap(near_rows, "c"), far_rows, swap(far_rows, "c"))
    away, middle, one, x0, c0 = select_call(where, packs, vocab_rows)
    r1 = partner(away, 4)
    sent = join_call(one, middle, r1, c0)
    got1, got2, got3 = (partner(value, k + 1) for k, value in enumerate(sent))

    mine = hidden.T
    stage = exchange(to_each(mine, nz), "z").reshape(-1, tokens)
    stage = exchange(to_each(stage, plane), PLANE)
    far_stage = swap(stage, "xh")
    near, sums, own = logits_call(where, goal, stage, table, vocab_count)

    stats = exchange(sums, VOCAB)
    far, _, _ = logits_call(where, goal, far_stage, table, 1)
    near_sib = swap(near, "c")
    far_sib = swap(far, "c")
    part, loss, w = part_call(where, goal, own, stats, near, (x0, r1, got1, got2, got3, c0), table)

    got = exchange(part, PLANE)
    part = jnp.sum(got[:, : width // plane].astype(F32), axis=0).reshape(nz, -1, tokens)
    part = jnp.sum(exchange(part, "z"), axis=0)
    hidden_grad = part.astype(BF16).T

    w_near = jnp.stack([w, swap(w, "c")])
    w_far = swap(w_near, "xh")
    w_all = jnp.concatenate([w_near, w_far], axis=0)
    table_grad = table_call(
        where, w_all, got, (near, near_sib, far, far_sib), vocab_rows
    )
    return loss.reshape(tokens), hidden_grad, table_grad


def solution(mesh):
    fine = Mesh(mesh.devices.reshape(2, 2, 4, 8, 2), ALL)
    placed = (P(DP, VOCAB), P(VOCAB, None), P(DP), P(ALL), P(ALL, None))
    return jax.shard_map(
        inner,
        mesh=fine,
        in_specs=placed,
        out_specs=(P(DP), P(DP, VOCAB), P(VOCAB, DP)),
        check_vma=False,
    )
```
